32 devices in a mesh: fsdp: 8 (over z, y), tp: 4 (over x, core).
Axes of the slice: x: 2, y: 2, z: 4, core: 2. Of those that a mesh axis runs over, the one named last changes fastest.
Arguments:
- tokens: bfloat16 [16384, 768], P(('fsdp', 'tp')), may hold values from -6 to 6
- pass_ids: int32 [16384], P(('fsdp', 'tp')), may hold values from 0 to 4
- prefix: int32 [8], P('fsdp'), may hold values from 0 to 2047
- cotangent: bfloat16 [16384, 768], P(('fsdp', 'tp')), may hold values from -6 to 6
- qkv_weight: bfloat16 [3, 768, 768], P(None, 'fsdp', 'tp'), may hold values from -0.21875 to 0.21875
- out_weight: bfloat16 [768, 768], P('tp', 'fsdp'), may hold values from -1.75 to 1.75
- fc1_weight: bfloat16 [768, 3072], P('fsdp', 'tp'), may hold values from -0.21875 to 0.21875
- fc2_weight: bfloat16 [3072, 768], P('tp', 'fsdp'), may hold values from -0.109375 to 0.109375
- ln1_gain: float32 [768], replicated, may hold values from 0.1 to 1.9
- ln1_bias: float32 [768], replicated, may hold values from -2 to 2
- qv_bias: float32 [2, 768], replicated, may hold values from -2 to 2
- out_bias: float32 [768], replicated, may hold values from -2 to 2
- ln2_gain: float32 [768], replicated, may hold values from 0.1 to 1.9
- ln2_bias: float32 [768], replicated, may hold values from -2 to 2
- fc1_bias: float32 [3072], replicated, may hold values from -3 to 3
- fc2_bias: float32 [768], replicated, may hold values from -2 to 2
- pass_table: float32 [5, 768], replicated, may hold values from -3 to 3
Outputs:
- activations: bfloat16 [16384, 768], P(('fsdp', 'tp'))
- input_grad: float32 [16384, 768], P(('fsdp', 'tp'))
- qkv_grad: float32 [3, 768, 768], P(None, 'fsdp', 'tp')
- out_grad: float32 [768, 768], P('tp', 'fsdp')
- fc1_grad: float32 [768, 3072], P('fsdp', 'tp')
- fc2_grad: float32 [3072, 768], P('tp', 'fsdp')
- ln1_gain_grad: float32 [768], replicated
- ln1_bias_grad: float32 [768], replicated
- qv_bias_grad: float32 [2, 768], replicated
- out_bias_grad: float32 [768], replicated
- ln2_gain_grad: float32 [768], replicated
- ln2_bias_grad: float32 [768], replicated
- fc1_bias_grad: float32 [3072], replicated
- fc2_bias_grad: float32 [768], replicated
- pass_table_grad: float32 [5, 768], replicated
The draws below stay inside these ranges and needn't reach their ends.
All inputs are finite; a program needn't handle non-finite values.
Results may differ from the reference program's by a relative error of at most 0.009.
Values may be sent and summed in bfloat16 or wider, within the bound.
A program may use at most 128 MiB of HBM per device.

```python
import jax
import jax.numpy as jnp
from jax import lax

D = 768
HEADS = 12
HD = 64
FF = 3072
NPASS = 5
QBLOCK = 512
SEQ = 2048
NSEQ = 8
TOKENS = 16384


def plant(values, stream_key, low, top_value):
    longest = values.shape.index(max(values.shape))
    spots = []
    for shift in (0, 1):
        where = [jax.random.randint(jax.random.fold_in(stream_key, axis), (), 0, length) for axis, length in enumerate(values.shape)]
        where[longest] = (where[longest] + shift) % values.shape[longest]
        spots.append(tuple(where))
    return values.at[spots[0]].set(low).at[spots[1]].set(top_value)


def steps_of(stream_key, extent, cuts, low, top_value):
    def one(dim, blocks):
        steps = jax.random.uniform(jax.random.fold_in(jax.random.fold_in(stream_key, 6), dim), (blocks,), jnp.float32, low / len(cuts), top_value / len(cuts))
        return jnp.repeat(jnp.exp(steps), extent[dim] // blocks).reshape((-1,) + (1,) * (len(extent) - dim - 1))

    level = one(*cuts[0])
    for cut in cuts[1:]:
        level = level * one(*cut)
    return level


def centred(key, shape, spread, bound, shards=(), kind=jnp.bfloat16):
    level = steps_of(key, shape, shards, -0.22, 0.18) if shards else 1.0
    entries = jax.random.normal(key, shape, jnp.float32) * spread * level
    return jnp.minimum(jnp.maximum(entries, -bound), bound).astype(kind)


def setup_inputs(seed: int = 0) -> dict:
    arg_keys = jax.random.split(jax.random.key(seed), 18)
    return {
        "tokens": centred(arg_keys[0], (TOKENS, D), 1.0, 6.0, ((0, 32),)),
        "pass_ids": plant(jax.random.randint(arg_keys[1], (TOKENS,), 0, NPASS), jax.random.fold_in(arg_keys[1], 1), 0, NPASS - 1).astype(jnp.int32),
        "prefix": plant(jax.random.randint(arg_keys[2], (NSEQ,), 0, SEQ), jax.random.fold_in(arg_keys[2], 1), 0, SEQ - 1).astype(jnp.int32),
        "cotangent": centred(arg_keys[3], (TOKENS, D), 1.0, 6.0, ((0, 32),)),
        "qkv_weight": centred(arg_keys[4], (3, D, D), D ** -0.5, 0.21875, ((1, 8), (2, 4))),
        "out_weight": centred(arg_keys[5], (D, D), (max(D // 64, 1)) ** -0.5, 1.75, ((0, 4), (1, 8))),
        "fc1_weight": centred(arg_keys[6], (D, FF), D ** -0.5, 0.21875, ((0, 8), (1, 4))),
        "fc2_weight": centred(arg_keys[7], (FF, D), FF ** -0.5, 0.109375, ((0, 4), (1, 8))),
        "ln1_gain": jnp.clip(1.0 + 0.18 * jax.random.normal(arg_keys[8], (D,), jnp.float32), 0.1, 1.9),
        "ln1_bias": centred(arg_keys[9], (D,), 0.3, 2.0, (), jnp.float32),
        "qv_bias": centred(arg_keys[10], (2, D), 0.3, 2.0, (), jnp.float32),
        "out_bias": centred(arg_keys[11], (D,), 0.3, 2.0, (), jnp.float32),
        "ln2_gain": jnp.clip(1.0 + 0.18 * jax.random.normal(arg_keys[12], (D,), jnp.float32), 0.1, 1.9),
        "ln2_bias": centred(arg_keys[13], (D,), 0.3, 2.0, (), jnp.float32),
        "fc1_bias": centred(arg_keys[14], (FF,), 0.5, 3.0, (), jnp.float32),
        "fc2_bias": centred(arg_keys[15], (D,), 0.3, 2.0, (), jnp.float32),
        "pass_table": centred(arg_keys[16], (NPASS, D), 0.5, 3.0, (), jnp.float32),
    }


HIGH = lax.Precision.HIGHEST
EPS = 1e-05
NEG_FILL = -1e+30

@jax.custom_vjp
def low(v):
    return lax.optimization_barrier(v.astype(jnp.bfloat16)).astype(jnp.float32)

@jax.custom_vjp
def low_back(v):
    return v

def low_keep(v):
    return (low(v), None)

def low_pass(kept, grad):
    return (grad,)

def back_keep(v):
    return (v, None)

def back_low(kept, grad):
    return (low(grad),)
low.defvjp(low_keep, low_pass)
low_back.defvjp(back_keep, back_low)

def layer_norm(rows_in, gain, shift):
    center = rows_in - lax.optimization_barrier(jnp.mean(rows_in, axis=-1, keepdims=True))
    scale_inv = lax.rsqrt(lax.optimization_barrier(jnp.mean(center * center, axis=-1, keepdims=True)) + EPS)
    return center * scale_inv * gain + shift

def attend_block(query_block, row_start, keys_all, values_all, prefix_len):
    scale = HD ** (-0.5)
    raw = jnp.einsum('qhe,khe->hqk', query_block, keys_all, precision=HIGH)
    scores = low_back(raw * scale)
    row_ids = row_start + jnp.arange(QBLOCK, dtype=jnp.int32)
    col_ids = jnp.arange(SEQ, dtype=jnp.int32)
    allowed = (col_ids[None, :] <= row_ids[:, None]) | (col_ids[None, :] < prefix_len)
    masked = jnp.where(allowed[None], scores, NEG_FILL)
    peak = lax.optimization_barrier(jnp.max(masked, axis=-1, keepdims=True))
    expo = jnp.exp(masked - peak)
    probs = expo / lax.optimization_barrier(jnp.sum(expo, axis=-1, keepdims=True))
    return jnp.einsum('hqk,khe->qhe', low(probs), values_all, precision=HIGH)

def forward(rows_in, ids_seq, prefix_len, params):
    qkv_weight, out_weight, fc1_weight, fc2_weight, ln1_gain, ln1_bias, qv_bias, out_bias, ln2_gain, ln2_bias, fc1_bias, fc2_bias, pass_table = params
    block_in = rows_in + pass_table[ids_seq]
    normed = low(layer_norm(block_in, ln1_gain, ln1_bias))
    projected = jnp.einsum('rd,kdc->krc', normed, qkv_weight, precision=HIGH)
    queries = low(low_back(projected[0] + qv_bias[0])).reshape(SEQ, HEADS, HD)
    keys_all = low(low_back(projected[1])).reshape(SEQ, HEADS, HD)
    values_all = low(low_back(projected[2] + qv_bias[1])).reshape(SEQ, HEADS, HD)
    query_blocks = queries.reshape(SEQ // QBLOCK, QBLOCK, HEADS, HD)
    block_starts = jnp.arange(SEQ // QBLOCK, dtype=jnp.int32) * QBLOCK
    remat_block = jax.checkpoint(attend_block)

    def map_block(item):
        return remat_block(item[0], item[1], keys_all, values_all, prefix_len)
    attended = lax.map(map_block, (query_blocks, block_starts))
    mixed = low(low_back(attended.reshape(SEQ, D)))
    middle = block_in + low_back(jnp.dot(mixed, out_weight, precision=HIGH)) + out_bias
    normed_two = low(layer_norm(middle, ln2_gain, ln2_bias))
    before = low_back(jnp.dot(normed_two, fc1_weight, precision=HIGH) + fc1_bias)
    hidden = low(jax.nn.gelu(before, approximate=True))
    return middle + low_back(jnp.dot(hidden, fc2_weight, precision=HIGH)) + fc2_bias

def reference(tokens, pass_ids, prefix, cotangent, qkv_weight, out_weight, fc1_weight, fc2_weight, ln1_gain, ln1_bias, qv_bias, out_bias, ln2_gain, ln2_bias, fc1_bias, fc2_bias, pass_table):
    params = (qkv_weight.astype(jnp.float32), out_weight.astype(jnp.float32), fc1_weight.astype(jnp.float32), fc2_weight.astype(jnp.float32), ln1_gain.astype(jnp.float32), ln1_bias.astype(jnp.float32), qv_bias.astype(jnp.float32), out_bias.astype(jnp.float32), ln2_gain.astype(jnp.float32), ln2_bias.astype(jnp.float32), fc1_bias.astype(jnp.float32), fc2_bias.astype(jnp.float32), pass_table.astype(jnp.float32))
    rows_all = tokens.astype(jnp.float32).reshape(NSEQ, SEQ, D)
    grads_all = cotangent.astype(jnp.float32).reshape(NSEQ, SEQ, D)
    ids_all = pass_ids.astype(jnp.int32).reshape(NSEQ, SEQ)

    def one_sequence(totals, item):
        rows_in, ids_seq, prefix_len, grad_seq = item

        def local_forward(rows_value, param_values):
            return forward(rows_value, ids_seq, prefix_len, param_values)
        result, pull_back = jax.vjp(local_forward, rows_in, params)
        grad_rows, grad_params = pull_back(grad_seq)
        totals = jax.tree.map(lambda left, right: left + right, totals, grad_params)
        return (totals, (result.astype(jnp.bfloat16), grad_rows))
    zero_grads = jax.tree.map(jnp.zeros_like, params)
    totals, outputs = lax.scan(one_sequence, zero_grads, (rows_all, ids_all, prefix.astype(jnp.int32), grads_all))
    results, grad_rows = outputs
    return (results.reshape(TOKENS, D), grad_rows.reshape(TOKENS, D), totals[0], totals[1], totals[2], totals[3], totals[4], totals[5], totals[6], totals[7], totals[8], totals[9], totals[10], totals[11], totals[12])
```

```python
from functools import partial

import jax
import jax.numpy as jnp
from jax import lax
from jax.sharding import PartitionSpec as P

HD = 64
NPASS = 5
QBLOCK = 512


HIGH = lax.Precision.HIGHEST
EPS = 1e-05
NEG_FILL = -1e30


def norm_forward(rows_in, gain, shift):
    center = rows_in - jnp.mean(rows_in, axis=-1, keepdims=True)
    scale_inv = lax.rsqrt(jnp.mean(center * center, axis=-1, keepdims=True) + EPS)
    unit_rows = center * scale_inv
    return (unit_rows * gain + shift, unit_rows, scale_inv)


def norm_backward(grad_out, unit_rows, scale_inv, gain):
    grad_unit = grad_out * gain
    first_mean = jnp.mean(grad_unit, axis=-1, keepdims=True)
    second_mean = jnp.mean(grad_unit * unit_rows, axis=-1, keepdims=True)
    grad_rows = scale_inv * (grad_unit - first_mean - unit_rows * second_mean)
    return (grad_rows, jnp.sum(grad_out * unit_rows, axis=0), jnp.sum(grad_out, axis=0))


def matmul_nt(left, right):
    return lax.dot_general(
        left, right, (((1,), (1,)), ((), ())), preferred_element_type=jnp.float32
    )


def matmul_tn(left, right):
    return lax.dot_general(
        left, right, (((0,), (0,)), ((), ())), preferred_element_type=jnp.float32
    )


def block_scores(query_block, keys_all, row_start, prefix_len, scale):
    raw = (
        jnp.einsum("qhe,khe->hqk", query_block, keys_all, preferred_element_type=jnp.float32)
        * scale
    )
    row_ids = row_start + jnp.arange(query_block.shape[0], dtype=jnp.int32)
    col_ids = jnp.arange(keys_all.shape[0], dtype=jnp.int32)
    allowed = (col_ids[None, :] <= row_ids[:, None]) | (col_ids[None, :] < prefix_len)
    return jnp.where(allowed[None], raw, NEG_FILL)


def attend_forward(queries, keys_all, values_all, prefix_len, scale):
    seq_len, heads_here, head_size = queries.shape
    block_count = seq_len // QBLOCK
    query_blocks = queries.reshape(block_count, QBLOCK, heads_here, head_size)
    block_starts = jnp.arange(block_count, dtype=jnp.int32) * QBLOCK

    def one_block(item):
        query_block, row_start = item
        masked = block_scores(query_block, keys_all, row_start, prefix_len, scale)
        peak = jnp.max(masked, axis=-1, keepdims=True)
        expo = jnp.exp(masked - peak)
        total_mass = jnp.sum(expo, axis=-1, keepdims=True)
        probs_low = (expo / total_mass).astype(jnp.bfloat16)
        out_block = jnp.einsum(
            "hqk,khe->qhe", probs_low, values_all, preferred_element_type=jnp.float32
        )
        return (out_block.astype(jnp.bfloat16), (peak + jnp.log(total_mass))[..., 0])

    outputs, log_mass = lax.map(one_block, (query_blocks, block_starts))
    return (outputs.reshape(seq_len, heads_here * head_size), log_mass)


def attend_backward(queries, keys_all, values_all, grad_mixed, log_mass, prefix_len, scale):
    seq_len, heads_here, head_size = queries.shape
    block_count = seq_len // QBLOCK
    query_blocks = queries.reshape(block_count, QBLOCK, heads_here, head_size)
    grad_blocks = grad_mixed.reshape(block_count, QBLOCK, heads_here, head_size)
    block_starts = jnp.arange(block_count, dtype=jnp.int32) * QBLOCK

    def one_block(carry, item):
        grad_keys, grad_values = carry
        query_block, grad_block, block_mass, row_start = item
        masked = block_scores(query_block, keys_all, row_start, prefix_len, scale)
        probs = jnp.exp(masked - block_mass[..., None])
        probs_low = probs.astype(jnp.bfloat16)
        grad_values = grad_values + jnp.einsum(
            "hqk,qhe->khe", probs_low, grad_block, preferred_element_type=jnp.float32
        )
        grad_probs = jnp.einsum(
            "qhe,khe->hqk", grad_block, values_all, preferred_element_type=jnp.float32
        )
        inner_sum = jnp.sum(probs * grad_probs, axis=-1, keepdims=True)
        grad_scores = (probs * (grad_probs - inner_sum)).astype(jnp.bfloat16)
        grad_query = (
            jnp.einsum("hqk,khe->qhe", grad_scores, keys_all, preferred_element_type=jnp.float32)
            * scale
        )
        grad_keys = (
            grad_keys
            + jnp.einsum(
                "hqk,qhe->khe", grad_scores, query_block, preferred_element_type=jnp.float32
            )
            * scale
        )
        return ((grad_keys, grad_values), grad_query)

    zero_state = jnp.zeros(keys_all.shape, jnp.float32)
    (grad_keys, grad_values), grad_queries = lax.scan(
        one_block, (zero_state, zero_state), (query_blocks, grad_blocks, log_mass, block_starts)
    )
    return (grad_queries.reshape(seq_len, heads_here, head_size), grad_keys, grad_values)


def on_device(
    tokens,
    pass_ids,
    prefix,
    cotangent,
    qkv_weight,
    out_weight,
    fc1_weight,
    fc2_weight,
    ln1_gain,
    ln1_bias,
    qv_bias,
    out_bias,
    ln2_gain,
    ln2_bias,
    fc1_bias,
    fc2_bias,
    pass_table,
):
    tp_count = lax.axis_size("tp")
    tp_rank = lax.axis_index("tp")
    local_rows = tokens.shape[0]
    seq_len = local_rows * tp_count
    cols_here = qkv_weight.shape[2]
    heads_here = cols_here // HD
    scale = HD ** (-0.5)
    prefix_len = prefix[0]
    gelu_tanh = partial(jax.nn.gelu, approximate=True)
    fsdp_count = lax.axis_size("fsdp")
    shards = (qkv_weight, out_weight, fc1_weight, fc2_weight)
    packed = jnp.concatenate([piece.reshape(-1) for piece in shards])
    gathered = lax.all_gather(packed, "fsdp", axis=0, tiled=False)
    pieces = []
    offset = 0
    for piece in shards:
        size = piece.size
        pieces.append(gathered[:, offset : offset + size].reshape((fsdp_count,) + piece.shape))
        offset += size
    qkv_cols = jnp.moveaxis(pieces[0], 0, 1).reshape(3, -1, cols_here)
    out_heads = jnp.moveaxis(pieces[1], 0, 1).reshape(out_weight.shape[0], -1)
    fc1_part = pieces[2].reshape(-1, fc1_weight.shape[1])
    fc2_part = jnp.moveaxis(pieces[3], 0, 1).reshape(fc2_weight.shape[0], -1)
    out_all = lax.all_gather(out_heads, "tp", axis=0, tiled=True)
    qkv_all = lax.all_gather(qkv_cols, "tp", axis=2, tiled=True)
    qkv_full, out_full = qkv_cols, out_heads
    hidden_here = fc1_part.shape[1]
    qv_here = lax.dynamic_slice_in_dim(qv_bias, tp_rank * cols_here, cols_here, 1)
    one_hot = (pass_ids[:, None] == jnp.arange(NPASS, dtype=jnp.int32)[None, :]).astype(jnp.float32)
    block_in = tokens.astype(jnp.float32) + jnp.dot(
        one_hot, pass_table, precision=HIGH, preferred_element_type=jnp.float32
    )
    normed, unit_one, inv_one = norm_forward(block_in, ln1_gain, ln1_bias)
    normed_all = lax.all_gather(normed.astype(jnp.bfloat16), "tp", axis=0, tiled=True)
    projected = jnp.einsum("rd,kdc->krc", normed_all, qkv_full, preferred_element_type=jnp.float32)
    queries = (projected[0] + qv_here[0]).astype(jnp.bfloat16).reshape(seq_len, heads_here, HD)
    keys_all = projected[1].astype(jnp.bfloat16).reshape(seq_len, heads_here, HD)
    values_all = (projected[2] + qv_here[1]).astype(jnp.bfloat16).reshape(seq_len, heads_here, HD)
    mixed, log_mass = attend_forward(queries, keys_all, values_all, prefix_len, scale)
    mixed_rows = lax.all_to_all(mixed, "tp", 0, 1, tiled=True)
    middle = block_in + jnp.dot(mixed_rows, out_all, preferred_element_type=jnp.float32) + out_bias
    normed_two, unit_two, inv_two = norm_forward(middle, ln2_gain, ln2_bias)
    normed_two = normed_two.astype(jnp.bfloat16)
    grad_top = cotangent.astype(jnp.float32)
    fc1_bias_here = lax.dynamic_slice_in_dim(fc1_bias, tp_rank * hidden_here, hidden_here, 0)
    normed_rows = lax.all_gather(normed_two, "tp", axis=0, tiled=True)
    before = jnp.dot(normed_rows, fc1_part, preferred_element_type=jnp.float32) + fc1_bias_here
    hidden = gelu_tanh(before).astype(jnp.bfloat16)
    result = (
        middle
        + lax.psum_scatter(
            jnp.dot(
                lax.slice_in_dim(hidden, 0, local_rows * lax.axis_size("tp"), axis=0),
                fc2_part,
                preferred_element_type=jnp.float32,
            ).astype(jnp.bfloat16),
            "tp",
            scatter_dimension=0,
            tiled=True,
        ).astype(jnp.float32)
        + fc2_bias
    )
    grad_rows = lax.all_gather(cotangent, "tp", axis=0, tiled=True)
    grad_hidden = matmul_nt(grad_rows, fc2_part)
    grad_before = jax.vjp(gelu_tanh, before)[1](grad_hidden)[0].astype(jnp.bfloat16)
    grad_fc1_bias = lax.dynamic_update_slice_in_dim(
        jnp.zeros(fc1_bias.shape, jnp.float32),
        jnp.sum(grad_before.astype(jnp.float32), axis=0),
        tp_rank * hidden_here,
        0,
    )
    grad_fc1 = matmul_tn(normed_rows, grad_before)
    grad_fc2 = matmul_tn(hidden, grad_rows)
    grad_normed_two = lax.psum_scatter(
        matmul_nt(grad_before, fc1_part), "tp", scatter_dimension=0, tiled=True
    )
    grad_fc2_bias = jnp.sum(grad_top, axis=0)
    grad_from_norm, grad_ln2_gain, grad_ln2_bias = norm_backward(
        grad_normed_two, unit_two, inv_two, ln2_gain
    )
    grad_middle = grad_top + grad_from_norm
    grad_out_bias = jnp.sum(grad_middle, axis=0)
    grad_attn_rows = lax.all_gather(grad_middle.astype(jnp.bfloat16), "tp", axis=0, tiled=True)
    grad_out_w = matmul_tn(mixed, grad_attn_rows)
    grad_mixed = (
        matmul_nt(grad_attn_rows, out_full).astype(jnp.bfloat16).reshape(seq_len, heads_here, HD)
    )
    grad_queries, grad_keys, grad_values = attend_backward(
        queries, keys_all, values_all, grad_mixed, log_mass, prefix_len, scale
    )
    grad_q_low = grad_queries.astype(jnp.bfloat16).reshape(seq_len, cols_here)
    grad_k_low = grad_keys.astype(jnp.bfloat16).reshape(seq_len, cols_here)
    grad_v_low = grad_values.astype(jnp.bfloat16).reshape(seq_len, cols_here)
    grad_proj = jnp.stack([grad_q_low, grad_k_low, grad_v_low], axis=1)
    grad_qv_here = jnp.stack(
        [
            jnp.sum(grad_q_low.astype(jnp.float32), axis=0),
            jnp.sum(grad_v_low.astype(jnp.float32), axis=0),
        ],
        axis=0,
    )
    grad_qv_bias = lax.dynamic_update_slice_in_dim(
        jnp.zeros(qv_bias.shape, jnp.float32), grad_qv_here, tp_rank * cols_here, 1
    )
    grad_qkv_w = jnp.einsum(
        "rd,rkc->kdc", normed_all, grad_proj, preferred_element_type=jnp.float32
    )
    grad_proj_rows = lax.all_to_all(grad_proj, "tp", 0, 2, tiled=True)
    grad_normed = jnp.einsum(
        "rkc,kdc->rd", grad_proj_rows, qkv_all, preferred_element_type=jnp.float32
    )
    grad_in_norm, grad_ln1_gain, grad_ln1_bias = norm_backward(
        grad_normed, unit_one, inv_one, ln1_gain
    )
    grad_input = grad_middle + grad_in_norm
    grad_table = lax.dot_general(
        one_hot,
        grad_input,
        (((0,), (0,)), ((), ())),
        precision=HIGH,
        preferred_element_type=jnp.float32,
    )
    qkv_shard, out_shard, fc1_shard, fc2_shard = (
        lax.psum_scatter(grad_qkv_w, "fsdp", scatter_dimension=1, tiled=True),
        lax.psum_scatter(grad_out_w, "fsdp", scatter_dimension=1, tiled=True),
        lax.psum_scatter(grad_fc1, "fsdp", scatter_dimension=0, tiled=True),
        lax.psum_scatter(grad_fc2, "fsdp", scatter_dimension=1, tiled=True),
    )
    summed = lax.psum(
        (
            grad_ln1_gain,
            grad_ln1_bias,
            grad_qv_bias,
            grad_out_bias,
            grad_ln2_gain,
            grad_ln2_bias,
            grad_fc1_bias,
            grad_fc2_bias,
            grad_table,
        ),
        ("fsdp", "tp"),
    )
    return (
        result.astype(jnp.bfloat16),
        grad_input,
        qkv_shard,
        out_shard,
        fc1_shard,
        fc2_shard,
        summed[0],
        summed[1],
        summed[2],
        summed[3],
        summed[4],
        summed[5],
        summed[6],
        summed[7],
        summed[8],
    )


def solution(mesh):
    placed = (
        P(("fsdp", "tp"), None),
        P(("fsdp", "tp")),
        P("fsdp"),
        P(("fsdp", "tp"), None),
        P(None, "fsdp", "tp"),
        P("tp", "fsdp"),
        P("fsdp", "tp"),
        P("tp", "fsdp"),
        P(),
        P(),
        P(),
        P(),
        P(),
        P(),
        P(),
        P(),
        P(),
    )
    return jax.shard_map(
        on_device,
        mesh=mesh,
        in_specs=placed,
        out_specs=(
            P(("fsdp", "tp"), None),
            P(("fsdp", "tp"), None),
            P(None, "fsdp", "tp"),
            P("tp", "fsdp"),
            P("fsdp", "tp"),
            P("tp", "fsdp"),
            P(),
            P(),
            P(),
            P(),
            P(),
            P(),
            P(),
            P(),
            P(),
        ),
        check_vma=False,
    )
```

```python
from functools import partial

import jax
import jax.numpy as jnp
from jax import lax
from jax.sharding import PartitionSpec as P

HD = 64
NPASS = 5
QBLOCK = 512


HIGH = lax.Precision.HIGHEST
EPS = 1e-05
NEG_FILL = -1e30


def norm_forward(rows_in, gain, shift):
    center = rows_in - jnp.mean(rows_in, axis=-1, keepdims=True)
    scale_inv = lax.rsqrt(jnp.mean(center * center, axis=-1, keepdims=True) + EPS)
    unit_rows = center * scale_inv
    return (unit_rows * gain + shift, unit_rows, scale_inv)


def norm_backward(grad_out, unit_rows, scale_inv, gain):
    grad_unit = grad_out * gain
    first_mean = jnp.mean(grad_unit, axis=-1, keepdims=True)
    second_mean = jnp.mean(grad_unit * unit_rows, axis=-1, keepdims=True)
    grad_rows = scale_inv * (grad_unit - first_mean - unit_rows * second_mean)
    return (grad_rows, jnp.sum(grad_out * unit_rows, axis=0), jnp.sum(grad_out, axis=0))


def matmul_nt(left, right):
    return lax.dot_general(
        left, right, (((1,), (1,)), ((), ())), preferred_element_type=jnp.float32
    )


def matmul_tn(left, right):
    return lax.dot_general(
        left, right, (((0,), (0,)), ((), ())), preferred_element_type=jnp.float32
    )


def block_scores(query_block, keys_all, row_start, prefix_len, scale):
    raw = (
        jnp.einsum("qhe,khe->hqk", query_block, keys_all, preferred_element_type=jnp.float32)
        * scale
    )
    row_ids = row_start + jnp.arange(query_block.shape[0], dtype=jnp.int32)
    col_ids = jnp.arange(keys_all.shape[0], dtype=jnp.int32)
    allowed = (col_ids[None, :] <= row_ids[:, None]) | (col_ids[None, :] < prefix_len)
    return jnp.where(allowed[None], raw, NEG_FILL)


def attend_forward(queries, keys_all, values_all, prefix_len, scale):
    seq_len, heads_here, head_size = queries.shape
    block_count = seq_len // QBLOCK
    query_blocks = queries.reshape(block_count, QBLOCK, heads_here, head_size)
    block_starts = jnp.arange(block_count, dtype=jnp.int32) * QBLOCK

    def one_block(item):
        query_block, row_start = item
        masked = block_scores(query_block, keys_all, row_start, prefix_len, scale)
        peak = jnp.max(masked, axis=-1, keepdims=True)
        expo = jnp.exp(masked - peak)
        total_mass = jnp.sum(expo, axis=-1, keepdims=True)
        probs_low = (expo / total_mass).astype(jnp.bfloat16)
        out_block = jnp.einsum(
            "hqk,khe->qhe", probs_low, values_all, preferred_element_type=jnp.float32
        )
        return (out_block.astype(jnp.bfloat16), (peak + jnp.log(total_mass))[..., 0])

    outputs, log_mass = lax.map(one_block, (query_blocks, block_starts))
    return (outputs.reshape(seq_len, heads_here * head_size), log_mass)


def attend_backward(queries, keys_all, values_all, grad_mixed, log_mass, prefix_len, scale):
    seq_len, heads_here, head_size = queries.shape
    block_count = seq_len // QBLOCK
    query_blocks = queries.reshape(block_count, QBLOCK, heads_here, head_size)
    grad_blocks = grad_mixed.reshape(block_count, QBLOCK, heads_here, head_size)
    block_starts = jnp.arange(block_count, dtype=jnp.int32) * QBLOCK

    def one_block(carry, item):
        grad_keys, grad_values = carry
        query_block, grad_block, block_mass, row_start = item
        masked = block_scores(query_block, keys_all, row_start, prefix_len, scale)
        probs = jnp.exp(masked - block_mass[..., None])
        probs_low = probs.astype(jnp.bfloat16)
        grad_values = grad_values + jnp.einsum(
            "hqk,qhe->khe", probs_low, grad_block, preferred_element_type=jnp.float32
        )
        grad_probs = jnp.einsum(
            "qhe,khe->hqk", grad_block, values_all, preferred_element_type=jnp.float32
        )
        inner_sum = jnp.sum(probs * grad_probs, axis=-1, keepdims=True)
        grad_scores = (probs * (grad_probs - inner_sum)).astype(jnp.bfloat16)
        grad_query = (
            jnp.einsum("hqk,khe->qhe", grad_scores, keys_all, preferred_element_type=jnp.float32)
            * scale
        )
        grad_keys = (
            grad_keys
            + jnp.einsum(
                "hqk,qhe->khe", grad_scores, query_block, preferred_element_type=jnp.float32
            )
            * scale
        )
        return ((grad_keys, grad_values), grad_query)

    zero_state = jnp.zeros(keys_all.shape, jnp.float32)
    (grad_keys, grad_values), grad_queries = lax.scan(
        one_block, (zero_state, zero_state), (query_blocks, grad_blocks, log_mass, block_starts)
    )
    return (grad_queries.reshape(seq_len, heads_here, head_size), grad_keys, grad_values)


def on_device(
    tokens,
    pass_ids,
    prefix,
    cotangent,
    qkv_weight,
    out_weight,
    fc1_weight,
    fc2_weight,
    ln1_gain,
    ln1_bias,
    qv_bias,
    out_bias,
    ln2_gain,
    ln2_bias,
    fc1_bias,
    fc2_bias,
    pass_table,
):
    tp_count = lax.axis_size("tp")
    tp_rank = lax.axis_index("tp")
    local_rows = tokens.shape[0]
    seq_len = local_rows * tp_count
    cols_here = qkv_weight.shape[2]
    heads_here = cols_here // HD
    scale = HD ** (-0.5)
    prefix_len = prefix[0]
    gelu_tanh = partial(jax.nn.gelu, approximate=True)
    fsdp_count = lax.axis_size("fsdp")
    shards = (qkv_weight, out_weight, fc1_weight, fc2_weight)
    packed = jnp.concatenate([piece.reshape(-1) for piece in shards])
    gathered = lax.all_gather(packed, "fsdp", axis=0, tiled=False)
    pieces = []
    offset = 0
    for piece in shards:
        size = piece.size
        pieces.append(gathered[:, offset : offset + size].reshape((fsdp_count,) + piece.shape))
        offset += size
    qkv_cols = jnp.moveaxis(pieces[0], 0, 1).reshape(3, -1, cols_here)
    out_heads = jnp.moveaxis(pieces[1], 0, 1).reshape(out_weight.shape[0], -1)
    fc1_part = pieces[2].reshape(-1, fc1_weight.shape[1])
    fc2_part = jnp.moveaxis(pieces[3], 0, 1).reshape(fc2_weight.shape[0], -1)
    out_all = lax.all_gather(out_heads, "tp", axis=0, tiled=True)
    qkv_all = lax.all_gather(qkv_cols, "tp", axis=2, tiled=True)
    qkv_full, out_full = qkv_cols, out_heads
    hidden_here = fc1_part.shape[1]
    qv_here = lax.dynamic_slice_in_dim(qv_bias, tp_rank * cols_here, cols_here, 1)
    one_hot = (pass_ids[:, None] == jnp.arange(NPASS, dtype=jnp.int32)[None, :]).astype(jnp.float32)
    block_in = tokens.astype(jnp.float32) + jnp.dot(
        one_hot, pass_table, precision=HIGH, preferred_element_type=jnp.float32
    )
    normed, unit_one, inv_one = norm_forward(block_in, ln1_gain, ln1_bias)
    normed_all = lax.all_gather(normed.astype(jnp.bfloat16), "tp", axis=0, tiled=True)
    projected = jnp.einsum("rd,kdc->krc", normed_all, qkv_full, preferred_element_type=jnp.float32)
    queries = (projected[0] + qv_here[0]).astype(jnp.bfloat16).reshape(seq_len, heads_here, HD)
    keys_all = projected[1].astype(jnp.bfloat16).reshape(seq_len, heads_here, HD)
    values_all = (projected[2] + qv_here[1]).astype(jnp.bfloat16).reshape(seq_len, heads_here, HD)
    mixed, log_mass = attend_forward(queries, keys_all, values_all, prefix_len, scale)
    mixed, qkv_all = lax.optimization_barrier((mixed, qkv_all))
    mixed_rows = lax.all_to_all(mixed, "tp", 0, 1, tiled=True)
    middle = block_in + jnp.dot(mixed_rows, out_all, preferred_element_type=jnp.float32) + out_bias
    normed_two, unit_two, inv_two = norm_forward(middle, ln2_gain, ln2_bias)
    normed_two = normed_two.astype(jnp.bfloat16)
    grad_top = cotangent.astype(jnp.float32)
    fc1_bias_here = lax.dynamic_slice_in_dim(fc1_bias, tp_rank * hidden_here, hidden_here, 0)
    normed_rows = lax.all_gather(normed_two, "tp", axis=0, tiled=True)
    before = jnp.dot(normed_rows, fc1_part, preferred_element_type=jnp.float32) + fc1_bias_here
    hidden = gelu_tanh(before).astype(jnp.bfloat16)
    fc2_partial = jnp.dot(hidden, fc2_part, preferred_element_type=jnp.float32).astype(jnp.bfloat16)
    grad_rows = lax.all_gather(cotangent, "tp", axis=0, tiled=True)
    grad_hidden = matmul_nt(grad_rows, fc2_part)
    grad_before = jax.vjp(gelu_tanh, before)[1](grad_hidden)[0].astype(jnp.bfloat16)
    grad_fc1_bias = lax.dynamic_update_slice_in_dim(
        jnp.zeros(fc1_bias.shape, jnp.float32),
        jnp.sum(grad_before.astype(jnp.float32), axis=0),
        tp_rank * hidden_here,
        0,
    )
    grad_fc1 = matmul_tn(normed_rows, grad_before)
    grad_fc2 = matmul_tn(hidden, grad_rows)
    grad_normed_two = lax.psum_scatter(
        matmul_nt(grad_before, fc1_part), "tp", scatter_dimension=0, tiled=True
    )
    grad_fc2_bias = jnp.sum(grad_top, axis=0)
    grad_from_norm, grad_ln2_gain, grad_ln2_bias = norm_backward(
        grad_normed_two, unit_two, inv_two, ln2_gain
    )
    grad_middle = grad_top + grad_from_norm
    grad_out_bias = jnp.sum(grad_middle, axis=0)
    grad_attn_rows = lax.all_gather(grad_middle.astype(jnp.bfloat16), "tp", axis=0, tiled=True)
    fc2_partial, grad_attn_rows = lax.optimization_barrier((fc2_partial, grad_attn_rows))
    result = (
        middle
        + lax.psum_scatter(fc2_partial, "tp", scatter_dimension=0, tiled=True).astype(jnp.float32)
        + fc2_bias
    )
    grad_out_w = matmul_tn(mixed, grad_attn_rows)
    fsdp_count = lax.axis_size("fsdp")
    dense_grads = (
        jnp.moveaxis(grad_out_w.reshape(grad_out_w.shape[0], fsdp_count, -1), 1, 0),
        grad_fc1.reshape(fsdp_count, -1, grad_fc1.shape[1]),
        jnp.moveaxis(grad_fc2.reshape(grad_fc2.shape[0], fsdp_count, -1), 1, 0),
    )
    dense_packed = jnp.concatenate([g.reshape(fsdp_count, -1) for g in dense_grads], axis=1)
    dense_summed = lax.psum_scatter(
        dense_packed.reshape(-1, grad_fc1.shape[1]), "fsdp", scatter_dimension=0, tiled=True
    ).reshape(1, -1)
    grad_mixed = (
        matmul_nt(grad_attn_rows, out_full).astype(jnp.bfloat16).reshape(seq_len, heads_here, HD)
    )
    grad_queries, grad_keys, grad_values = attend_backward(
        queries, keys_all, values_all, grad_mixed, log_mass, prefix_len, scale
    )
    grad_q_low = grad_queries.astype(jnp.bfloat16).reshape(seq_len, cols_here)
    grad_k_low = grad_keys.astype(jnp.bfloat16).reshape(seq_len, cols_here)
    grad_v_low = grad_values.astype(jnp.bfloat16).reshape(seq_len, cols_here)
    grad_proj = jnp.stack([grad_q_low, grad_k_low, grad_v_low], axis=1)
    grad_proj, result, dense_summed = lax.optimization_barrier((grad_proj, result, dense_summed))
    dense_shards = []
    offset = 0
    for g in dense_grads:
        size = g[0].size
        dense_shards.append(dense_summed[0, offset : offset + size].reshape(g.shape[1:]))
        offset += size
    out_shard, fc1_shard, fc2_shard = dense_shards
    grad_qv_here = jnp.stack(
        [
            jnp.sum(grad_q_low.astype(jnp.float32), axis=0),
            jnp.sum(grad_v_low.astype(jnp.float32), axis=0),
        ],
        axis=0,
    )
    grad_qv_bias = lax.dynamic_update_slice_in_dim(
        jnp.zeros(qv_bias.shape, jnp.float32), grad_qv_here, tp_rank * cols_here, 1
    )
    grad_qkv_w = jnp.einsum(
        "rd,rkc->kdc", normed_all, grad_proj, preferred_element_type=jnp.float32
    )
    grad_proj_rows = lax.all_to_all(grad_proj, "tp", 0, 2, tiled=True)
    grad_normed = jnp.einsum(
        "rkc,kdc->rd", grad_proj_rows, qkv_all, preferred_element_type=jnp.float32
    )
    grad_in_norm, grad_ln1_gain, grad_ln1_bias = norm_backward(
        grad_normed, unit_one, inv_one, ln1_gain
    )
    grad_input = grad_middle + grad_in_norm
    grad_table = lax.dot_general(
        one_hot,
        grad_input,
        (((0,), (0,)), ((), ())),
        precision=HIGH,
        preferred_element_type=jnp.float32,
    )
    qkv_shard = lax.psum_scatter(grad_qkv_w, "fsdp", scatter_dimension=1, tiled=True)
    summed = lax.psum(
        (
            grad_ln1_gain,
            grad_ln1_bias,
            grad_qv_bias,
            grad_out_bias,
            grad_ln2_gain,
            grad_ln2_bias,
            grad_fc1_bias,
            grad_fc2_bias,
            grad_table,
        ),
        ("fsdp", "tp"),
    )
    return (
        result.astype(jnp.bfloat16),
        grad_input,
        qkv_shard,
        out_shard,
        fc1_shard,
        fc2_shard,
        summed[0],
        summed[1],
        summed[2],
        summed[3],
        summed[4],
        summed[5],
        summed[6],
        summed[7],
        summed[8],
    )


def solution(mesh):
    placed = (
        P(("fsdp", "tp"), None),
        P(("fsdp", "tp")),
        P("fsdp"),
        P(("fsdp", "tp"), None),
        P(None, "fsdp", "tp"),
        P("tp", "fsdp"),
        P("fsdp", "tp"),
        P("tp", "fsdp"),
        P(),
        P(),
        P(),
        P(),
        P(),
        P(),
        P(),
        P(),
        P(),
    )
    return jax.shard_map(
        on_device,
        mesh=mesh,
        in_specs=placed,
        out_specs=(
            P(("fsdp", "tp"), None),
            P(("fsdp", "tp"), None),
            P(None, "fsdp", "tp"),
            P("tp", "fsdp"),
            P("fsdp", "tp"),
            P("tp", "fsdp"),
            P(),
            P(),
            P(),
            P(),
            P(),
            P(),
            P(),
            P(),
            P(),
        ),
        check_vma=False,
    )
```

```python
from functools import partial

import jax
import jax.numpy as jnp
from jax import lax
from jax.sharding import PartitionSpec as P

HD = 64
NPASS = 5
QBLOCK = 512


HIGH = lax.Precision.HIGHEST
EPS = 1e-05
NEG_FILL = -1e30


def norm_forward(rows_in, gain, shift):
    center = rows_in - jnp.mean(rows_in, axis=-1, keepdims=True)
    scale_inv = lax.rsqrt(jnp.mean(center * center, axis=-1, keepdims=True) + EPS)
    unit_rows = center * scale_inv
    return (unit_rows * gain + shift, unit_rows, scale_inv)


def norm_backward(grad_out, unit_rows, scale_inv, gain):
    grad_unit = grad_out * gain
    first_mean = jnp.mean(grad_unit, axis=-1, keepdims=True)
    second_mean = jnp.mean(grad_unit * unit_rows, axis=-1, keepdims=True)
    grad_rows = scale_inv * (grad_unit - first_mean - unit_rows * second_mean)
    return (grad_rows, jnp.sum(grad_out * unit_rows, axis=0), jnp.sum(grad_out, axis=0))


def matmul_nt(left, right):
    return lax.dot_general(
        left, right, (((1,), (1,)), ((), ())), preferred_element_type=jnp.float32
    )


def matmul_tn(left, right):
    return lax.dot_general(
        left, right, (((0,), (0,)), ((), ())), preferred_element_type=jnp.float32
    )


def block_scores(query_block, keys_all, row_start, prefix_len, scale):
    raw = (
        jnp.einsum("qhe,khe->hqk", query_block, keys_all, preferred_element_type=jnp.float32)
        * scale
    )
    row_ids = row_start + jnp.arange(query_block.shape[0], dtype=jnp.int32)
    col_ids = jnp.arange(keys_all.shape[0], dtype=jnp.int32)
    allowed = (col_ids[None, :] <= row_ids[:, None]) | (col_ids[None, :] < prefix_len)
    return jnp.where(allowed[None], raw, NEG_FILL)


def attend_forward(queries, keys_all, values_all, prefix_len, scale):
    seq_len, heads_here, head_size = queries.shape
    block_count = seq_len // QBLOCK
    query_blocks = queries.reshape(block_count, QBLOCK, heads_here, head_size)
    block_starts = jnp.arange(block_count, dtype=jnp.int32) * QBLOCK

    def one_block(item):
        query_block, row_start = item
        masked = block_scores(query_block, keys_all, row_start, prefix_len, scale)
        peak = jnp.max(masked, axis=-1, keepdims=True)
        expo = jnp.exp(masked - peak)
        total_mass = jnp.sum(expo, axis=-1, keepdims=True)
        probs_low = (expo / total_mass).astype(jnp.bfloat16)
        out_block = jnp.einsum(
            "hqk,khe->qhe", probs_low, values_all, preferred_element_type=jnp.float32
        )
        return (out_block.astype(jnp.bfloat16), (peak + jnp.log(total_mass))[..., 0])

    outputs, log_mass = lax.map(one_block, (query_blocks, block_starts))
    return (outputs.reshape(seq_len, heads_here * head_size), log_mass)


def attend_backward(queries, keys_all, values_all, grad_mixed, log_mass, prefix_len, scale):
    seq_len, heads_here, head_size = queries.shape
    block_count = seq_len // QBLOCK
    query_blocks = queries.reshape(block_count, QBLOCK, heads_here, head_size)
    grad_blocks = grad_mixed.reshape(block_count, QBLOCK, heads_here, head_size)
    block_starts = jnp.arange(block_count, dtype=jnp.int32) * QBLOCK

    def one_block(carry, item):
        grad_keys, grad_values = carry
        query_block, grad_block, block_mass, row_start = item
        masked = block_scores(query_block, keys_all, row_start, prefix_len, scale)
        probs = jnp.exp(masked - block_mass[..., None])
        probs_low = probs.astype(jnp.bfloat16)
        grad_values = grad_values + jnp.einsum(
            "hqk,qhe->khe", probs_low, grad_block, preferred_element_type=jnp.float32
        )
        grad_probs = jnp.einsum(
            "qhe,khe->hqk", grad_block, values_all, preferred_element_type=jnp.float32
        )
        inner_sum = jnp.sum(probs * grad_probs, axis=-1, keepdims=True)
        grad_scores = (probs * (grad_probs - inner_sum)).astype(jnp.bfloat16)
        grad_query = (
            jnp.einsum("hqk,khe->qhe", grad_scores, keys_all, preferred_element_type=jnp.float32)
            * scale
        )
        grad_keys = (
            grad_keys
            + jnp.einsum(
                "hqk,qhe->khe", grad_scores, query_block, preferred_element_type=jnp.float32
            )
            * scale
        )
        return ((grad_keys, grad_values), grad_query)

    zero_state = jnp.zeros(keys_all.shape, jnp.float32)
    (grad_keys, grad_values), grad_queries = lax.scan(
        one_block, (zero_state, zero_state), (query_blocks, grad_blocks, log_mass, block_starts)
    )
    return (grad_queries.reshape(seq_len, heads_here, head_size), grad_keys, grad_values)


def on_device(
    tokens,
    pass_ids,
    prefix,
    cotangent,
    qkv_weight,
    out_weight,
    fc1_weight,
    fc2_weight,
    ln1_gain,
    ln1_bias,
    qv_bias,
    out_bias,
    ln2_gain,
    ln2_bias,
    fc1_bias,
    fc2_bias,
    pass_table,
):
    tp_count = lax.axis_size("tp")
    tp_rank = lax.axis_index("tp")
    local_rows = tokens.shape[0]
    seq_len = local_rows * tp_count
    cols_here = qkv_weight.shape[2]
    heads_here = cols_here // HD
    scale = HD ** (-0.5)
    prefix_len = prefix[0]
    gelu_tanh = partial(jax.nn.gelu, approximate=True)
    fsdp_count = lax.axis_size("fsdp")
    qkv_cols = lax.all_gather(qkv_weight, "fsdp", axis=1, tiled=True)
    qkv_full = qkv_cols
    hidden_here = fc1_weight.shape[1]
    qv_here = lax.dynamic_slice_in_dim(qv_bias, tp_rank * cols_here, cols_here, 1)
    one_hot = (pass_ids[:, None] == jnp.arange(NPASS, dtype=jnp.int32)[None, :]).astype(jnp.float32)
    block_in = tokens.astype(jnp.float32) + jnp.dot(
        one_hot, pass_table, precision=HIGH, preferred_element_type=jnp.float32
    )
    normed, unit_one, inv_one = norm_forward(block_in, ln1_gain, ln1_bias)
    normed_all = lax.all_gather(normed.astype(jnp.bfloat16), "tp", axis=0, tiled=True)
    shards = (out_weight, fc1_weight, fc2_weight)
    packed = jnp.concatenate([piece.reshape(-1) for piece in shards])
    packed, normed_all = lax.optimization_barrier((packed, normed_all))
    gathered = lax.all_gather(packed, "fsdp", axis=0, tiled=False)
    pieces = []
    offset = 0
    for piece in shards:
        size = piece.size
        pieces.append(gathered[:, offset : offset + size].reshape((fsdp_count,) + piece.shape))
        offset += size
    out_heads = jnp.moveaxis(pieces[0], 0, 1).reshape(out_weight.shape[0], -1)
    fc1_part = pieces[1].reshape(-1, fc1_weight.shape[1])
    fc2_part = jnp.moveaxis(pieces[2], 0, 1).reshape(fc2_weight.shape[0], -1)
    out_all = lax.all_gather(out_heads, "tp", axis=0, tiled=True)
    qkv_all = lax.all_gather(qkv_cols, "tp", axis=2, tiled=True)
    out_full = out_heads
    grad_rows = lax.all_gather(cotangent, "tp", axis=0, tiled=True)
    projected = jnp.einsum("rd,kdc->krc", normed_all, qkv_full, preferred_element_type=jnp.float32)
    queries = (projected[0] + qv_here[0]).astype(jnp.bfloat16).reshape(seq_len, heads_here, HD)
    keys_all = projected[1].astype(jnp.bfloat16).reshape(seq_len, heads_here, HD)
    values_all = (projected[2] + qv_here[1]).astype(jnp.bfloat16).reshape(seq_len, heads_here, HD)
    mixed, log_mass = attend_forward(queries, keys_all, values_all, prefix_len, scale)
    mixed, grad_rows = lax.optimization_barrier((mixed, grad_rows))
    mixed_rows = lax.all_to_all(mixed, "tp", 0, 1, tiled=True)
    middle = block_in + jnp.dot(mixed_rows, out_all, preferred_element_type=jnp.float32) + out_bias
    normed_two, unit_two, inv_two = norm_forward(middle, ln2_gain, ln2_bias)
    normed_two = normed_two.astype(jnp.bfloat16)
    grad_top = cotangent.astype(jnp.float32)
    fc1_bias_here = lax.dynamic_slice_in_dim(fc1_bias, tp_rank * hidden_here, hidden_here, 0)
    normed_rows = lax.all_gather(normed_two, "tp", axis=0, tiled=True)
    before = jnp.dot(normed_rows, fc1_part, preferred_element_type=jnp.float32) + fc1_bias_here
    hidden = gelu_tanh(before).astype(jnp.bfloat16)
    fc2_partial = jnp.dot(hidden, fc2_part, preferred_element_type=jnp.float32).astype(jnp.bfloat16)
    grad_hidden = matmul_nt(grad_rows, fc2_part)
    grad_before = jax.vjp(gelu_tanh, before)[1](grad_hidden)[0].astype(jnp.bfloat16)
    grad_fc1_bias = lax.dynamic_update_slice_in_dim(
        jnp.zeros(fc1_bias.shape, jnp.float32),
        jnp.sum(grad_before.astype(jnp.float32), axis=0),
        tp_rank * hidden_here,
        0,
    )
    grad_fc1 = matmul_tn(normed_rows, grad_before)
    grad_fc2 = matmul_tn(hidden, grad_rows)
    grad_normed_two = lax.psum_scatter(
        matmul_nt(grad_before, fc1_part), "tp", scatter_dimension=0, tiled=True
    )
    grad_normed_two, fc2_partial, grad_fc1, grad_fc2 = lax.optimization_barrier(
        (grad_normed_two, fc2_partial, grad_fc1, grad_fc2)
    )
    grad_fc2_bias = jnp.sum(grad_top, axis=0)
    grad_from_norm, grad_ln2_gain, grad_ln2_bias = norm_backward(
        grad_normed_two, unit_two, inv_two, ln2_gain
    )
    grad_middle = grad_top + grad_from_norm
    grad_out_bias = jnp.sum(grad_middle, axis=0)
    grad_attn_rows = lax.all_gather(grad_middle.astype(jnp.bfloat16), "tp", axis=0, tiled=True)
    fc2_partial, grad_attn_rows = lax.optimization_barrier((fc2_partial, grad_attn_rows))
    result = (
        middle
        + lax.psum_scatter(fc2_partial, "tp", scatter_dimension=0, tiled=True).astype(jnp.float32)
        + fc2_bias
    )
    grad_out_w = matmul_tn(mixed, grad_attn_rows)
    fsdp_count = lax.axis_size("fsdp")
    dense_grads = (
        jnp.moveaxis(grad_out_w.reshape(grad_out_w.shape[0], fsdp_count, -1), 1, 0),
        grad_fc1.reshape(fsdp_count, -1, grad_fc1.shape[1]),
        jnp.moveaxis(grad_fc2.reshape(grad_fc2.shape[0], fsdp_count, -1), 1, 0),
    )
    dense_packed = jnp.concatenate([g.reshape(fsdp_count, -1) for g in dense_grads], axis=1)
    dense_summed = lax.psum_scatter(
        dense_packed.reshape(-1, grad_fc1.shape[1]), "fsdp", scatter_dimension=0, tiled=True
    ).reshape(1, -1)
    grad_mixed = (
        matmul_nt(grad_attn_rows, out_full).astype(jnp.bfloat16).reshape(seq_len, heads_here, HD)
    )
    grad_queries, grad_keys, grad_values = attend_backward(
        queries, keys_all, values_all, grad_mixed, log_mass, prefix_len, scale
    )
    grad_q_low = grad_queries.astype(jnp.bfloat16).reshape(seq_len, cols_here)
    grad_k_low = grad_keys.astype(jnp.bfloat16).reshape(seq_len, cols_here)
    grad_v_low = grad_values.astype(jnp.bfloat16).reshape(seq_len, cols_here)
    grad_proj = jnp.stack([grad_q_low, grad_k_low, grad_v_low], axis=1)
    grad_proj, result, dense_summed = lax.optimization_barrier((grad_proj, result, dense_summed))
    dense_shards = []
    offset = 0
    for g in dense_grads:
        size = g[0].size
        dense_shards.append(dense_summed[0, offset : offset + size].reshape(g.shape[1:]))
        offset += size
    out_shard, fc1_shard, fc2_shard = dense_shards
    grad_qv_here = jnp.stack(
        [
            jnp.sum(grad_q_low.astype(jnp.float32), axis=0),
            jnp.sum(grad_v_low.astype(jnp.float32), axis=0),
        ],
        axis=0,
    )
    grad_qv_bias = lax.dynamic_update_slice_in_dim(
        jnp.zeros(qv_bias.shape, jnp.float32), grad_qv_here, tp_rank * cols_here, 1
    )
    grad_qkv_w = jnp.einsum(
        "rd,rkc->kdc", normed_all, grad_proj, preferred_element_type=jnp.float32
    )
    grad_proj_rows = lax.all_to_all(grad_proj, "tp", 0, 2, tiled=True)
    grad_proj_rows, qkv_all = lax.optimization_barrier((grad_proj_rows, qkv_all))
    grad_normed = jnp.einsum(
        "rkc,kdc->rd", grad_proj_rows, qkv_all, preferred_element_type=jnp.float32
    )
    grad_in_norm, grad_ln1_gain, grad_ln1_bias = norm_backward(
        grad_normed, unit_one, inv_one, ln1_gain
    )
    grad_input = grad_middle + grad_in_norm
    grad_table = lax.dot_general(
        one_hot,
        grad_input,
        (((0,), (0,)), ((), ())),
        precision=HIGH,
        preferred_element_type=jnp.float32,
    )
    qkv_shard = lax.psum_scatter(grad_qkv_w, "fsdp", scatter_dimension=1, tiled=True)
    summed = lax.psum(
        (
            grad_ln1_gain,
            grad_ln1_bias,
            grad_qv_bias,
            grad_out_bias,
            grad_ln2_gain,
            grad_ln2_bias,
            grad_fc1_bias,
            grad_fc2_bias,
            grad_table,
        ),
        ("fsdp", "tp"),
    )
    return (
        result.astype(jnp.bfloat16),
        grad_input,
        qkv_shard,
        out_shard,
        fc1_shard,
        fc2_shard,
        summed[0],
        summed[1],
        summed[2],
        summed[3],
        summed[4],
        summed[5],
        summed[6],
        summed[7],
        summed[8],
    )


def solution(mesh):
    placed = (
        P(("fsdp", "tp"), None),
        P(("fsdp", "tp")),
        P("fsdp"),
        P(("fsdp", "tp"), None),
        P(None, "fsdp", "tp"),
        P("tp", "fsdp"),
        P("fsdp", "tp"),
        P("tp", "fsdp"),
        P(),
        P(),
        P(),
        P(),
        P(),
        P(),
        P(),
        P(),
        P(),
    )
    return jax.shard_map(
        on_device,
        mesh=mesh,
        in_specs=placed,
        out_specs=(
            P(("fsdp", "tp"), None),
            P(("fsdp", "tp"), None),
            P(None, "fsdp", "tp"),
            P("tp", "fsdp"),
            P("fsdp", "tp"),
            P("tp", "fsdp"),
            P(),
            P(),
            P(),
            P(),
            P(),
            P(),
            P(),
            P(),
            P(),
        ),
        check_vma=False,
    )
```

```python
from functools import partial

import jax
import jax.numpy as jnp
from jax import lax
from jax.sharding import PartitionSpec as P

HD = 64
NPASS = 5
QBLOCK = 512


HIGH = lax.Precision.HIGHEST
EPS = 1e-05
NEG_FILL = -1e30


def norm_forward(rows_in, gain, shift):
    center = rows_in - jnp.mean(rows_in, axis=-1, keepdims=True)
    scale_inv = lax.rsqrt(jnp.mean(center * center, axis=-1, keepdims=True) + EPS)
    unit_rows = center * scale_inv
    return (unit_rows * gain + shift, unit_rows, scale_inv)


def norm_backward(grad_out, unit_rows, scale_inv, gain):
    grad_unit = grad_out * gain
    first_mean = jnp.mean(grad_unit, axis=-1, keepdims=True)
    second_mean = jnp.mean(grad_unit * unit_rows, axis=-1, keepdims=True)
    grad_rows = scale_inv * (grad_unit - first_mean - unit_rows * second_mean)
    return (grad_rows, jnp.sum(grad_out * unit_rows, axis=0), jnp.sum(grad_out, axis=0))


def matmul_nt(left, right):
    return lax.dot_general(
        left, right, (((1,), (1,)), ((), ())), preferred_element_type=jnp.float32
    )


def matmul_tn(left, right):
    return lax.dot_general(
        left, right, (((0,), (0,)), ((), ())), preferred_element_type=jnp.float32
    )


def block_scores(query_block, keys_all, row_start, prefix_len, scale):
    raw = (
        jnp.einsum("qhe,khe->hqk", query_block, keys_all, preferred_element_type=jnp.float32)
        * scale
    )
    row_ids = row_start + jnp.arange(query_block.shape[0], dtype=jnp.int32)
    col_ids = jnp.arange(keys_all.shape[0], dtype=jnp.int32)
    allowed = (col_ids[None, :] <= row_ids[:, None]) | (col_ids[None, :] < prefix_len)
    return jnp.where(allowed[None], raw, NEG_FILL)


def attend_forward(queries, keys_all, values_all, prefix_len, scale):
    seq_len, heads_here, head_size = queries.shape
    block_count = seq_len // QBLOCK
    query_blocks = queries.reshape(block_count, QBLOCK, heads_here, head_size)
    block_starts = jnp.arange(block_count, dtype=jnp.int32) * QBLOCK

    def one_block(item):
        query_block, row_start = item
        masked = block_scores(query_block, keys_all, row_start, prefix_len, scale)
        peak = jnp.max(masked, axis=-1, keepdims=True)
        expo = jnp.exp(masked - peak)
        total_mass = jnp.sum(expo, axis=-1, keepdims=True)
        probs_low = (expo / total_mass).astype(jnp.bfloat16)
        out_block = jnp.einsum(
            "hqk,khe->qhe", probs_low, values_all, preferred_element_type=jnp.float32
        )
        return (out_block.astype(jnp.bfloat16), (peak + jnp.log(total_mass))[..., 0])

    outputs, log_mass = lax.map(one_block, (query_blocks, block_starts))
    return (outputs.reshape(seq_len, heads_here * head_size), log_mass)


def attend_backward(queries, keys_all, values_all, grad_mixed, log_mass, prefix_len, scale):
    seq_len, heads_here, head_size = queries.shape
    block_count = seq_len // QBLOCK
    query_blocks = queries.reshape(block_count, QBLOCK, heads_here, head_size)
    grad_blocks = grad_mixed.reshape(block_count, QBLOCK, heads_here, head_size)
    block_starts = jnp.arange(block_count, dtype=jnp.int32) * QBLOCK

    def one_block(carry, item):
        grad_keys, grad_values = carry
        query_block, grad_block, block_mass, row_start = item
        masked = block_scores(query_block, keys_all, row_start, prefix_len, scale)
        probs = jnp.exp(masked - block_mass[..., None])
        probs_low = probs.astype(jnp.bfloat16)
        grad_values = grad_values + jnp.einsum(
            "hqk,qhe->khe", probs_low, grad_block, preferred_element_type=jnp.float32
        )
        grad_probs = jnp.einsum(
            "qhe,khe->hqk", grad_block, values_all, preferred_element_type=jnp.float32
        )
        inner_sum = jnp.sum(probs * grad_probs, axis=-1, keepdims=True)
        grad_scores = (probs * (grad_probs - inner_sum)).astype(jnp.bfloat16)
        grad_query = (
            jnp.einsum("hqk,khe->qhe", grad_scores, keys_all, preferred_element_type=jnp.float32)
            * scale
        )
        grad_keys = (
            grad_keys
            + jnp.einsum(
                "hqk,qhe->khe", grad_scores, query_block, preferred_element_type=jnp.float32
            )
            * scale
        )
        return ((grad_keys, grad_values), grad_query)

    zero_state = jnp.zeros(keys_all.shape, jnp.float32)
    (grad_keys, grad_values), grad_queries = lax.scan(
        one_block, (zero_state, zero_state), (query_blocks, grad_blocks, log_mass, block_starts)
    )
    return (grad_queries.reshape(seq_len, heads_here, head_size), grad_keys, grad_values)


def on_device(
    tokens,
    pass_ids,
    prefix,
    cotangent,
    qkv_weight,
    out_weight,
    fc1_weight,
    fc2_weight,
    ln1_gain,
    ln1_bias,
    qv_bias,
    out_bias,
    ln2_gain,
    ln2_bias,
    fc1_bias,
    fc2_bias,
    pass_table,
):
    tp_count = lax.axis_size("tp")
    tp_rank = lax.axis_index("tp")
    local_rows = tokens.shape[0]
    seq_len = local_rows * tp_count
    cols_here = qkv_weight.shape[2]
    heads_here = cols_here // HD
    scale = HD ** (-0.5)
    prefix_len = prefix[0]
    gelu_tanh = partial(jax.nn.gelu, approximate=True)
    fsdp_count = lax.axis_size("fsdp")
    qkv_cols = lax.all_gather(qkv_weight, "fsdp", axis=1, tiled=True)
    qkv_full = qkv_cols
    hidden_here = fc1_weight.shape[1]
    qv_here = lax.dynamic_slice_in_dim(qv_bias, tp_rank * cols_here, cols_here, 1)
    one_hot = (pass_ids[:, None] == jnp.arange(NPASS, dtype=jnp.int32)[None, :]).astype(jnp.float32)
    block_in = tokens.astype(jnp.float32) + jnp.dot(
        one_hot, pass_table, precision=HIGH, preferred_element_type=jnp.float32
    )
    normed, unit_one, inv_one = norm_forward(block_in, ln1_gain, ln1_bias)
    normed_all = lax.all_gather(normed.astype(jnp.bfloat16), "tp", axis=0, tiled=True)
    shards = (out_weight, fc1_weight, fc2_weight)
    packed = jnp.concatenate([piece.reshape(-1) for piece in shards])
    packed, qkv_cols, normed_all = lax.optimization_barrier((packed, qkv_cols, normed_all))
    qkv_full = qkv_cols
    gathered = lax.all_gather(packed, "fsdp", axis=0, tiled=False)
    pieces = []
    offset = 0
    for piece in shards:
        size = piece.size
        pieces.append(gathered[:, offset : offset + size].reshape((fsdp_count,) + piece.shape))
        offset += size
    out_heads = jnp.moveaxis(pieces[0], 0, 1).reshape(out_weight.shape[0], -1)
    fc1_part = pieces[1].reshape(-1, fc1_weight.shape[1])
    fc2_part = jnp.moveaxis(pieces[2], 0, 1).reshape(fc2_weight.shape[0], -1)
    out_all = lax.all_gather(out_heads, "tp", axis=0, tiled=True)
    qkv_all = lax.all_gather(qkv_cols, "tp", axis=2, tiled=True)
    out_full = out_heads
    grad_rows = lax.all_gather(cotangent, "tp", axis=0, tiled=True)
    projected = jnp.einsum("rd,kdc->krc", normed_all, qkv_full, preferred_element_type=jnp.float32)
    queries = (projected[0] + qv_here[0]).astype(jnp.bfloat16).reshape(seq_len, heads_here, HD)
    keys_all = projected[1].astype(jnp.bfloat16).reshape(seq_len, heads_here, HD)
    values_all = (projected[2] + qv_here[1]).astype(jnp.bfloat16).reshape(seq_len, heads_here, HD)
    mixed, log_mass = attend_forward(queries, keys_all, values_all, prefix_len, scale)
    mixed, grad_rows = lax.optimization_barrier((mixed, grad_rows))
    mixed_rows = lax.all_to_all(mixed, "tp", 0, 1, tiled=True)
    middle = block_in + jnp.dot(mixed_rows, out_all, preferred_element_type=jnp.float32) + out_bias
    normed_two, unit_two, inv_two = norm_forward(middle, ln2_gain, ln2_bias)
    normed_two = normed_two.astype(jnp.bfloat16)
    grad_top = cotangent.astype(jnp.float32)
    fc1_bias_here = lax.dynamic_slice_in_dim(fc1_bias, tp_rank * hidden_here, hidden_here, 0)
    normed_rows = lax.all_gather(normed_two, "tp", axis=0, tiled=True)
    before = jnp.dot(normed_rows, fc1_part, preferred_element_type=jnp.float32) + fc1_bias_here
    hidden = gelu_tanh(before).astype(jnp.bfloat16)
    fc2_partial = jnp.dot(hidden, fc2_part, preferred_element_type=jnp.float32).astype(jnp.bfloat16)
    grad_hidden = matmul_nt(grad_rows, fc2_part)
    grad_before = jax.vjp(gelu_tanh, before)[1](grad_hidden)[0].astype(jnp.bfloat16)
    grad_fc1_bias = lax.dynamic_update_slice_in_dim(
        jnp.zeros(fc1_bias.shape, jnp.float32),
        jnp.sum(grad_before.astype(jnp.float32), axis=0),
        tp_rank * hidden_here,
        0,
    )
    grad_fc1 = matmul_tn(normed_rows, grad_before)
    grad_fc2 = matmul_tn(hidden, grad_rows)
    grad_normed_two = lax.psum_scatter(
        matmul_nt(grad_before, fc1_part), "tp", scatter_dimension=0, tiled=True
    )
    grad_normed_two, fc2_partial, grad_fc1, grad_fc2 = lax.optimization_barrier(
        (grad_normed_two, fc2_partial, grad_fc1, grad_fc2)
    )
    grad_fc2_bias = jnp.sum(grad_top, axis=0)
    grad_from_norm, grad_ln2_gain, grad_ln2_bias = norm_backward(
        grad_normed_two, unit_two, inv_two, ln2_gain
    )
    grad_middle = grad_top + grad_from_norm
    grad_out_bias = jnp.sum(grad_middle, axis=0)
    grad_attn_rows = lax.all_gather(grad_middle.astype(jnp.bfloat16), "tp", axis=0, tiled=True)
    fc2_partial, grad_attn_rows = lax.optimization_barrier((fc2_partial, grad_attn_rows))
    result = (
        middle
        + lax.psum_scatter(fc2_partial, "tp", scatter_dimension=0, tiled=True).astype(jnp.float32)
        + fc2_bias
    )
    grad_out_w = matmul_tn(mixed, grad_attn_rows)
    fsdp_count = lax.axis_size("fsdp")
    dense_grads = (
        jnp.moveaxis(grad_out_w.reshape(grad_out_w.shape[0], fsdp_count, -1), 1, 0),
        grad_fc1.reshape(fsdp_count, -1, grad_fc1.shape[1]),
        jnp.moveaxis(grad_fc2.reshape(grad_fc2.shape[0], fsdp_count, -1), 1, 0),
    )
    dense_packed = jnp.concatenate([g.reshape(fsdp_count, -1) for g in dense_grads], axis=1)
    dense_summed = lax.psum_scatter(
        dense_packed.reshape(-1, grad_fc1.shape[1]), "fsdp", scatter_dimension=0, tiled=True
    ).reshape(1, -1)
    grad_mixed = (
        matmul_nt(grad_attn_rows, out_full).astype(jnp.bfloat16).reshape(seq_len, heads_here, HD)
    )
    grad_queries, grad_keys, grad_values = attend_backward(
        queries, keys_all, values_all, grad_mixed, log_mass, prefix_len, scale
    )
    grad_q_low = grad_queries.astype(jnp.bfloat16).reshape(seq_len, cols_here)
    grad_k_low = grad_keys.astype(jnp.bfloat16).reshape(seq_len, cols_here)
    grad_v_low = grad_values.astype(jnp.bfloat16).reshape(seq_len, cols_here)
    grad_proj = jnp.stack([grad_q_low, grad_k_low, grad_v_low], axis=1)
    grad_proj, result, dense_summed = lax.optimization_barrier((grad_proj, result, dense_summed))
    dense_shards = []
    offset = 0
    for g in dense_grads:
        size = g[0].size
        dense_shards.append(dense_summed[0, offset : offset + size].reshape(g.shape[1:]))
        offset += size
    out_shard, fc1_shard, fc2_shard = dense_shards
    grad_qv_here = jnp.stack(
        [
            jnp.sum(grad_q_low.astype(jnp.float32), axis=0),
            jnp.sum(grad_v_low.astype(jnp.float32), axis=0),
        ],
        axis=0,
    )
    grad_qv_bias = lax.dynamic_update_slice_in_dim(
        jnp.zeros(qv_bias.shape, jnp.float32), grad_qv_here, tp_rank * cols_here, 1
    )
    grad_qkv_w = jnp.einsum(
        "rd,rkc->kdc", normed_all, grad_proj, preferred_element_type=jnp.float32
    )
    grad_proj_rows = lax.all_to_all(grad_proj, "tp", 0, 2, tiled=True)
    grad_proj_rows, qkv_all = lax.optimization_barrier((grad_proj_rows, qkv_all))
    grad_normed = jnp.einsum(
        "rkc,kdc->rd", grad_proj_rows, qkv_all, preferred_element_type=jnp.float32
    )
    grad_in_norm, grad_ln1_gain, grad_ln1_bias = norm_backward(
        grad_normed, unit_one, inv_one, ln1_gain
    )
    grad_input = grad_middle + grad_in_norm
    grad_table = lax.dot_general(
        one_hot,
        grad_input,
        (((0,), (0,)), ((), ())),
        precision=HIGH,
        preferred_element_type=jnp.float32,
    )
    qkv_shard = lax.psum_scatter(grad_qkv_w, "fsdp", scatter_dimension=1, tiled=True)
    summed = lax.psum(
        (
            grad_ln1_gain,
            grad_ln1_bias,
            grad_qv_bias,
            grad_out_bias,
            grad_ln2_gain,
            grad_ln2_bias,
            grad_fc1_bias,
            grad_fc2_bias,
            grad_table,
        ),
        ("fsdp", "tp"),
    )
    return (
        result.astype(jnp.bfloat16),
        grad_input,
        qkv_shard,
        out_shard,
        fc1_shard,
        fc2_shard,
        summed[0],
        summed[1],
        summed[2],
        summed[3],
        summed[4],
        summed[5],
        summed[6],
        summed[7],
        summed[8],
    )


def solution(mesh):
    placed = (
        P(("fsdp", "tp"), None),
        P(("fsdp", "tp")),
        P("fsdp"),
        P(("fsdp", "tp"), None),
        P(None, "fsdp", "tp"),
        P("tp", "fsdp"),
        P("fsdp", "tp"),
        P("tp", "fsdp"),
        P(),
        P(),
        P(),
        P(),
        P(),
        P(),
        P(),
        P(),
        P(),
    )
    return jax.shard_map(
        on_device,
        mesh=mesh,
        in_specs=placed,
        out_specs=(
            P(("fsdp", "tp"), None),
            P(("fsdp", "tp"), None),
            P(None, "fsdp", "tp"),
            P("tp", "fsdp"),
            P("fsdp", "tp"),
            P("tp", "fsdp"),
            P(),
            P(),
            P(),
            P(),
            P(),
            P(),
            P(),
            P(),
            P(),
        ),
        check_vma=False,
    )
```

```python
from functools import partial

import jax
import jax.numpy as jnp
from jax import lax
from jax.sharding import PartitionSpec as P

HD = 64
NPASS = 5
QBLOCK = 512


HIGH = lax.Precision.HIGHEST
EPS = 1e-05
NEG_FILL = -1e30


def norm_forward(rows_in, gain, shift):
    center = rows_in - jnp.mean(rows_in, axis=-1, keepdims=True)
    scale_inv = lax.rsqrt(jnp.mean(center * center, axis=-1, keepdims=True) + EPS)
    unit_rows = center * scale_inv
    return (unit_rows * gain + shift, unit_rows, scale_inv)


def norm_backward(grad_out, unit_rows, scale_inv, gain):
    grad_unit = grad_out * gain
    first_mean = jnp.mean(grad_unit, axis=-1, keepdims=True)
    second_mean = jnp.mean(grad_unit * unit_rows, axis=-1, keepdims=True)
    grad_rows = scale_inv * (grad_unit - first_mean - unit_rows * second_mean)
    return (grad_rows, jnp.sum(grad_out * unit_rows, axis=0), jnp.sum(grad_out, axis=0))


def matmul_nt(left, right):
    return lax.dot_general(
        left, right, (((1,), (1,)), ((), ())), preferred_element_type=jnp.float32
    )


def matmul_tn(left, right):
    return lax.dot_general(
        left, right, (((0,), (0,)), ((), ())), preferred_element_type=jnp.float32
    )


def block_scores(query_block, keys_all, row_start, prefix_len, scale):
    raw = (
        jnp.einsum("qhe,khe->hqk", query_block, keys_all, preferred_element_type=jnp.float32)
        * scale
    )
    row_ids = row_start + jnp.arange(query_block.shape[0], dtype=jnp.int32)
    col_ids = jnp.arange(keys_all.shape[0], dtype=jnp.int32)
    allowed = (col_ids[None, :] <= row_ids[:, None]) | (col_ids[None, :] < prefix_len)
    return jnp.where(allowed[None], raw, NEG_FILL)


def attend_forward(queries, keys_all, values_all, prefix_len, scale):
    seq_len, heads_here, head_size = queries.shape
    block_count = seq_len // QBLOCK
    query_blocks = queries.reshape(block_count, QBLOCK, heads_here, head_size)
    block_starts = jnp.arange(block_count, dtype=jnp.int32) * QBLOCK

    def one_block(item):
        query_block, row_start = item
        masked = block_scores(query_block, keys_all, row_start, prefix_len, scale)
        peak = jnp.max(masked, axis=-1, keepdims=True)
        expo = jnp.exp(masked - peak)
        total_mass = jnp.sum(expo, axis=-1, keepdims=True)
        probs_low = (expo / total_mass).astype(jnp.bfloat16)
        out_block = jnp.einsum(
            "hqk,khe->qhe", probs_low, values_all, preferred_element_type=jnp.float32
        )
        return (out_block.astype(jnp.bfloat16), (peak + jnp.log(total_mass))[..., 0])

    outputs, log_mass = lax.map(one_block, (query_blocks, block_starts))
    return (outputs.reshape(seq_len, heads_here * head_size), log_mass)


def attend_backward(queries, keys_all, values_all, grad_mixed, log_mass, prefix_len, scale):
    seq_len, heads_here, head_size = queries.shape
    block_count = seq_len // QBLOCK
    query_blocks = queries.reshape(block_count, QBLOCK, heads_here, head_size)
    grad_blocks = grad_mixed.reshape(block_count, QBLOCK, heads_here, head_size)
    block_starts = jnp.arange(block_count, dtype=jnp.int32) * QBLOCK

    def one_block(carry, item):
        grad_keys, grad_values = carry
        query_block, grad_block, block_mass, row_start = item
        masked = block_scores(query_block, keys_all, row_start, prefix_len, scale)
        probs = jnp.exp(masked - block_mass[..., None])
        probs_low = probs.astype(jnp.bfloat16)
        grad_values = grad_values + jnp.einsum(
            "hqk,qhe->khe", probs_low, grad_block, preferred_element_type=jnp.float32
        )
        grad_probs = jnp.einsum(
            "qhe,khe->hqk", grad_block, values_all, preferred_element_type=jnp.float32
        )
        inner_sum = jnp.sum(probs * grad_probs, axis=-1, keepdims=True)
        grad_scores = (probs * (grad_probs - inner_sum)).astype(jnp.bfloat16)
        grad_query = (
            jnp.einsum("hqk,khe->qhe", grad_scores, keys_all, preferred_element_type=jnp.float32)
            * scale
        )
        grad_keys = (
            grad_keys
            + jnp.einsum(
                "hqk,qhe->khe", grad_scores, query_block, preferred_element_type=jnp.float32
            )
            * scale
        )
        return ((grad_keys, grad_values), grad_query)

    zero_state = jnp.zeros(keys_all.shape, jnp.float32)
    (grad_keys, grad_values), grad_queries = lax.scan(
        one_block, (zero_state, zero_state), (query_blocks, grad_blocks, log_mass, block_starts)
    )
    return (grad_queries.reshape(seq_len, heads_here, head_size), grad_keys, grad_values)


def on_device(
    tokens,
    pass_ids,
    prefix,
    cotangent,
    qkv_weight,
    out_weight,
    fc1_weight,
    fc2_weight,
    ln1_gain,
    ln1_bias,
    qv_bias,
    out_bias,
    ln2_gain,
    ln2_bias,
    fc1_bias,
    fc2_bias,
    pass_table,
):
    tp_count = lax.axis_size("tp")
    tp_rank = lax.axis_index("tp")
    local_rows = tokens.shape[0]
    seq_len = local_rows * tp_count
    cols_here = qkv_weight.shape[2]
    heads_here = cols_here // HD
    scale = HD ** (-0.5)
    prefix_len = prefix[0]
    gelu_tanh = partial(jax.nn.gelu, approximate=True)
    fsdp_count = lax.axis_size("fsdp")
    qkv_cols = lax.all_gather(qkv_weight, "fsdp", axis=1, tiled=True)
    qkv_full = qkv_cols
    hidden_here = fc1_weight.shape[1]
    qv_here = lax.dynamic_slice_in_dim(qv_bias, tp_rank * cols_here, cols_here, 1)
    one_hot = (pass_ids[:, None] == jnp.arange(NPASS, dtype=jnp.int32)[None, :]).astype(jnp.float32)
    block_in = tokens.astype(jnp.float32) + jnp.dot(
        one_hot, pass_table, precision=HIGH, preferred_element_type=jnp.float32
    )
    normed, unit_one, inv_one = norm_forward(block_in, ln1_gain, ln1_bias)
    normed_all = lax.all_gather(normed.astype(jnp.bfloat16), "tp", axis=0, tiled=True)
    out_pieces = lax.all_gather(out_weight, ("fsdp", "tp"), axis=0, tiled=False)
    out_pieces = out_pieces.reshape((fsdp_count, tp_count) + out_weight.shape)
    out_all = jnp.transpose(out_pieces, (1, 2, 0, 3)).reshape(
        tp_count * out_weight.shape[0], fsdp_count * out_weight.shape[1]
    )
    out_full = lax.dynamic_slice_in_dim(out_all, tp_rank * out_weight.shape[0], out_weight.shape[0], 0)
    shards = (fc1_weight, fc2_weight)
    packed = jnp.concatenate([piece.reshape(-1) for piece in shards])
    packed, qkv_cols, normed_all = lax.optimization_barrier((packed, qkv_cols, normed_all))
    qkv_full = qkv_cols
    gathered = lax.all_gather(packed, "fsdp", axis=0, tiled=False)
    qkv_all = lax.all_gather(qkv_cols, "tp", axis=2, tiled=True)
    grad_rows = lax.all_gather(cotangent, "tp", axis=0, tiled=True)
    projected = jnp.einsum("rd,kdc->krc", normed_all, qkv_full, preferred_element_type=jnp.float32)
    queries = (projected[0] + qv_here[0]).astype(jnp.bfloat16).reshape(seq_len, heads_here, HD)
    keys_all = projected[1].astype(jnp.bfloat16).reshape(seq_len, heads_here, HD)
    values_all = (projected[2] + qv_here[1]).astype(jnp.bfloat16).reshape(seq_len, heads_here, HD)
    mixed, log_mass = attend_forward(queries, keys_all, values_all, prefix_len, scale)
    mixed, grad_rows, gathered = lax.optimization_barrier((mixed, grad_rows, gathered))
    pieces = []
    offset = 0
    for piece in shards:
        size = piece.size
        pieces.append(gathered[:, offset : offset + size].reshape((fsdp_count,) + piece.shape))
        offset += size
    fc1_part = pieces[0].reshape(-1, fc1_weight.shape[1])
    fc2_part = jnp.moveaxis(pieces[1], 0, 1).reshape(fc2_weight.shape[0], -1)
    mixed_rows = lax.all_to_all(mixed, "tp", 0, 1, tiled=True)
    middle = block_in + jnp.dot(mixed_rows, out_all, preferred_element_type=jnp.float32) + out_bias
    normed_two, unit_two, inv_two = norm_forward(middle, ln2_gain, ln2_bias)
    normed_two = normed_two.astype(jnp.bfloat16)
    grad_top = cotangent.astype(jnp.float32)
    fc1_bias_here = lax.dynamic_slice_in_dim(fc1_bias, tp_rank * hidden_here, hidden_here, 0)
    normed_rows = lax.all_gather(normed_two, "tp", axis=0, tiled=True)
    before = jnp.dot(normed_rows, fc1_part, preferred_element_type=jnp.float32) + fc1_bias_here
    hidden = gelu_tanh(before).astype(jnp.bfloat16)
    fc2_partial = jnp.dot(hidden, fc2_part, preferred_element_type=jnp.float32).astype(jnp.bfloat16)
    grad_hidden = matmul_nt(grad_rows, fc2_part)
    grad_before = jax.vjp(gelu_tanh, before)[1](grad_hidden)[0].astype(jnp.bfloat16)
    grad_fc1_bias = lax.dynamic_update_slice_in_dim(
        jnp.zeros(fc1_bias.shape, jnp.float32),
        jnp.sum(grad_before.astype(jnp.float32), axis=0),
        tp_rank * hidden_here,
        0,
    )
    grad_fc1 = matmul_tn(normed_rows, grad_before)
    grad_fc2 = matmul_tn(hidden, grad_rows)
    grad_normed_two = lax.psum_scatter(
        matmul_nt(grad_before, fc1_part), "tp", scatter_dimension=0, tiled=True
    )
    grad_normed_two, fc2_partial, grad_fc1, grad_fc2 = lax.optimization_barrier(
        (grad_normed_two, fc2_partial, grad_fc1, grad_fc2)
    )
    grad_fc2_bias = jnp.sum(grad_top, axis=0)
    grad_from_norm, grad_ln2_gain, grad_ln2_bias = norm_backward(
        grad_normed_two, unit_two, inv_two, ln2_gain
    )
    grad_middle = grad_top + grad_from_norm
    grad_out_bias = jnp.sum(grad_middle, axis=0)
    grad_attn_rows = lax.all_gather(grad_middle.astype(jnp.bfloat16), "tp", axis=0, tiled=True)
    fc2_partial, grad_attn_rows = lax.optimization_barrier((fc2_partial, grad_attn_rows))
    result = (
        middle
        + lax.psum_scatter(fc2_partial, "tp", scatter_dimension=0, tiled=True).astype(jnp.float32)
        + fc2_bias
    )
    grad_out_w = matmul_tn(mixed, grad_attn_rows)
    fsdp_count = lax.axis_size("fsdp")
    dense_grads = (
        jnp.moveaxis(grad_out_w.reshape(grad_out_w.shape[0], fsdp_count, -1), 1, 0),
        grad_fc1.reshape(fsdp_count, -1, grad_fc1.shape[1]),
        jnp.moveaxis(grad_fc2.reshape(grad_fc2.shape[0], fsdp_count, -1), 1, 0),
    )
    dense_packed = jnp.concatenate([g.reshape(fsdp_count, -1) for g in dense_grads], axis=1)
    dense_summed = lax.psum_scatter(
        dense_packed.reshape(-1, grad_fc1.shape[1]), "fsdp", scatter_dimension=0, tiled=True
    ).reshape(1, -1)
    grad_mixed = (
        matmul_nt(grad_attn_rows, out_full).astype(jnp.bfloat16).reshape(seq_len, heads_here, HD)
    )
    grad_queries, grad_keys, grad_values = attend_backward(
        queries, keys_all, values_all, grad_mixed, log_mass, prefix_len, scale
    )
    grad_q_low = grad_queries.astype(jnp.bfloat16).reshape(seq_len, cols_here)
    grad_k_low = grad_keys.astype(jnp.bfloat16).reshape(seq_len, cols_here)
    grad_v_low = grad_values.astype(jnp.bfloat16).reshape(seq_len, cols_here)
    grad_proj = jnp.stack([grad_q_low, grad_k_low, grad_v_low], axis=1)
    grad_proj, result, dense_summed = lax.optimization_barrier((grad_proj, result, dense_summed))
    dense_shards = []
    offset = 0
    for g in dense_grads:
        size = g[0].size
        dense_shards.append(dense_summed[0, offset : offset + size].reshape(g.shape[1:]))
        offset += size
    out_shard, fc1_shard, fc2_shard = dense_shards
    grad_qv_here = jnp.stack(
        [
            jnp.sum(grad_q_low.astype(jnp.float32), axis=0),
            jnp.sum(grad_v_low.astype(jnp.float32), axis=0),
        ],
        axis=0,
    )
    grad_qv_bias = lax.dynamic_update_slice_in_dim(
        jnp.zeros(qv_bias.shape, jnp.float32), grad_qv_here, tp_rank * cols_here, 1
    )
    grad_qkv_w = jnp.einsum(
        "rd,rkc->kdc", normed_all, grad_proj, preferred_element_type=jnp.float32
    )
    grad_proj_rows = lax.all_to_all(grad_proj, "tp", 0, 2, tiled=True)
    grad_proj_rows, qkv_all = lax.optimization_barrier((grad_proj_rows, qkv_all))
    grad_normed = jnp.einsum(
        "rkc,kdc->rd", grad_proj_rows, qkv_all, preferred_element_type=jnp.float32
    )
    grad_in_norm, grad_ln1_gain, grad_ln1_bias = norm_backward(
        grad_normed, unit_one, inv_one, ln1_gain
    )
    grad_input = grad_middle + grad_in_norm
    grad_table = lax.dot_general(
        one_hot,
        grad_input,
        (((0,), (0,)), ((), ())),
        precision=HIGH,
        preferred_element_type=jnp.float32,
    )
    qkv_shard = lax.psum_scatter(grad_qkv_w, "fsdp", scatter_dimension=1, tiled=True)
    summed = lax.psum(
        (
            grad_ln1_gain,
            grad_ln1_bias,
            grad_qv_bias,
            grad_out_bias,
            grad_ln2_gain,
            grad_ln2_bias,
            grad_fc1_bias,
            grad_fc2_bias,
            grad_table,
        ),
        ("fsdp", "tp"),
    )
    return (
        result.astype(jnp.bfloat16),
        grad_input,
        qkv_shard,
        out_shard,
        fc1_shard,
        fc2_shard,
        summed[0],
        summed[1],
        summed[2],
        summed[3],
        summed[4],
        summed[5],
        summed[6],
        summed[7],
        summed[8],
    )


def solution(mesh):
    placed = (
        P(("fsdp", "tp"), None),
        P(("fsdp", "tp")),
        P("fsdp"),
        P(("fsdp", "tp"), None),
        P(None, "fsdp", "tp"),
        P("tp", "fsdp"),
        P("fsdp", "tp"),
        P("tp", "fsdp"),
        P(),
        P(),
        P(),
        P(),
        P(),
        P(),
        P(),
        P(),
        P(),
    )
    return jax.shard_map(
        on_device,
        mesh=mesh,
        in_specs=placed,
        out_specs=(
            P(("fsdp", "tp"), None),
            P(("fsdp", "tp"), None),
            P(None, "fsdp", "tp"),
            P("tp", "fsdp"),
            P("fsdp", "tp"),
            P("tp", "fsdp"),
            P(),
            P(),
            P(),
            P(),
            P(),
            P(),
            P(),
            P(),
            P(),
        ),
        check_vma=False,
    )
```

```python
import functools
from functools import partial

import jax
import jax.numpy as jnp
from jax import lax
from jax.experimental import pallas as pl
from jax.experimental.pallas import tpu as pltpu
from jax.sharding import PartitionSpec as P

HD = 64
NPASS = 5
QBLOCK = 512


HIGH = lax.Precision.HIGHEST
EPS = 1e-05
NEG_FILL = -1e30


def norm_forward(rows_in, gain, shift):
    center = rows_in - jnp.mean(rows_in, axis=-1, keepdims=True)
    scale_inv = lax.rsqrt(jnp.mean(center * center, axis=-1, keepdims=True) + EPS)
    unit_rows = center * scale_inv
    return (unit_rows * gain + shift, unit_rows, scale_inv)


def norm_backward(grad_out, unit_rows, scale_inv, gain):
    grad_unit = grad_out * gain
    first_mean = jnp.mean(grad_unit, axis=-1, keepdims=True)
    second_mean = jnp.mean(grad_unit * unit_rows, axis=-1, keepdims=True)
    grad_rows = scale_inv * (grad_unit - first_mean - unit_rows * second_mean)
    return (grad_rows, jnp.sum(grad_out * unit_rows, axis=0), jnp.sum(grad_out, axis=0))


def matmul_nt(left, right):
    return lax.dot_general(
        left, right, (((1,), (1,)), ((), ())), preferred_element_type=jnp.float32
    )


def matmul_tn(left, right):
    return lax.dot_general(
        left, right, (((0,), (0,)), ((), ())), preferred_element_type=jnp.float32
    )


def block_scores(query_block, keys_all, row_start, prefix_len, scale):
    raw = (
        jnp.einsum("qhe,khe->hqk", query_block, keys_all, preferred_element_type=jnp.float32)
        * scale
    )
    row_ids = row_start + jnp.arange(query_block.shape[0], dtype=jnp.int32)
    col_ids = jnp.arange(keys_all.shape[0], dtype=jnp.int32)
    allowed = (col_ids[None, :] <= row_ids[:, None]) | (col_ids[None, :] < prefix_len)
    return jnp.where(allowed[None], raw, NEG_FILL)


ATT_QB = 256


def _mask(prefix_len, qb, rows, cols):
    row = qb * rows + lax.broadcasted_iota(jnp.int32, (rows, cols), 0)
    col = lax.broadcasted_iota(jnp.int32, (rows, cols), 1)
    return (col <= row) | (col < prefix_len)


def _nt(a, b):
    return lax.dot_general(a, b, (((1,), (1,)), ((), ())), preferred_element_type=jnp.float32)


def _tn(a, b):
    return lax.dot_general(a, b, (((0,), (0,)), ((), ())), preferred_element_type=jnp.float32)


def _fwd_kernel(scale, prefix_ref, q_ref, k_ref, v_ref, o_ref, lse_ref):
    qb = pl.program_id(1)
    q = q_ref[0]
    rows, cols = q.shape[0], k_ref.shape[1]
    scores = _nt(q, k_ref[0]) * scale
    scores = jnp.where(_mask(prefix_ref[0], qb, rows, cols), scores, NEG_FILL)
    peak = jnp.max(scores, axis=-1, keepdims=True)
    expo = jnp.exp(scores - peak)
    total = jnp.sum(expo, axis=-1, keepdims=True)
    probs_low = (expo / total).astype(jnp.bfloat16)
    out = jnp.dot(probs_low, v_ref[0], preferred_element_type=jnp.float32)
    o_ref[0] = out.astype(o_ref.dtype)
    lse_ref[0] = peak + jnp.log(total)


def _bwd_kernel(scale, prefix_ref, q_ref, k_ref, v_ref, do_ref, lse_ref,
                dq_ref, dk_ref, dv_ref, dk_acc, dv_acc):
    qb = pl.program_id(1)

    @pl.when(qb == 0)
    def _():
        dk_acc[...] = jnp.zeros_like(dk_acc)
        dv_acc[...] = jnp.zeros_like(dv_acc)

    q = q_ref[0]
    k = k_ref[0]
    grad_out = do_ref[0]
    rows, cols = q.shape[0], k.shape[0]
    scores = _nt(q, k) * scale
    scores = jnp.where(_mask(prefix_ref[0], qb, rows, cols), scores, NEG_FILL)
    probs = jnp.exp(scores - lse_ref[0])
    dv_acc[...] += _tn(probs.astype(jnp.bfloat16), grad_out)
    grad_probs = _nt(grad_out, v_ref[0])
    inner = jnp.sum(probs * grad_probs, axis=-1, keepdims=True)
    grad_scores = (probs * (grad_probs - inner)).astype(jnp.bfloat16)
    dq_ref[0] = (jnp.dot(grad_scores, k, preferred_element_type=jnp.float32) * scale).astype(dq_ref.dtype)
    dk_acc[...] += _tn(grad_scores, q)

    @pl.when(qb == pl.num_programs(1) - 1)
    def _():
        dk_ref[0] = (dk_acc[...] * scale).astype(dk_ref.dtype)
        dv_ref[0] = dv_acc[...].astype(dv_ref.dtype)


def attn_forward(prefix, q, k, v, scale):
    heads, seq, hd = q.shape
    qb = min(ATT_QB, seq)
    grid = (heads, seq // qb)
    q_spec = pl.BlockSpec((1, qb, hd), lambda h, i, p: (h, i, 0))
    kv_spec = pl.BlockSpec((1, seq, hd), lambda h, i, p: (h, 0, 0))
    lse_spec = pl.BlockSpec((1, qb, 1), lambda h, i, p: (h, i, 0))
    return pl.pallas_call(
        functools.partial(_fwd_kernel, scale),
        out_shape=(jax.ShapeDtypeStruct((heads, seq, hd), jnp.bfloat16),
                   jax.ShapeDtypeStruct((heads, seq, 1), jnp.float32)),
        grid_spec=pltpu.PrefetchScalarGridSpec(
            num_scalar_prefetch=1, grid=grid,
            in_specs=[q_spec, kv_spec, kv_spec],
            out_specs=[q_spec, lse_spec]),
        compiler_params=pltpu.CompilerParams(
            dimension_semantics=("arbitrary", "arbitrary"),
            vmem_limit_bytes=48 * 1024 * 1024),
        cost_estimate=pl.CostEstimate(
            flops=4 * heads * seq * seq * hd, transcendentals=heads * seq * seq,
            bytes_accessed=4 * heads * seq * hd * 2),
    )(prefix, q, k, v)


def attn_backward(prefix, q, k, v, grad_out, lse, scale):
    heads, seq, hd = q.shape
    qb = min(ATT_QB, seq)
    grid = (heads, seq // qb)
    q_spec = pl.BlockSpec((1, qb, hd), lambda h, i, p: (h, i, 0))
    kv_spec = pl.BlockSpec((1, seq, hd), lambda h, i, p: (h, 0, 0))
    lse_spec = pl.BlockSpec((1, qb, 1), lambda h, i, p: (h, i, 0))
    shape = jax.ShapeDtypeStruct((heads, seq, hd), jnp.bfloat16)
    return pl.pallas_call(
        functools.partial(_bwd_kernel, scale),
        out_shape=(shape, shape, shape),
        grid_spec=pltpu.PrefetchScalarGridSpec(
            num_scalar_prefetch=1, grid=grid,
            in_specs=[q_spec, kv_spec, kv_spec, q_spec, lse_spec],
            out_specs=[q_spec, kv_spec, kv_spec],
            scratch_shapes=[pltpu.VMEM((seq, hd), jnp.float32),
                            pltpu.VMEM((seq, hd), jnp.float32)]),
        compiler_params=pltpu.CompilerParams(
            dimension_semantics=("arbitrary", "arbitrary"),
            vmem_limit_bytes=48 * 1024 * 1024),
        cost_estimate=pl.CostEstimate(
            flops=10 * heads * seq * seq * hd, transcendentals=heads * seq * seq,
            bytes_accessed=8 * heads * seq * hd * 2),
    )(prefix, q, k, v, grad_out, lse)


def on_device(
    tokens,
    pass_ids,
    prefix,
    cotangent,
    qkv_weight,
    out_weight,
    fc1_weight,
    fc2_weight,
    ln1_gain,
    ln1_bias,
    qv_bias,
    out_bias,
    ln2_gain,
    ln2_bias,
    fc1_bias,
    fc2_bias,
    pass_table,
):
    tp_count = lax.axis_size("tp")
    tp_rank = lax.axis_index("tp")
    local_rows = tokens.shape[0]
    seq_len = local_rows * tp_count
    cols_here = qkv_weight.shape[2]
    heads_here = cols_here // HD
    scale = HD ** (-0.5)
    prefix_len = prefix[0]
    gelu_tanh = partial(jax.nn.gelu, approximate=True)
    fsdp_count = lax.axis_size("fsdp")
    qkv_cols = lax.all_gather(qkv_weight, "fsdp", axis=1, tiled=True)
    qkv_full = qkv_cols
    hidden_here = fc1_weight.shape[1]
    qv_here = lax.dynamic_slice_in_dim(qv_bias, tp_rank * cols_here, cols_here, 1)
    one_hot = (pass_ids[:, None] == jnp.arange(NPASS, dtype=jnp.int32)[None, :]).astype(jnp.float32)
    block_in = tokens.astype(jnp.float32) + jnp.dot(
        one_hot, pass_table, precision=HIGH, preferred_element_type=jnp.float32
    )
    normed, unit_one, inv_one = norm_forward(block_in, ln1_gain, ln1_bias)
    normed_all = lax.all_gather(normed.astype(jnp.bfloat16), "tp", axis=0, tiled=True)
    out_pieces = lax.all_gather(out_weight, ("fsdp", "tp"), axis=0, tiled=False)
    out_pieces = out_pieces.reshape((fsdp_count, tp_count) + out_weight.shape)
    out_all = jnp.transpose(out_pieces, (1, 2, 0, 3)).reshape(
        tp_count * out_weight.shape[0], fsdp_count * out_weight.shape[1]
    )
    out_full = lax.dynamic_slice_in_dim(out_all, tp_rank * out_weight.shape[0], out_weight.shape[0], 0)
    shards = (fc1_weight, fc2_weight)
    packed = jnp.concatenate([piece.reshape(-1) for piece in shards])
    packed, qkv_cols, normed_all = lax.optimization_barrier((packed, qkv_cols, normed_all))
    qkv_full = qkv_cols
    gathered = lax.all_gather(packed, "fsdp", axis=0, tiled=False)
    qkv_all = lax.all_gather(qkv_cols, "tp", axis=2, tiled=True)
    grad_rows = lax.all_gather(cotangent, "tp", axis=0, tiled=True)
    projected = jnp.einsum("rd,kdc->krc", normed_all, qkv_full, preferred_element_type=jnp.float32)
    queries = (projected[0] + qv_here[0]).astype(jnp.bfloat16).reshape(seq_len, heads_here, HD)
    keys_all = projected[1].astype(jnp.bfloat16).reshape(seq_len, heads_here, HD)
    values_all = (projected[2] + qv_here[1]).astype(jnp.bfloat16).reshape(seq_len, heads_here, HD)
    q_heads = jnp.transpose(queries, (1, 0, 2))
    k_heads = jnp.transpose(keys_all, (1, 0, 2))
    v_heads = jnp.transpose(values_all, (1, 0, 2))
    out_heads, log_mass = attn_forward(prefix, q_heads, k_heads, v_heads, scale)
    mixed = jnp.transpose(out_heads, (1, 0, 2)).reshape(seq_len, cols_here)
    mixed, grad_rows, gathered = lax.optimization_barrier((mixed, grad_rows, gathered))
    pieces = []
    offset = 0
    for piece in shards:
        size = piece.size
        pieces.append(gathered[:, offset : offset + size].reshape((fsdp_count,) + piece.shape))
        offset += size
    fc1_part = pieces[0].reshape(-1, fc1_weight.shape[1])
    fc2_part = jnp.moveaxis(pieces[1], 0, 1).reshape(fc2_weight.shape[0], -1)
    mixed_rows = lax.all_to_all(mixed, "tp", 0, 1, tiled=True)
    middle = block_in + jnp.dot(mixed_rows, out_all, preferred_element_type=jnp.float32) + out_bias
    normed_two, unit_two, inv_two = norm_forward(middle, ln2_gain, ln2_bias)
    normed_two = normed_two.astype(jnp.bfloat16)
    grad_top = cotangent.astype(jnp.float32)
    fc1_bias_here = lax.dynamic_slice_in_dim(fc1_bias, tp_rank * hidden_here, hidden_here, 0)
    normed_rows = lax.all_gather(normed_two, "tp", axis=0, tiled=True)
    before = jnp.dot(normed_rows, fc1_part, preferred_element_type=jnp.float32) + fc1_bias_here
    hidden = gelu_tanh(before).astype(jnp.bfloat16)
    fc2_partial = jnp.dot(hidden, fc2_part, preferred_element_type=jnp.float32).astype(jnp.bfloat16)
    grad_hidden = matmul_nt(grad_rows, fc2_part)
    grad_before = jax.vjp(gelu_tanh, before)[1](grad_hidden)[0].astype(jnp.bfloat16)
    grad_fc1_bias = lax.dynamic_update_slice_in_dim(
        jnp.zeros(fc1_bias.shape, jnp.float32),
        jnp.sum(grad_before.astype(jnp.float32), axis=0),
        tp_rank * hidden_here,
        0,
    )
    grad_fc1 = matmul_tn(normed_rows, grad_before)
    grad_fc2 = matmul_tn(hidden, grad_rows)
    grad_normed_two = lax.psum_scatter(
        matmul_nt(grad_before, fc1_part), "tp", scatter_dimension=0, tiled=True
    )
    grad_normed_two, fc2_partial, grad_fc1, grad_fc2 = lax.optimization_barrier(
        (grad_normed_two, fc2_partial, grad_fc1, grad_fc2)
    )
    grad_fc2_bias = jnp.sum(grad_top, axis=0)
    grad_from_norm, grad_ln2_gain, grad_ln2_bias = norm_backward(
        grad_normed_two, unit_two, inv_two, ln2_gain
    )
    grad_middle = grad_top + grad_from_norm
    grad_out_bias = jnp.sum(grad_middle, axis=0)
    grad_attn_rows = lax.all_gather(grad_middle.astype(jnp.bfloat16), "tp", axis=0, tiled=True)
    fc2_partial, grad_attn_rows = lax.optimization_barrier((fc2_partial, grad_attn_rows))
    result = (
        middle
        + lax.psum_scatter(fc2_partial, "tp", scatter_dimension=0, tiled=True).astype(jnp.float32)
        + fc2_bias
    )
    grad_out_w = matmul_tn(mixed, grad_attn_rows)
    fsdp_count = lax.axis_size("fsdp")
    dense_grads = (
        jnp.moveaxis(grad_out_w.reshape(grad_out_w.shape[0], fsdp_count, -1), 1, 0),
        grad_fc1.reshape(fsdp_count, -1, grad_fc1.shape[1]),
        jnp.moveaxis(grad_fc2.reshape(grad_fc2.shape[0], fsdp_count, -1), 1, 0),
    )
    dense_packed = jnp.concatenate([g.reshape(fsdp_count, -1) for g in dense_grads], axis=1)
    dense_summed = lax.psum_scatter(
        dense_packed.reshape(-1, grad_fc1.shape[1]), "fsdp", scatter_dimension=0, tiled=True
    ).reshape(1, -1)
    grad_mixed = (
        matmul_nt(grad_attn_rows, out_full).astype(jnp.bfloat16).reshape(seq_len, heads_here, HD)
    )
    grad_q_heads, grad_k_heads, grad_v_heads = attn_backward(
        prefix, q_heads, k_heads, v_heads, jnp.transpose(grad_mixed, (1, 0, 2)), log_mass, scale
    )
    grad_q_low = jnp.transpose(grad_q_heads, (1, 0, 2)).reshape(seq_len, cols_here)
    grad_k_low = jnp.transpose(grad_k_heads, (1, 0, 2)).reshape(seq_len, cols_here)
    grad_v_low = jnp.transpose(grad_v_heads, (1, 0, 2)).reshape(seq_len, cols_here)
    grad_proj = jnp.stack([grad_q_low, grad_k_low, grad_v_low], axis=1)
    grad_proj, result, dense_summed = lax.optimization_barrier((grad_proj, result, dense_summed))
    dense_shards = []
    offset = 0
    for g in dense_grads:
        size = g[0].size
        dense_shards.append(dense_summed[0, offset : offset + size].reshape(g.shape[1:]))
        offset += size
    out_shard, fc1_shard, fc2_shard = dense_shards
    grad_qv_here = jnp.stack(
        [
            jnp.sum(grad_q_low.astype(jnp.float32), axis=0),
            jnp.sum(grad_v_low.astype(jnp.float32), axis=0),
        ],
        axis=0,
    )
    grad_qv_bias = lax.dynamic_update_slice_in_dim(
        jnp.zeros(qv_bias.shape, jnp.float32), grad_qv_here, tp_rank * cols_here, 1
    )
    grad_qkv_w = jnp.einsum(
        "rd,rkc->kdc", normed_all, grad_proj, preferred_element_type=jnp.float32
    )
    grad_proj_rows = lax.all_to_all(grad_proj, "tp", 0, 2, tiled=True)
    grad_proj_rows, qkv_all = lax.optimization_barrier((grad_proj_rows, qkv_all))
    grad_normed = jnp.einsum(
        "rkc,kdc->rd", grad_proj_rows, qkv_all, preferred_element_type=jnp.float32
    )
    grad_in_norm, grad_ln1_gain, grad_ln1_bias = norm_backward(
        grad_normed, unit_one, inv_one, ln1_gain
    )
    grad_input = grad_middle + grad_in_norm
    grad_table = lax.dot_general(
        one_hot,
        grad_input,
        (((0,), (0,)), ((), ())),
        precision=HIGH,
        preferred_element_type=jnp.float32,
    )
    qkv_shard = lax.psum_scatter(grad_qkv_w, "fsdp", scatter_dimension=1, tiled=True)
    summed = lax.psum(
        (
            grad_ln1_gain,
            grad_ln1_bias,
            grad_qv_bias,
            grad_out_bias,
            grad_ln2_gain,
            grad_ln2_bias,
            grad_fc1_bias,
            grad_fc2_bias,
            grad_table,
        ),
        ("fsdp", "tp"),
    )
    return (
        result.astype(jnp.bfloat16),
        grad_input,
        qkv_shard,
        out_shard,
        fc1_shard,
        fc2_shard,
        summed[0],
        summed[1],
        summed[2],
        summed[3],
        summed[4],
        summed[5],
        summed[6],
        summed[7],
        summed[8],
    )


def solution(mesh):
    placed = (
        P(("fsdp", "tp"), None),
        P(("fsdp", "tp")),
        P("fsdp"),
        P(("fsdp", "tp"), None),
        P(None, "fsdp", "tp"),
        P("tp", "fsdp"),
        P("fsdp", "tp"),
        P("tp", "fsdp"),
        P(),
        P(),
        P(),
        P(),
        P(),
        P(),
        P(),
        P(),
        P(),
    )
    return jax.shard_map(
        on_device,
        mesh=mesh,
        in_specs=placed,
        out_specs=(
            P(("fsdp", "tp"), None),
            P(("fsdp", "tp"), None),
            P(None, "fsdp", "tp"),
            P("tp", "fsdp"),
            P("fsdp", "tp"),
            P("tp", "fsdp"),
            P(),
            P(),
            P(),
            P(),
            P(),
            P(),
            P(),
            P(),
            P(),
        ),
        check_vma=False,
    )
```

```python
import functools
from functools import partial

import jax
import jax.numpy as jnp
from jax import lax
from jax.experimental import pallas as pl
from jax.experimental.pallas import tpu as pltpu
from jax.sharding import PartitionSpec as P

HD = 64
NPASS = 5
QBLOCK = 512


HIGH = lax.Precision.HIGHEST
EPS = 1e-05
NEG_FILL = -1e30


def norm_forward(rows_in, gain, shift):
    center = rows_in - jnp.mean(rows_in, axis=-1, keepdims=True)
    scale_inv = lax.rsqrt(jnp.mean(center * center, axis=-1, keepdims=True) + EPS)
    unit_rows = center * scale_inv
    return (unit_rows * gain + shift, unit_rows, scale_inv)


def norm_backward(grad_out, unit_rows, scale_inv, gain):
    grad_unit = grad_out * gain
    first_mean = jnp.mean(grad_unit, axis=-1, keepdims=True)
    second_mean = jnp.mean(grad_unit * unit_rows, axis=-1, keepdims=True)
    grad_rows = scale_inv * (grad_unit - first_mean - unit_rows * second_mean)
    return (grad_rows, jnp.sum(grad_out * unit_rows, axis=0), jnp.sum(grad_out, axis=0))


def matmul_nt(left, right):
    return lax.dot_general(
        left, right, (((1,), (1,)), ((), ())), preferred_element_type=jnp.float32
    )


def matmul_tn(left, right):
    return lax.dot_general(
        left, right, (((0,), (0,)), ((), ())), preferred_element_type=jnp.float32
    )


def block_scores(query_block, keys_all, row_start, prefix_len, scale):
    raw = (
        jnp.einsum("qhe,khe->hqk", query_block, keys_all, preferred_element_type=jnp.float32)
        * scale
    )
    row_ids = row_start + jnp.arange(query_block.shape[0], dtype=jnp.int32)
    col_ids = jnp.arange(keys_all.shape[0], dtype=jnp.int32)
    allowed = (col_ids[None, :] <= row_ids[:, None]) | (col_ids[None, :] < prefix_len)
    return jnp.where(allowed[None], raw, NEG_FILL)


ATT_QB = 256


def _mask(prefix_len, qb, rows, cols):
    row = qb * rows + lax.broadcasted_iota(jnp.int32, (rows, cols), 0)
    col = lax.broadcasted_iota(jnp.int32, (rows, cols), 1)
    return (col <= row) | (col < prefix_len)


def _nt(a, b):
    return lax.dot_general(a, b, (((1,), (1,)), ((), ())), preferred_element_type=jnp.float32)


def _tn(a, b):
    return lax.dot_general(a, b, (((0,), (0,)), ((), ())), preferred_element_type=jnp.float32)


def _fwd_kernel(scale, prefix_ref, q_ref, k_ref, v_ref, o_ref, lse_ref):
    qb = pl.program_id(1)
    q = q_ref[0]
    rows, cols = q.shape[0], k_ref.shape[1]
    scores = _nt(q, k_ref[0]) * scale
    scores = jnp.where(_mask(prefix_ref[0], qb, rows, cols), scores, NEG_FILL)
    peak = jnp.max(scores, axis=-1, keepdims=True)
    expo = jnp.exp(scores - peak)
    total = jnp.sum(expo, axis=-1, keepdims=True)
    probs_low = (expo / total).astype(jnp.bfloat16)
    out = jnp.dot(probs_low, v_ref[0], preferred_element_type=jnp.float32)
    o_ref[0] = out.astype(o_ref.dtype)
    lse_ref[0] = peak + jnp.log(total)


def _bwd_kernel(scale, prefix_ref, q_ref, k_ref, v_ref, do_ref, lse_ref,
                dq_ref, dk_ref, dv_ref, dk_acc, dv_acc):
    qb = pl.program_id(1)

    @pl.when(qb == 0)
    def _():
        dk_acc[...] = jnp.zeros_like(dk_acc)
        dv_acc[...] = jnp.zeros_like(dv_acc)

    q = q_ref[0]
    k = k_ref[0]
    grad_out = do_ref[0]
    rows, cols = q.shape[0], k.shape[0]
    scores = _nt(q, k) * scale
    scores = jnp.where(_mask(prefix_ref[0], qb, rows, cols), scores, NEG_FILL)
    probs = jnp.exp(scores - lse_ref[0])
    dv_acc[...] += _tn(probs.astype(jnp.bfloat16), grad_out)
    grad_probs = _nt(grad_out, v_ref[0])
    inner = jnp.sum(probs * grad_probs, axis=-1, keepdims=True)
    grad_scores = (probs * (grad_probs - inner)).astype(jnp.bfloat16)
    dq_ref[0] = (jnp.dot(grad_scores, k, preferred_element_type=jnp.float32) * scale).astype(dq_ref.dtype)
    dk_acc[...] += _tn(grad_scores, q)

    @pl.when(qb == pl.num_programs(1) - 1)
    def _():
        dk_ref[0] = (dk_acc[...] * scale).astype(dk_ref.dtype)
        dv_ref[0] = dv_acc[...].astype(dv_ref.dtype)


def attn_forward(prefix, q, k, v, scale):
    heads, seq, hd = q.shape
    qb = min(ATT_QB, seq)
    grid = (heads, seq // qb)
    q_spec = pl.BlockSpec((1, qb, hd), lambda h, i, p: (h, i, 0))
    kv_spec = pl.BlockSpec((1, seq, hd), lambda h, i, p: (h, 0, 0))
    lse_spec = pl.BlockSpec((1, qb, 1), lambda h, i, p: (h, i, 0))
    return pl.pallas_call(
        functools.partial(_fwd_kernel, scale),
        out_shape=(jax.ShapeDtypeStruct((heads, seq, hd), jnp.bfloat16),
                   jax.ShapeDtypeStruct((heads, seq, 1), jnp.float32)),
        grid_spec=pltpu.PrefetchScalarGridSpec(
            num_scalar_prefetch=1, grid=grid,
            in_specs=[q_spec, kv_spec, kv_spec],
            out_specs=[q_spec, lse_spec]),
        compiler_params=pltpu.CompilerParams(
            dimension_semantics=("arbitrary", "arbitrary"),
            vmem_limit_bytes=48 * 1024 * 1024),
        cost_estimate=pl.CostEstimate(
            flops=4 * heads * seq * seq * hd, transcendentals=heads * seq * seq,
            bytes_accessed=4 * heads * seq * hd * 2),
    )(prefix, q, k, v)


def attn_backward(prefix, q, k, v, grad_out, lse, scale):
    heads, seq, hd = q.shape
    qb = min(ATT_QB, seq)
    grid = (heads, seq // qb)
    q_spec = pl.BlockSpec((1, qb, hd), lambda h, i, p: (h, i, 0))
    kv_spec = pl.BlockSpec((1, seq, hd), lambda h, i, p: (h, 0, 0))
    lse_spec = pl.BlockSpec((1, qb, 1), lambda h, i, p: (h, i, 0))
    shape = jax.ShapeDtypeStruct((heads, seq, hd), jnp.bfloat16)
    return pl.pallas_call(
        functools.partial(_bwd_kernel, scale),
        out_shape=(shape, shape, shape),
        grid_spec=pltpu.PrefetchScalarGridSpec(
            num_scalar_prefetch=1, grid=grid,
            in_specs=[q_spec, kv_spec, kv_spec, q_spec, lse_spec],
            out_specs=[q_spec, kv_spec, kv_spec],
            scratch_shapes=[pltpu.VMEM((seq, hd), jnp.float32),
                            pltpu.VMEM((seq, hd), jnp.float32)]),
        compiler_params=pltpu.CompilerParams(
            dimension_semantics=("arbitrary", "arbitrary"),
            vmem_limit_bytes=48 * 1024 * 1024),
        cost_estimate=pl.CostEstimate(
            flops=10 * heads * seq * seq * hd, transcendentals=heads * seq * seq,
            bytes_accessed=8 * heads * seq * hd * 2),
    )(prefix, q, k, v, grad_out, lse)


def on_device(
    tokens,
    pass_ids,
    prefix,
    cotangent,
    qkv_weight,
    out_weight,
    fc1_weight,
    fc2_weight,
    ln1_gain,
    ln1_bias,
    qv_bias,
    out_bias,
    ln2_gain,
    ln2_bias,
    fc1_bias,
    fc2_bias,
    pass_table,
):
    tp_count = lax.axis_size("tp")
    tp_rank = lax.axis_index("tp")
    local_rows = tokens.shape[0]
    seq_len = local_rows * tp_count
    cols_here = qkv_weight.shape[2]
    heads_here = cols_here // HD
    scale = HD ** (-0.5)
    prefix_len = prefix[0]
    gelu_tanh = partial(jax.nn.gelu, approximate=True)
    fsdp_count = lax.axis_size("fsdp")
    qkv_cols = lax.all_gather(qkv_weight, "fsdp", axis=1, tiled=True)
    qkv_full = qkv_cols
    hidden_here = fc1_weight.shape[1]
    qv_here = lax.dynamic_slice_in_dim(qv_bias, tp_rank * cols_here, cols_here, 1)
    one_hot = (pass_ids[:, None] == jnp.arange(NPASS, dtype=jnp.int32)[None, :]).astype(jnp.float32)
    block_in = tokens.astype(jnp.float32) + jnp.dot(
        one_hot, pass_table, precision=HIGH, preferred_element_type=jnp.float32
    )
    normed, unit_one, inv_one = norm_forward(block_in, ln1_gain, ln1_bias)
    normed_all = lax.all_gather(normed.astype(jnp.bfloat16), "tp", axis=0, tiled=True)
    shards = (out_weight, fc1_weight, fc2_weight)
    packed = jnp.concatenate([piece.reshape(-1) for piece in shards])
    packed, qkv_cols, normed_all = lax.optimization_barrier((packed, qkv_cols, normed_all))
    qkv_full = qkv_cols
    gathered = lax.all_gather(packed, "fsdp", axis=0, tiled=False)
    qkv_all = lax.all_gather(qkv_cols, "tp", axis=2, tiled=True)
    grad_rows = lax.all_gather(cotangent, "tp", axis=0, tiled=True)
    projected = jnp.einsum("rd,kdc->krc", normed_all, qkv_full, preferred_element_type=jnp.float32)
    queries = (projected[0] + qv_here[0]).astype(jnp.bfloat16).reshape(seq_len, heads_here, HD)
    keys_all = projected[1].astype(jnp.bfloat16).reshape(seq_len, heads_here, HD)
    values_all = (projected[2] + qv_here[1]).astype(jnp.bfloat16).reshape(seq_len, heads_here, HD)
    q_heads = jnp.transpose(queries, (1, 0, 2))
    k_heads = jnp.transpose(keys_all, (1, 0, 2))
    v_heads = jnp.transpose(values_all, (1, 0, 2))
    out_heads, log_mass = attn_forward(prefix, q_heads, k_heads, v_heads, scale)
    mixed = jnp.transpose(out_heads, (1, 0, 2)).reshape(seq_len, cols_here)
    pieces = []
    offset = 0
    for piece in shards:
        size = piece.size
        pieces.append(gathered[:, offset : offset + size].reshape((fsdp_count,) + piece.shape))
        offset += size
    out_full = jnp.moveaxis(pieces[0], 0, 1).reshape(out_weight.shape[0], -1)
    fc1_part = pieces[1].reshape(-1, fc1_weight.shape[1])
    fc2_part = jnp.moveaxis(pieces[2], 0, 1).reshape(fc2_weight.shape[0], -1)
    out_all = lax.all_gather(out_full, "tp", axis=0, tiled=True)
    mixed, grad_rows, out_all, fc1_part, fc2_part = lax.optimization_barrier(
        (mixed, grad_rows, out_all, fc1_part, fc2_part)
    )
    mixed_rows = lax.all_to_all(mixed, "tp", 0, 1, tiled=True)
    middle = block_in + jnp.dot(mixed_rows, out_all, preferred_element_type=jnp.float32) + out_bias
    normed_two, unit_two, inv_two = norm_forward(middle, ln2_gain, ln2_bias)
    normed_two = normed_two.astype(jnp.bfloat16)
    grad_top = cotangent.astype(jnp.float32)
    fc1_bias_here = lax.dynamic_slice_in_dim(fc1_bias, tp_rank * hidden_here, hidden_here, 0)
    normed_rows = lax.all_gather(normed_two, "tp", axis=0, tiled=True)
    before = jnp.dot(normed_rows, fc1_part, preferred_element_type=jnp.float32) + fc1_bias_here
    hidden = gelu_tanh(before).astype(jnp.bfloat16)
    fc2_partial = jnp.dot(hidden, fc2_part, preferred_element_type=jnp.float32).astype(jnp.bfloat16)
    grad_hidden = matmul_nt(grad_rows, fc2_part)
    grad_before = jax.vjp(gelu_tanh, before)[1](grad_hidden)[0].astype(jnp.bfloat16)
    grad_fc1_bias = lax.dynamic_update_slice_in_dim(
        jnp.zeros(fc1_bias.shape, jnp.float32),
        jnp.sum(grad_before.astype(jnp.float32), axis=0),
        tp_rank * hidden_here,
        0,
    )
    grad_fc1 = matmul_tn(normed_rows, grad_before)
    grad_fc2 = matmul_tn(hidden, grad_rows)
    grad_normed_two = lax.psum_scatter(
        matmul_nt(grad_before, fc1_part), "tp", scatter_dimension=0, tiled=True
    )
    grad_normed_two, fc2_partial, grad_fc1, grad_fc2 = lax.optimization_barrier(
        (grad_normed_two, fc2_partial, grad_fc1, grad_fc2)
    )
    grad_fc2_bias = jnp.sum(grad_top, axis=0)
    grad_from_norm, grad_ln2_gain, grad_ln2_bias = norm_backward(
        grad_normed_two, unit_two, inv_two, ln2_gain
    )
    grad_middle = grad_top + grad_from_norm
    grad_out_bias = jnp.sum(grad_middle, axis=0)
    grad_attn_rows = lax.all_gather(grad_middle.astype(jnp.bfloat16), "tp", axis=0, tiled=True)
    fc2_partial, grad_attn_rows = lax.optimization_barrier((fc2_partial, grad_attn_rows))
    fc2_parts = lax.all_to_all(
        fc2_partial.reshape(tp_count, local_rows, -1), "tp", 0, 0, tiled=True
    )
    result = middle + jnp.sum(fc2_parts.astype(jnp.float32), axis=0) + fc2_bias
    grad_out_w = matmul_tn(mixed, grad_attn_rows)
    fsdp_count = lax.axis_size("fsdp")
    dense_grads = (
        jnp.moveaxis(grad_out_w.reshape(grad_out_w.shape[0], fsdp_count, -1), 1, 0),
        grad_fc1.reshape(fsdp_count, -1, grad_fc1.shape[1]),
        jnp.moveaxis(grad_fc2.reshape(grad_fc2.shape[0], fsdp_count, -1), 1, 0),
    )
    dense_packed = jnp.concatenate([g.reshape(fsdp_count, -1) for g in dense_grads], axis=1)
    dense_summed = lax.psum_scatter(
        dense_packed.reshape(-1, grad_fc1.shape[1]), "fsdp", scatter_dimension=0, tiled=True
    ).reshape(1, -1)
    grad_mixed = (
        matmul_nt(grad_attn_rows, out_full).astype(jnp.bfloat16).reshape(seq_len, heads_here, HD)
    )
    grad_q_heads, grad_k_heads, grad_v_heads = attn_backward(
        prefix, q_heads, k_heads, v_heads, jnp.transpose(grad_mixed, (1, 0, 2)), log_mass, scale
    )
    grad_proj = jnp.stack([grad_q_heads, grad_k_heads, grad_v_heads], axis=0)
    grad_proj, result, dense_summed = lax.optimization_barrier((grad_proj, result, dense_summed))
    dense_shards = []
    offset = 0
    for g in dense_grads:
        size = g[0].size
        dense_shards.append(dense_summed[0, offset : offset + size].reshape(g.shape[1:]))
        offset += size
    out_shard, fc1_shard, fc2_shard = dense_shards
    grad_qv_here = jnp.stack(
        [
            jnp.sum(grad_q_heads.astype(jnp.float32), axis=1).reshape(-1),
            jnp.sum(grad_v_heads.astype(jnp.float32), axis=1).reshape(-1),
        ],
        axis=0,
    )
    grad_qv_bias = lax.dynamic_update_slice_in_dim(
        jnp.zeros(qv_bias.shape, jnp.float32), grad_qv_here, tp_rank * cols_here, 1
    )
    grad_qkv_w = jnp.einsum(
        "rd,khre->kdhe", normed_all, grad_proj, preferred_element_type=jnp.float32
    ).reshape(3, normed_all.shape[1], cols_here)
    grad_proj_rows = lax.all_to_all(grad_proj, "tp", 2, 1, tiled=True)
    grad_proj_rows, qkv_all = lax.optimization_barrier((grad_proj_rows, qkv_all))
    grad_normed = jnp.einsum(
        "khre,kdhe->rd",
        grad_proj_rows,
        qkv_all.reshape(3, qkv_all.shape[1], -1, HD),
        preferred_element_type=jnp.float32,
    )
    grad_in_norm, grad_ln1_gain, grad_ln1_bias = norm_backward(
        grad_normed, unit_one, inv_one, ln1_gain
    )
    grad_input = grad_middle + grad_in_norm
    grad_table = lax.dot_general(
        one_hot,
        grad_input,
        (((0,), (0,)), ((), ())),
        precision=HIGH,
        preferred_element_type=jnp.float32,
    )
    qkv_shard = lax.psum_scatter(grad_qkv_w, "fsdp", scatter_dimension=1, tiled=True)
    summed = lax.psum(
        (
            grad_ln1_gain,
            grad_ln1_bias,
            grad_qv_bias,
            grad_out_bias,
            grad_ln2_gain,
            grad_ln2_bias,
            grad_fc1_bias,
            grad_fc2_bias,
            grad_table,
        ),
        ("fsdp", "tp"),
    )
    return (
        result.astype(jnp.bfloat16),
        grad_input,
        qkv_shard,
        out_shard,
        fc1_shard,
        fc2_shard,
        summed[0],
        summed[1],
        summed[2],
        summed[3],
        summed[4],
        summed[5],
        summed[6],
        summed[7],
        summed[8],
    )


def solution(mesh):
    placed = (
        P(("fsdp", "tp"), None),
        P(("fsdp", "tp")),
        P("fsdp"),
        P(("fsdp", "tp"), None),
        P(None, "fsdp", "tp"),
        P("tp", "fsdp"),
        P("fsdp", "tp"),
        P("tp", "fsdp"),
        P(),
        P(),
        P(),
        P(),
        P(),
        P(),
        P(),
        P(),
        P(),
    )
    return jax.shard_map(
        on_device,
        mesh=mesh,
        in_specs=placed,
        out_specs=(
            P(("fsdp", "tp"), None),
            P(("fsdp", "tp"), None),
            P(None, "fsdp", "tp"),
            P("tp", "fsdp"),
            P("fsdp", "tp"),
            P("tp", "fsdp"),
            P(),
            P(),
            P(),
            P(),
            P(),
            P(),
            P(),
            P(),
            P(),
        ),
        check_vma=False,
    )
```

```python
import functools
from functools import partial

import jax
import jax.numpy as jnp
from jax import lax
from jax.experimental import pallas as pl
from jax.experimental.pallas import tpu as pltpu
from jax.sharding import PartitionSpec as P

HD = 64
NPASS = 5
QBLOCK = 512


HIGH = lax.Precision.HIGHEST
EPS = 1e-05
NEG_FILL = -1e30


def norm_forward(rows_in, gain, shift):
    center = rows_in - jnp.mean(rows_in, axis=-1, keepdims=True)
    scale_inv = lax.rsqrt(jnp.mean(center * center, axis=-1, keepdims=True) + EPS)
    unit_rows = center * scale_inv
    return (unit_rows * gain + shift, unit_rows, scale_inv)


def norm_backward(grad_out, unit_rows, scale_inv, gain):
    grad_unit = grad_out * gain
    first_mean = jnp.mean(grad_unit, axis=-1, keepdims=True)
    second_mean = jnp.mean(grad_unit * unit_rows, axis=-1, keepdims=True)
    grad_rows = scale_inv * (grad_unit - first_mean - unit_rows * second_mean)
    return (grad_rows, jnp.sum(grad_out * unit_rows, axis=0), jnp.sum(grad_out, axis=0))


def matmul_nt(left, right):
    return lax.dot_general(
        left, right, (((1,), (1,)), ((), ())), preferred_element_type=jnp.float32
    )


def matmul_tn(left, right):
    return lax.dot_general(
        left, right, (((0,), (0,)), ((), ())), preferred_element_type=jnp.float32
    )


def block_scores(query_block, keys_all, row_start, prefix_len, scale):
    raw = (
        jnp.einsum("qhe,khe->hqk", query_block, keys_all, preferred_element_type=jnp.float32)
        * scale
    )
    row_ids = row_start + jnp.arange(query_block.shape[0], dtype=jnp.int32)
    col_ids = jnp.arange(keys_all.shape[0], dtype=jnp.int32)
    allowed = (col_ids[None, :] <= row_ids[:, None]) | (col_ids[None, :] < prefix_len)
    return jnp.where(allowed[None], raw, NEG_FILL)


ATT_QB = 256


def _mask(prefix_len, qb, rows, cols):
    row = qb * rows + lax.broadcasted_iota(jnp.int32, (rows, cols), 0)
    col = lax.broadcasted_iota(jnp.int32, (rows, cols), 1)
    return (col <= row) | (col < prefix_len)


def _nt(a, b):
    return lax.dot_general(a, b, (((1,), (1,)), ((), ())), preferred_element_type=jnp.float32)


def _tn(a, b):
    return lax.dot_general(a, b, (((0,), (0,)), ((), ())), preferred_element_type=jnp.float32)


def _fwd_kernel(scale, prefix_ref, q_ref, k_ref, v_ref, o_ref, lse_ref):
    qb = pl.program_id(1)
    q = q_ref[0]
    rows, cols = q.shape[0], k_ref.shape[1]
    scores = _nt(q, k_ref[0]) * scale
    scores = jnp.where(_mask(prefix_ref[0], qb, rows, cols), scores, NEG_FILL)
    peak = jnp.max(scores, axis=-1, keepdims=True)
    expo = jnp.exp(scores - peak)
    total = jnp.sum(expo, axis=-1, keepdims=True)
    probs_low = (expo / total).astype(jnp.bfloat16)
    out = jnp.dot(probs_low, v_ref[0], preferred_element_type=jnp.float32)
    o_ref[0] = out.astype(o_ref.dtype)
    lse_ref[0] = peak + jnp.log(total)


def _bwd_kernel(scale, prefix_ref, q_ref, k_ref, v_ref, do_ref, lse_ref,
                dq_ref, dk_ref, dv_ref, dk_acc, dv_acc):
    qb = pl.program_id(1)

    @pl.when(qb == 0)
    def _():
        dk_acc[...] = jnp.zeros_like(dk_acc)
        dv_acc[...] = jnp.zeros_like(dv_acc)

    q = q_ref[0]
    k = k_ref[0]
    grad_out = do_ref[0]
    rows, cols = q.shape[0], k.shape[0]
    scores = _nt(q, k) * scale
    scores = jnp.where(_mask(prefix_ref[0], qb, rows, cols), scores, NEG_FILL)
    probs = jnp.exp(scores - lse_ref[0])
    dv_acc[...] += _tn(probs.astype(jnp.bfloat16), grad_out)
    grad_probs = _nt(grad_out, v_ref[0])
    inner = jnp.sum(probs * grad_probs, axis=-1, keepdims=True)
    grad_scores = (probs * (grad_probs - inner)).astype(jnp.bfloat16)
    dq_ref[0] = (jnp.dot(grad_scores, k, preferred_element_type=jnp.float32) * scale).astype(dq_ref.dtype)
    dk_acc[...] += _tn(grad_scores, q)

    @pl.when(qb == pl.num_programs(1) - 1)
    def _():
        dk_ref[0] = (dk_acc[...] * scale).astype(dk_ref.dtype)
        dv_ref[0] = dv_acc[...].astype(dv_ref.dtype)


def attn_forward(prefix, q, k, v, scale):
    heads, seq, hd = q.shape
    qb = min(ATT_QB, seq)
    grid = (heads, seq // qb)
    q_spec = pl.BlockSpec((1, qb, hd), lambda h, i, p: (h, i, 0))
    kv_spec = pl.BlockSpec((1, seq, hd), lambda h, i, p: (h, 0, 0))
    lse_spec = pl.BlockSpec((1, qb, 1), lambda h, i, p: (h, i, 0))
    return pl.pallas_call(
        functools.partial(_fwd_kernel, scale),
        out_shape=(jax.ShapeDtypeStruct((heads, seq, hd), jnp.bfloat16),
                   jax.ShapeDtypeStruct((heads, seq, 1), jnp.float32)),
        grid_spec=pltpu.PrefetchScalarGridSpec(
            num_scalar_prefetch=1, grid=grid,
            in_specs=[q_spec, kv_spec, kv_spec],
            out_specs=[q_spec, lse_spec]),
        compiler_params=pltpu.CompilerParams(
            dimension_semantics=("arbitrary", "arbitrary"),
            vmem_limit_bytes=48 * 1024 * 1024),
        cost_estimate=pl.CostEstimate(
            flops=4 * heads * seq * seq * hd, transcendentals=heads * seq * seq,
            bytes_accessed=4 * heads * seq * hd * 2),
    )(prefix, q, k, v)


def attn_backward(prefix, q, k, v, grad_out, lse, scale):
    heads, seq, hd = q.shape
    qb = min(ATT_QB, seq)
    grid = (heads, seq // qb)
    q_spec = pl.BlockSpec((1, qb, hd), lambda h, i, p: (h, i, 0))
    kv_spec = pl.BlockSpec((1, seq, hd), lambda h, i, p: (h, 0, 0))
    lse_spec = pl.BlockSpec((1, qb, 1), lambda h, i, p: (h, i, 0))
    shape = jax.ShapeDtypeStruct((heads, seq, hd), jnp.bfloat16)
    return pl.pallas_call(
        functools.partial(_bwd_kernel, scale),
        out_shape=(shape, shape, shape),
        grid_spec=pltpu.PrefetchScalarGridSpec(
            num_scalar_prefetch=1, grid=grid,
            in_specs=[q_spec, kv_spec, kv_spec, q_spec, lse_spec],
            out_specs=[q_spec, kv_spec, kv_spec],
            scratch_shapes=[pltpu.VMEM((seq, hd), jnp.float32),
                            pltpu.VMEM((seq, hd), jnp.float32)]),
        compiler_params=pltpu.CompilerParams(
            dimension_semantics=("arbitrary", "arbitrary"),
            vmem_limit_bytes=48 * 1024 * 1024),
        cost_estimate=pl.CostEstimate(
            flops=10 * heads * seq * seq * hd, transcendentals=heads * seq * seq,
            bytes_accessed=8 * heads * seq * hd * 2),
    )(prefix, q, k, v, grad_out, lse)


def on_device(
    tokens,
    pass_ids,
    prefix,
    cotangent,
    qkv_weight,
    out_weight,
    fc1_weight,
    fc2_weight,
    ln1_gain,
    ln1_bias,
    qv_bias,
    out_bias,
    ln2_gain,
    ln2_bias,
    fc1_bias,
    fc2_bias,
    pass_table,
):
    tp_count = lax.axis_size("tp")
    tp_rank = lax.axis_index("tp")
    local_rows = tokens.shape[0]
    seq_len = local_rows * tp_count
    cols_here = qkv_weight.shape[2]
    heads_here = cols_here // HD
    scale = HD ** (-0.5)
    prefix_len = prefix[0]
    gelu_tanh = partial(jax.nn.gelu, approximate=True)
    fsdp_count = lax.axis_size("fsdp")
    qkv_cols = lax.all_gather(qkv_weight, "fsdp", axis=1, tiled=True)
    qkv_full = qkv_cols
    hidden_here = fc1_weight.shape[1]
    qv_here = lax.dynamic_slice_in_dim(qv_bias, tp_rank * cols_here, cols_here, 1)
    one_hot = (pass_ids[:, None] == jnp.arange(NPASS, dtype=jnp.int32)[None, :]).astype(jnp.float32)
    block_in = tokens.astype(jnp.float32) + jnp.dot(
        one_hot, pass_table, precision=HIGH, preferred_element_type=jnp.float32
    )
    normed, unit_one, inv_one = norm_forward(block_in, ln1_gain, ln1_bias)
    normed_all = lax.all_gather(normed.astype(jnp.bfloat16), "tp", axis=0, tiled=True)
    shards = (out_weight, fc1_weight, fc2_weight)
    packed = jnp.concatenate([piece.reshape(-1) for piece in shards])
    packed, qkv_cols, normed_all = lax.optimization_barrier((packed, qkv_cols, normed_all))
    qkv_full = qkv_cols
    gathered = lax.all_gather(packed, "fsdp", axis=0, tiled=False)
    qkv_copies = jnp.broadcast_to(qkv_cols[None], (tp_count,) + qkv_cols.shape)
    qkv_all = lax.all_to_all(qkv_copies, "tp", 0, 0, tiled=True)
    grad_rows = lax.all_gather(cotangent, "tp", axis=0, tiled=True)
    projected = jnp.einsum("rd,kdc->krc", normed_all, qkv_full, preferred_element_type=jnp.float32)
    queries = (projected[0] + qv_here[0]).astype(jnp.bfloat16).reshape(seq_len, heads_here, HD)
    keys_all = projected[1].astype(jnp.bfloat16).reshape(seq_len, heads_here, HD)
    values_all = (projected[2] + qv_here[1]).astype(jnp.bfloat16).reshape(seq_len, heads_here, HD)
    q_heads = jnp.transpose(queries, (1, 0, 2))
    k_heads = jnp.transpose(keys_all, (1, 0, 2))
    v_heads = jnp.transpose(values_all, (1, 0, 2))
    out_heads, log_mass = attn_forward(prefix, q_heads, k_heads, v_heads, scale)
    out_heads, qkv_all = lax.optimization_barrier((out_heads, qkv_all))
    mixed = jnp.transpose(out_heads, (1, 0, 2)).reshape(seq_len, cols_here)
    pieces = []
    offset = 0
    for piece in shards:
        size = piece.size
        pieces.append(gathered[:, offset : offset + size].reshape((fsdp_count,) + piece.shape))
        offset += size
    out_full = jnp.moveaxis(pieces[0], 0, 1).reshape(out_weight.shape[0], -1)
    fc1_part = pieces[1].reshape(-1, fc1_weight.shape[1])
    fc2_part = jnp.moveaxis(pieces[2], 0, 1).reshape(fc2_weight.shape[0], -1)
    out_all = lax.all_gather(out_full, "tp", axis=0, tiled=True)
    mixed, grad_rows, out_all, fc1_part, fc2_part = lax.optimization_barrier(
        (mixed, grad_rows, out_all, fc1_part, fc2_part)
    )
    mixed_rows = lax.all_to_all(mixed, "tp", 0, 1, tiled=True)
    middle = block_in + jnp.dot(mixed_rows, out_all, preferred_element_type=jnp.float32) + out_bias
    normed_two, unit_two, inv_two = norm_forward(middle, ln2_gain, ln2_bias)
    normed_two = normed_two.astype(jnp.bfloat16)
    grad_top = cotangent.astype(jnp.float32)
    fc1_bias_here = lax.dynamic_slice_in_dim(fc1_bias, tp_rank * hidden_here, hidden_here, 0)
    normed_rows = lax.all_gather(normed_two, "tp", axis=0, tiled=True)
    before = jnp.dot(normed_rows, fc1_part, preferred_element_type=jnp.float32) + fc1_bias_here
    hidden = gelu_tanh(before).astype(jnp.bfloat16)
    fc2_partial = jnp.dot(hidden, fc2_part, preferred_element_type=jnp.float32).astype(jnp.bfloat16)
    grad_hidden = matmul_nt(grad_rows, fc2_part)
    grad_before = jax.vjp(gelu_tanh, before)[1](grad_hidden)[0].astype(jnp.bfloat16)
    grad_fc1_bias = lax.dynamic_update_slice_in_dim(
        jnp.zeros(fc1_bias.shape, jnp.float32),
        jnp.sum(grad_before.astype(jnp.float32), axis=0),
        tp_rank * hidden_here,
        0,
    )
    grad_fc1 = matmul_tn(normed_rows, grad_before)
    grad_fc2 = matmul_tn(hidden, grad_rows)
    grad_normed_two = lax.psum_scatter(
        matmul_nt(grad_before, fc1_part), "tp", scatter_dimension=0, tiled=True
    )
    grad_normed_two, fc2_partial, grad_fc1, grad_fc2 = lax.optimization_barrier(
        (grad_normed_two, fc2_partial, grad_fc1, grad_fc2)
    )
    grad_fc2_bias = jnp.sum(grad_top, axis=0)
    grad_from_norm, grad_ln2_gain, grad_ln2_bias = norm_backward(
        grad_normed_two, unit_two, inv_two, ln2_gain
    )
    grad_middle = grad_top + grad_from_norm
    grad_out_bias = jnp.sum(grad_middle, axis=0)
    grad_attn_rows = lax.all_gather(grad_middle.astype(jnp.bfloat16), "tp", axis=0, tiled=True)
    fc2_partial, grad_attn_rows = lax.optimization_barrier((fc2_partial, grad_attn_rows))
    fc2_parts = lax.all_to_all(
        fc2_partial.reshape(tp_count, local_rows, -1), "tp", 0, 0, tiled=True
    )
    result = middle + jnp.sum(fc2_parts.astype(jnp.float32), axis=0) + fc2_bias
    grad_out_w = matmul_tn(mixed, grad_attn_rows)
    fsdp_count = lax.axis_size("fsdp")
    dense_grads = (
        jnp.moveaxis(grad_out_w.reshape(grad_out_w.shape[0], fsdp_count, -1), 1, 0),
        grad_fc1.reshape(fsdp_count, -1, grad_fc1.shape[1]),
        jnp.moveaxis(grad_fc2.reshape(grad_fc2.shape[0], fsdp_count, -1), 1, 0),
    )
    dense_packed = jnp.concatenate([g.reshape(fsdp_count, -1) for g in dense_grads], axis=1)
    dense_summed = lax.psum_scatter(
        dense_packed.reshape(-1, grad_fc1.shape[1]), "fsdp", scatter_dimension=0, tiled=True
    ).reshape(1, -1)
    grad_mixed = (
        matmul_nt(grad_attn_rows, out_full).astype(jnp.bfloat16).reshape(seq_len, heads_here, HD)
    )
    grad_q_heads, grad_k_heads, grad_v_heads = attn_backward(
        prefix, q_heads, k_heads, v_heads, jnp.transpose(grad_mixed, (1, 0, 2)), log_mass, scale
    )
    grad_proj = jnp.stack([grad_q_heads, grad_k_heads, grad_v_heads], axis=0)
    grad_proj, result = lax.optimization_barrier((grad_proj, result))
    grad_qv_here = jnp.stack(
        [
            jnp.sum(grad_q_heads.astype(jnp.float32), axis=1).reshape(-1),
            jnp.sum(grad_v_heads.astype(jnp.float32), axis=1).reshape(-1),
        ],
        axis=0,
    )
    grad_qv_bias = lax.dynamic_update_slice_in_dim(
        jnp.zeros(qv_bias.shape, jnp.float32), grad_qv_here, tp_rank * cols_here, 1
    )
    grad_qkv_w = jnp.einsum(
        "rd,khre->kdhe", normed_all, grad_proj, preferred_element_type=jnp.float32
    ).reshape(3, normed_all.shape[1], cols_here)
    grad_proj_rows = lax.all_to_all(grad_proj, "tp", 2, 1, tiled=True)
    grad_proj_rows, dense_summed = lax.optimization_barrier((grad_proj_rows, dense_summed))
    grad_normed = jnp.einsum(
        "kshre,skdhe->rd",
        grad_proj_rows.reshape(3, tp_count, heads_here, local_rows, HD),
        qkv_all.reshape(tp_count, 3, qkv_all.shape[2], heads_here, HD),
        preferred_element_type=jnp.float32,
    )
    dense_shards = []
    offset = 0
    for g in dense_grads:
        size = g[0].size
        dense_shards.append(dense_summed[0, offset : offset + size].reshape(g.shape[1:]))
        offset += size
    out_shard, fc1_shard, fc2_shard = dense_shards
    grad_in_norm, grad_ln1_gain, grad_ln1_bias = norm_backward(
        grad_normed, unit_one, inv_one, ln1_gain
    )
    grad_input = grad_middle + grad_in_norm
    grad_table = lax.dot_general(
        one_hot,
        grad_input,
        (((0,), (0,)), ((), ())),
        precision=HIGH,
        preferred_element_type=jnp.float32,
    )
    qkv_shard = lax.psum_scatter(grad_qkv_w, "fsdp", scatter_dimension=1, tiled=True)
    summed = lax.psum(
        (
            grad_ln1_gain,
            grad_ln1_bias,
            grad_qv_bias,
            grad_out_bias,
            grad_ln2_gain,
            grad_ln2_bias,
            grad_fc1_bias,
            grad_fc2_bias,
            grad_table,
        ),
        ("fsdp", "tp"),
    )
    return (
        result.astype(jnp.bfloat16),
        grad_input,
        qkv_shard,
        out_shard,
        fc1_shard,
        fc2_shard,
        summed[0],
        summed[1],
        summed[2],
        summed[3],
        summed[4],
        summed[5],
        summed[6],
        summed[7],
        summed[8],
    )


def solution(mesh):
    placed = (
        P(("fsdp", "tp"), None),
        P(("fsdp", "tp")),
        P("fsdp"),
        P(("fsdp", "tp"), None),
        P(None, "fsdp", "tp"),
        P("tp", "fsdp"),
        P("fsdp", "tp"),
        P("tp", "fsdp"),
        P(),
        P(),
        P(),
        P(),
        P(),
        P(),
        P(),
        P(),
        P(),
    )
    return jax.shard_map(
        on_device,
        mesh=mesh,
        in_specs=placed,
        out_specs=(
            P(("fsdp", "tp"), None),
            P(("fsdp", "tp"), None),
            P(None, "fsdp", "tp"),
            P("tp", "fsdp"),
            P("fsdp", "tp"),
            P("tp", "fsdp"),
            P(),
            P(),
            P(),
            P(),
            P(),
            P(),
            P(),
            P(),
            P(),
        ),
        check_vma=False,
    )
```

```python
import functools
from functools import partial

import jax
import jax.numpy as jnp
from jax import lax
from jax.experimental import pallas as pl
from jax.experimental.pallas import tpu as pltpu
from jax.sharding import PartitionSpec as P

HD = 64
NPASS = 5
QBLOCK = 512


HIGH = lax.Precision.HIGHEST
EPS = 1e-05
NEG_FILL = -1e30


def norm_forward(rows_in, gain, shift):
    center = rows_in - jnp.mean(rows_in, axis=-1, keepdims=True)
    scale_inv = lax.rsqrt(jnp.mean(center * center, axis=-1, keepdims=True) + EPS)
    unit_rows = center * scale_inv
    return (unit_rows * gain + shift, unit_rows, scale_inv)


def norm_backward(grad_out, unit_rows, scale_inv, gain):
    grad_unit = grad_out * gain
    first_mean = jnp.mean(grad_unit, axis=-1, keepdims=True)
    second_mean = jnp.mean(grad_unit * unit_rows, axis=-1, keepdims=True)
    grad_rows = scale_inv * (grad_unit - first_mean - unit_rows * second_mean)
    return (grad_rows, jnp.sum(grad_out * unit_rows, axis=0), jnp.sum(grad_out, axis=0))


def matmul_nt(left, right):
    return lax.dot_general(
        left, right, (((1,), (1,)), ((), ())), preferred_element_type=jnp.float32
    )


def matmul_tn(left, right):
    return lax.dot_general(
        left, right, (((0,), (0,)), ((), ())), preferred_element_type=jnp.float32
    )


def block_scores(query_block, keys_all, row_start, prefix_len, scale):
    raw = (
        jnp.einsum("qhe,khe->hqk", query_block, keys_all, preferred_element_type=jnp.float32)
        * scale
    )
    row_ids = row_start + jnp.arange(query_block.shape[0], dtype=jnp.int32)
    col_ids = jnp.arange(keys_all.shape[0], dtype=jnp.int32)
    allowed = (col_ids[None, :] <= row_ids[:, None]) | (col_ids[None, :] < prefix_len)
    return jnp.where(allowed[None], raw, NEG_FILL)


ATT_QB = 256


def _mask(prefix_len, qb, rows, cols):
    row = qb * rows + lax.broadcasted_iota(jnp.int32, (rows, cols), 0)
    col = lax.broadcasted_iota(jnp.int32, (rows, cols), 1)
    return (col <= row) | (col < prefix_len)


def _nt(a, b):
    return lax.dot_general(a, b, (((1,), (1,)), ((), ())), preferred_element_type=jnp.float32)


def _tn(a, b):
    return lax.dot_general(a, b, (((0,), (0,)), ((), ())), preferred_element_type=jnp.float32)


def _fwd_kernel(scale, prefix_ref, q_ref, k_ref, v_ref, o_ref, lse_ref):
    qb = pl.program_id(1)
    q = q_ref[0]
    rows, cols = q.shape[0], k_ref.shape[1]
    scores = _nt(q, k_ref[0]) * scale
    scores = jnp.where(_mask(prefix_ref[0], qb, rows, cols), scores, NEG_FILL)
    peak = jnp.max(scores, axis=-1, keepdims=True)
    expo = jnp.exp(scores - peak)
    total = jnp.sum(expo, axis=-1, keepdims=True)
    probs_low = (expo / total).astype(jnp.bfloat16)
    out = jnp.dot(probs_low, v_ref[0], preferred_element_type=jnp.float32)
    o_ref[0, 0] = out.astype(o_ref.dtype)
    lse_ref[0] = peak + jnp.log(total)


def _bwd_kernel(scale, prefix_ref, q_ref, k_ref, v_ref, do_ref, lse_ref,
                dq_ref, dk_ref, dv_ref, dk_acc, dv_acc):
    qb = pl.program_id(1)

    @pl.when(qb == 0)
    def _():
        dk_acc[...] = jnp.zeros_like(dk_acc)
        dv_acc[...] = jnp.zeros_like(dv_acc)

    q = q_ref[0]
    k = k_ref[0]
    grad_out = do_ref[0]
    rows, cols = q.shape[0], k.shape[0]
    scores = _nt(q, k) * scale
    scores = jnp.where(_mask(prefix_ref[0], qb, rows, cols), scores, NEG_FILL)
    probs = jnp.exp(scores - lse_ref[0])
    dv_acc[...] += _tn(probs.astype(jnp.bfloat16), grad_out)
    grad_probs = _nt(grad_out, v_ref[0])
    inner = jnp.sum(probs * grad_probs, axis=-1, keepdims=True)
    grad_scores = (probs * (grad_probs - inner)).astype(jnp.bfloat16)
    dq_ref[0, 0] = (jnp.dot(grad_scores, k, preferred_element_type=jnp.float32) * scale).astype(dq_ref.dtype)
    dk_acc[...] += _tn(grad_scores, q)

    @pl.when(qb == pl.num_programs(1) - 1)
    def _():
        groups, rows, hd = dk_ref.shape[0], dk_ref.shape[2], dk_ref.shape[3]
        dk_ref[:, 0] = (dk_acc[...] * scale).astype(dk_ref.dtype).reshape(groups, rows, hd)
        dv_ref[:, 0] = dv_acc[...].astype(dv_ref.dtype).reshape(groups, rows, hd)


def attn_forward(prefix, q, k, v, scale, groups):
    heads, seq, hd = q.shape
    qb = min(ATT_QB, seq // groups)
    per = seq // groups // qb
    grid = (heads, seq // qb)
    q_spec = pl.BlockSpec((1, qb, hd), lambda h, i, p: (h, i, 0))
    kv_spec = pl.BlockSpec((1, seq, hd), lambda h, i, p: (h, 0, 0))
    lse_spec = pl.BlockSpec((1, qb, 1), lambda h, i, p: (h, i, 0))
    o_spec = pl.BlockSpec((1, 1, qb, hd), lambda h, i, p: (i // per, h, i % per, 0))
    return pl.pallas_call(
        functools.partial(_fwd_kernel, scale),
        out_shape=(jax.ShapeDtypeStruct((groups, heads, seq // groups, hd), jnp.bfloat16),
                   jax.ShapeDtypeStruct((heads, seq, 1), jnp.float32)),
        grid_spec=pltpu.PrefetchScalarGridSpec(
            num_scalar_prefetch=1, grid=grid,
            in_specs=[q_spec, kv_spec, kv_spec],
            out_specs=[o_spec, lse_spec]),
        compiler_params=pltpu.CompilerParams(
            dimension_semantics=("arbitrary", "arbitrary"),
            vmem_limit_bytes=48 * 1024 * 1024),
        cost_estimate=pl.CostEstimate(
            flops=4 * heads * seq * seq * hd, transcendentals=heads * seq * seq,
            bytes_accessed=4 * heads * seq * hd * 2),
    )(prefix, q, k, v)


def attn_backward(prefix, q, k, v, grad_out, lse, scale, groups):
    heads, seq, hd = q.shape
    qb = min(ATT_QB, seq // groups)
    per = seq // groups // qb
    grid = (heads, seq // qb)
    q_spec = pl.BlockSpec((1, qb, hd), lambda h, i, p: (h, i, 0))
    kv_spec = pl.BlockSpec((1, seq, hd), lambda h, i, p: (h, 0, 0))
    lse_spec = pl.BlockSpec((1, qb, 1), lambda h, i, p: (h, i, 0))
    dq_spec = pl.BlockSpec((1, 1, qb, hd), lambda h, i, p: (i // per, h, i % per, 0))
    dkv_spec = pl.BlockSpec((groups, 1, seq // groups, hd), lambda h, i, p: (0, h, 0, 0))
    shape = jax.ShapeDtypeStruct((groups, heads, seq // groups, hd), jnp.bfloat16)
    return pl.pallas_call(
        functools.partial(_bwd_kernel, scale),
        out_shape=(shape, shape, shape),
        grid_spec=pltpu.PrefetchScalarGridSpec(
            num_scalar_prefetch=1, grid=grid,
            in_specs=[q_spec, kv_spec, kv_spec, q_spec, lse_spec],
            out_specs=[dq_spec, dkv_spec, dkv_spec],
            scratch_shapes=[pltpu.VMEM((seq, hd), jnp.float32),
                            pltpu.VMEM((seq, hd), jnp.float32)]),
        compiler_params=pltpu.CompilerParams(
            dimension_semantics=("arbitrary", "arbitrary"),
            vmem_limit_bytes=48 * 1024 * 1024),
        cost_estimate=pl.CostEstimate(
            flops=10 * heads * seq * seq * hd, transcendentals=heads * seq * seq,
            bytes_accessed=8 * heads * seq * hd * 2),
    )(prefix, q, k, v, grad_out, lse)


def on_device(
    tokens,
    pass_ids,
    prefix,
    cotangent,
    qkv_weight,
    out_weight,
    fc1_weight,
    fc2_weight,
    ln1_gain,
    ln1_bias,
    qv_bias,
    out_bias,
    ln2_gain,
    ln2_bias,
    fc1_bias,
    fc2_bias,
    pass_table,
):
    tp_count = lax.axis_size("tp")
    tp_rank = lax.axis_index("tp")
    local_rows = tokens.shape[0]
    seq_len = local_rows * tp_count
    cols_here = qkv_weight.shape[2]
    heads_here = cols_here // HD
    scale = HD ** (-0.5)
    prefix_len = prefix[0]
    gelu_tanh = partial(jax.nn.gelu, approximate=True)
    fsdp_count = lax.axis_size("fsdp")
    qkv_cols = lax.all_gather(qkv_weight, "fsdp", axis=1, tiled=True)
    qkv_full = qkv_cols
    hidden_here = fc1_weight.shape[1]
    qv_here = lax.dynamic_slice_in_dim(qv_bias, tp_rank * cols_here, cols_here, 1)
    one_hot = (pass_ids[:, None] == jnp.arange(NPASS, dtype=jnp.int32)[None, :]).astype(jnp.float32)
    block_in = tokens.astype(jnp.float32) + jnp.dot(
        one_hot, pass_table, precision=HIGH, preferred_element_type=jnp.float32
    )
    normed, unit_one, inv_one = norm_forward(block_in, ln1_gain, ln1_bias)
    normed_all = lax.all_gather(normed.astype(jnp.bfloat16), "tp", axis=0, tiled=True)
    shards = (out_weight, fc1_weight, fc2_weight)
    packed = jnp.concatenate([piece.reshape(-1) for piece in shards])
    packed, qkv_cols, normed_all = lax.optimization_barrier((packed, qkv_cols, normed_all))
    qkv_full = qkv_cols
    gathered = lax.all_gather(packed, "fsdp", axis=0, tiled=False)
    qkv_copies = jnp.broadcast_to(qkv_cols[None], (tp_count,) + qkv_cols.shape)
    qkv_all = lax.all_to_all(qkv_copies, "tp", 0, 0, tiled=True)
    grad_rows = lax.all_gather(cotangent, "tp", axis=0, tiled=True)
    projected = jnp.einsum("rd,kdc->krc", normed_all, qkv_full, preferred_element_type=jnp.float32)
    queries = (projected[0] + qv_here[0]).astype(jnp.bfloat16).reshape(seq_len, heads_here, HD)
    keys_all = projected[1].astype(jnp.bfloat16).reshape(seq_len, heads_here, HD)
    values_all = (projected[2] + qv_here[1]).astype(jnp.bfloat16).reshape(seq_len, heads_here, HD)
    q_heads = jnp.transpose(queries, (1, 0, 2))
    k_heads = jnp.transpose(keys_all, (1, 0, 2))
    v_heads = jnp.transpose(values_all, (1, 0, 2))
    mixed, log_mass = attn_forward(prefix, q_heads, k_heads, v_heads, scale, tp_count)
    mixed, qkv_all = lax.optimization_barrier((mixed, qkv_all))
    pieces = []
    offset = 0
    for piece in shards:
        size = piece.size
        pieces.append(gathered[:, offset : offset + size].reshape((fsdp_count,) + piece.shape))
        offset += size
    out_full = jnp.moveaxis(pieces[0], 0, 1).reshape(out_weight.shape[0], -1)
    fc1_part = pieces[1].reshape(-1, fc1_weight.shape[1])
    fc2_part = jnp.moveaxis(pieces[2], 0, 1).reshape(fc2_weight.shape[0], -1)
    out_all = lax.all_gather(out_full, "tp", axis=0, tiled=True)
    mixed, grad_rows, out_all, fc1_part, fc2_part = lax.optimization_barrier(
        (mixed, grad_rows, out_all, fc1_part, fc2_part)
    )
    mixed_rows = lax.all_to_all(mixed, "tp", 0, 0, tiled=True)
    middle = (
        block_in
        + jnp.einsum(
            "shre,shem->rm",
            mixed_rows,
            out_all.reshape(tp_count, heads_here, HD, -1),
            preferred_element_type=jnp.float32,
        )
        + out_bias
    )
    normed_two, unit_two, inv_two = norm_forward(middle, ln2_gain, ln2_bias)
    normed_two = normed_two.astype(jnp.bfloat16)
    grad_top = cotangent.astype(jnp.float32)
    fc1_bias_here = lax.dynamic_slice_in_dim(fc1_bias, tp_rank * hidden_here, hidden_here, 0)
    normed_rows = lax.all_gather(normed_two, "tp", axis=0, tiled=True)
    before = jnp.dot(normed_rows, fc1_part, preferred_element_type=jnp.float32) + fc1_bias_here
    hidden = gelu_tanh(before).astype(jnp.bfloat16)
    fc2_partial = jnp.dot(hidden, fc2_part, preferred_element_type=jnp.float32).astype(jnp.bfloat16)
    grad_hidden = matmul_nt(grad_rows, fc2_part)
    grad_before = jax.vjp(gelu_tanh, before)[1](grad_hidden)[0].astype(jnp.bfloat16)
    grad_fc1_bias = lax.dynamic_update_slice_in_dim(
        jnp.zeros(fc1_bias.shape, jnp.float32),
        jnp.sum(grad_before.astype(jnp.float32), axis=0),
        tp_rank * hidden_here,
        0,
    )
    grad_fc1 = matmul_tn(normed_rows, grad_before)
    grad_fc2 = matmul_tn(hidden, grad_rows)
    grad_normed_two = lax.psum_scatter(
        matmul_nt(grad_before, fc1_part), "tp", scatter_dimension=0, tiled=True
    )
    grad_normed_two, fc2_partial, grad_fc1, grad_fc2 = lax.optimization_barrier(
        (grad_normed_two, fc2_partial, grad_fc1, grad_fc2)
    )
    grad_fc2_bias = jnp.sum(grad_top, axis=0)
    grad_from_norm, grad_ln2_gain, grad_ln2_bias = norm_backward(
        grad_normed_two, unit_two, inv_two, ln2_gain
    )
    grad_middle = grad_top + grad_from_norm
    grad_out_bias = jnp.sum(grad_middle, axis=0)
    grad_attn_rows = lax.all_gather(grad_middle.astype(jnp.bfloat16), "tp", axis=0, tiled=True)
    fc2_partial, grad_attn_rows = lax.optimization_barrier((fc2_partial, grad_attn_rows))
    fc2_parts = lax.all_to_all(
        fc2_partial.reshape(tp_count, local_rows, -1), "tp", 0, 0, tiled=True
    )
    result = middle + jnp.sum(fc2_parts.astype(jnp.float32), axis=0) + fc2_bias
    grad_out_w = jnp.einsum(
        "thre,trm->hem",
        mixed,
        grad_attn_rows.reshape(tp_count, local_rows, -1),
        preferred_element_type=jnp.float32,
    ).reshape(cols_here, -1)
    fsdp_count = lax.axis_size("fsdp")
    dense_grads = (
        jnp.moveaxis(grad_out_w.reshape(grad_out_w.shape[0], fsdp_count, -1), 1, 0),
        grad_fc1.reshape(fsdp_count, -1, grad_fc1.shape[1]),
        jnp.moveaxis(grad_fc2.reshape(grad_fc2.shape[0], fsdp_count, -1), 1, 0),
    )
    dense_packed = jnp.concatenate([g.reshape(fsdp_count, -1) for g in dense_grads], axis=1)
    dense_summed = lax.psum_scatter(
        dense_packed.reshape(-1, grad_fc1.shape[1]), "fsdp", scatter_dimension=0, tiled=True
    ).reshape(1, -1)
    grad_mixed = (
        matmul_nt(grad_attn_rows, out_full).astype(jnp.bfloat16).reshape(seq_len, heads_here, HD)
    )
    grad_q_heads, grad_k_heads, grad_v_heads = attn_backward(
        prefix, q_heads, k_heads, v_heads, jnp.transpose(grad_mixed, (1, 0, 2)), log_mass, scale,
        tp_count,
    )
    grad_q_heads, grad_k_heads, grad_v_heads, result = lax.optimization_barrier(
        (grad_q_heads, grad_k_heads, grad_v_heads, result)
    )
    grad_kinds = (grad_q_heads, grad_k_heads, grad_v_heads)
    grad_qv_here = jnp.stack(
        [
            jnp.sum(grad_q_heads.astype(jnp.float32), axis=(0, 2)).reshape(-1),
            jnp.sum(grad_v_heads.astype(jnp.float32), axis=(0, 2)).reshape(-1),
        ],
        axis=0,
    )
    grad_qv_bias = lax.dynamic_update_slice_in_dim(
        jnp.zeros(qv_bias.shape, jnp.float32), grad_qv_here, tp_rank * cols_here, 1
    )
    normed_groups = normed_all.reshape(tp_count, local_rows, -1)
    grad_qkv_w = jnp.stack(
        [
            jnp.einsum("trd,thre->dhe", normed_groups, g, preferred_element_type=jnp.float32)
            for g in grad_kinds
        ]
    ).reshape(3, normed_all.shape[1], cols_here)
    grad_rows_kinds = [lax.all_to_all(g, "tp", 0, 0, tiled=True) for g in grad_kinds]
    grad_rows_kinds, dense_summed = lax.optimization_barrier((grad_rows_kinds, dense_summed))
    qkv_split = qkv_all.reshape(tp_count, 3, qkv_all.shape[2], heads_here, HD)
    grad_normed = sum(
        jnp.einsum("shre,sdhe->rd", g, qkv_split[:, kind], preferred_element_type=jnp.float32)
        for kind, g in enumerate(grad_rows_kinds)
    )
    dense_shards = []
    offset = 0
    for g in dense_grads:
        size = g[0].size
        dense_shards.append(dense_summed[0, offset : offset + size].reshape(g.shape[1:]))
        offset += size
    out_shard, fc1_shard, fc2_shard = dense_shards
    grad_in_norm, grad_ln1_gain, grad_ln1_bias = norm_backward(
        grad_normed, unit_one, inv_one, ln1_gain
    )
    grad_input = grad_middle + grad_in_norm
    grad_table = lax.dot_general(
        one_hot,
        grad_input,
        (((0,), (0,)), ((), ())),
        precision=HIGH,
        preferred_element_type=jnp.float32,
    )
    qkv_shard = lax.psum_scatter(grad_qkv_w, "fsdp", scatter_dimension=1, tiled=True)
    summed = lax.psum(
        (
            grad_ln1_gain,
            grad_ln1_bias,
            grad_qv_bias,
            grad_out_bias,
            grad_ln2_gain,
            grad_ln2_bias,
            grad_fc1_bias,
            grad_fc2_bias,
            grad_table,
        ),
        ("fsdp", "tp"),
    )
    return (
        result.astype(jnp.bfloat16),
        grad_input,
        qkv_shard,
        out_shard,
        fc1_shard,
        fc2_shard,
        summed[0],
        summed[1],
        summed[2],
        summed[3],
        summed[4],
        summed[5],
        summed[6],
        summed[7],
        summed[8],
    )


def solution(mesh):
    placed = (
        P(("fsdp", "tp"), None),
        P(("fsdp", "tp")),
        P("fsdp"),
        P(("fsdp", "tp"), None),
        P(None, "fsdp", "tp"),
        P("tp", "fsdp"),
        P("fsdp", "tp"),
        P("tp", "fsdp"),
        P(),
        P(),
        P(),
        P(),
        P(),
        P(),
        P(),
        P(),
        P(),
    )
    return jax.shard_map(
        on_device,
        mesh=mesh,
        in_specs=placed,
        out_specs=(
            P(("fsdp", "tp"), None),
            P(("fsdp", "tp"), None),
            P(None, "fsdp", "tp"),
            P("tp", "fsdp"),
            P("fsdp", "tp"),
            P("tp", "fsdp"),
            P(),
            P(),
            P(),
            P(),
            P(),
            P(),
            P(),
            P(),
            P(),
        ),
        check_vma=False,
    )
```

```python
import functools
from functools import partial

import jax
import jax.numpy as jnp
from jax import lax
from jax.experimental import pallas as pl
from jax.experimental.pallas import tpu as pltpu
from jax.sharding import PartitionSpec as P

HD = 64
NPASS = 5
QBLOCK = 512


HIGH = lax.Precision.HIGHEST
EPS = 1e-05
NEG_FILL = -1e30


def norm_forward(rows_in, gain, shift):
    center = rows_in - jnp.mean(rows_in, axis=-1, keepdims=True)
    scale_inv = lax.rsqrt(jnp.mean(center * center, axis=-1, keepdims=True) + EPS)
    unit_rows = center * scale_inv
    return (unit_rows * gain + shift, unit_rows, scale_inv)


def norm_backward(grad_out, unit_rows, scale_inv, gain):
    grad_unit = grad_out * gain
    first_mean = jnp.mean(grad_unit, axis=-1, keepdims=True)
    second_mean = jnp.mean(grad_unit * unit_rows, axis=-1, keepdims=True)
    grad_rows = scale_inv * (grad_unit - first_mean - unit_rows * second_mean)
    return (grad_rows, jnp.sum(grad_out * unit_rows, axis=0), jnp.sum(grad_out, axis=0))


def matmul_nt(left, right):
    return lax.dot_general(
        left, right, (((1,), (1,)), ((), ())), preferred_element_type=jnp.float32
    )


def matmul_tn(left, right):
    return lax.dot_general(
        left, right, (((0,), (0,)), ((), ())), preferred_element_type=jnp.float32
    )


def block_scores(query_block, keys_all, row_start, prefix_len, scale):
    raw = (
        jnp.einsum("qhe,khe->hqk", query_block, keys_all, preferred_element_type=jnp.float32)
        * scale
    )
    row_ids = row_start + jnp.arange(query_block.shape[0], dtype=jnp.int32)
    col_ids = jnp.arange(keys_all.shape[0], dtype=jnp.int32)
    allowed = (col_ids[None, :] <= row_ids[:, None]) | (col_ids[None, :] < prefix_len)
    return jnp.where(allowed[None], raw, NEG_FILL)


ATT_QB = 256


def _mask(prefix_len, qb, rows, cols):
    row = qb * rows + lax.broadcasted_iota(jnp.int32, (rows, cols), 0)
    col = lax.broadcasted_iota(jnp.int32, (rows, cols), 1)
    return (col <= row) | (col < prefix_len)


def _nt(a, b):
    return lax.dot_general(a, b, (((1,), (1,)), ((), ())), preferred_element_type=jnp.float32)


def _tn(a, b):
    return lax.dot_general(a, b, (((0,), (0,)), ((), ())), preferred_element_type=jnp.float32)


def _fwd_kernel(scale, prefix_ref, q_ref, k_ref, v_ref, o_ref, lse_ref):
    qb = pl.program_id(1)
    q = q_ref[0]
    rows, cols = q.shape[0], k_ref.shape[1]
    scores = _nt(q, k_ref[0]) * scale
    scores = jnp.where(_mask(prefix_ref[0], qb, rows, cols), scores, NEG_FILL)
    peak = jnp.max(scores, axis=-1, keepdims=True)
    expo = jnp.exp(scores - peak)
    total = jnp.sum(expo, axis=-1, keepdims=True)
    probs_low = (expo / total).astype(jnp.bfloat16)
    out = jnp.dot(probs_low, v_ref[0], preferred_element_type=jnp.float32)
    o_ref[0, 0] = out.astype(o_ref.dtype)
    lse_ref[0] = peak + jnp.log(total)


def _bwd_kernel(scale, prefix_ref, q_ref, k_ref, v_ref, do_ref, lse_ref,
                dq_ref, dk_ref, dv_ref, dk_acc, dv_acc):
    qb = pl.program_id(1)

    @pl.when(qb == 0)
    def _():
        dk_acc[...] = jnp.zeros_like(dk_acc)
        dv_acc[...] = jnp.zeros_like(dv_acc)

    q = q_ref[0]
    k = k_ref[0]
    grad_out = do_ref[0]
    rows, cols = q.shape[0], k.shape[0]
    scores = _nt(q, k) * scale
    scores = jnp.where(_mask(prefix_ref[0], qb, rows, cols), scores, NEG_FILL)
    probs = jnp.exp(scores - lse_ref[0])
    dv_acc[...] += _tn(probs.astype(jnp.bfloat16), grad_out)
    grad_probs = _nt(grad_out, v_ref[0])
    inner = jnp.sum(probs * grad_probs, axis=-1, keepdims=True)
    grad_scores = (probs * (grad_probs - inner)).astype(jnp.bfloat16)
    dq_ref[0, 0] = (jnp.dot(grad_scores, k, preferred_element_type=jnp.float32) * scale).astype(dq_ref.dtype)
    dk_acc[...] += _tn(grad_scores, q)

    @pl.when(qb == pl.num_programs(1) - 1)
    def _():
        groups, rows, hd = dk_ref.shape[0], dk_ref.shape[2], dk_ref.shape[3]
        dk_ref[:, 0] = (dk_acc[...] * scale).astype(dk_ref.dtype).reshape(groups, rows, hd)
        dv_ref[:, 0] = dv_acc[...].astype(dv_ref.dtype).reshape(groups, rows, hd)


def attn_forward(prefix, q, k, v, scale, groups):
    heads, seq, hd = q.shape
    qb = min(ATT_QB, seq // groups)
    per = seq // groups // qb
    grid = (heads, seq // qb)
    q_spec = pl.BlockSpec((1, qb, hd), lambda h, i, p: (h, i, 0))
    kv_spec = pl.BlockSpec((1, seq, hd), lambda h, i, p: (h, 0, 0))
    lse_spec = pl.BlockSpec((1, qb, 1), lambda h, i, p: (h, i, 0))
    o_spec = pl.BlockSpec((1, 1, qb, hd), lambda h, i, p: (i // per, h, i % per, 0))
    return pl.pallas_call(
        functools.partial(_fwd_kernel, scale),
        out_shape=(jax.ShapeDtypeStruct((groups, heads, seq // groups, hd), jnp.bfloat16),
                   jax.ShapeDtypeStruct((heads, seq, 1), jnp.float32)),
        grid_spec=pltpu.PrefetchScalarGridSpec(
            num_scalar_prefetch=1, grid=grid,
            in_specs=[q_spec, kv_spec, kv_spec],
            out_specs=[o_spec, lse_spec]),
        compiler_params=pltpu.CompilerParams(
            dimension_semantics=("arbitrary", "arbitrary"),
            vmem_limit_bytes=48 * 1024 * 1024),
        cost_estimate=pl.CostEstimate(
            flops=4 * heads * seq * seq * hd, transcendentals=heads * seq * seq,
            bytes_accessed=4 * heads * seq * hd * 2),
    )(prefix, q, k, v)


def attn_backward(prefix, q, k, v, grad_out, lse, scale, groups):
    heads, seq, hd = q.shape
    qb = min(ATT_QB, seq // groups)
    per = seq // groups // qb
    grid = (heads, seq // qb)
    q_spec = pl.BlockSpec((1, qb, hd), lambda h, i, p: (h, i, 0))
    kv_spec = pl.BlockSpec((1, seq, hd), lambda h, i, p: (h, 0, 0))
    lse_spec = pl.BlockSpec((1, qb, 1), lambda h, i, p: (h, i, 0))
    dq_spec = pl.BlockSpec((1, 1, qb, hd), lambda h, i, p: (i // per, h, i % per, 0))
    dkv_spec = pl.BlockSpec((groups, 1, seq // groups, hd), lambda h, i, p: (0, h, 0, 0))
    shape = jax.ShapeDtypeStruct((groups, heads, seq // groups, hd), jnp.bfloat16)
    return pl.pallas_call(
        functools.partial(_bwd_kernel, scale),
        out_shape=(shape, shape, shape),
        grid_spec=pltpu.PrefetchScalarGridSpec(
            num_scalar_prefetch=1, grid=grid,
            in_specs=[q_spec, kv_spec, kv_spec, q_spec, lse_spec],
            out_specs=[dq_spec, dkv_spec, dkv_spec],
            scratch_shapes=[pltpu.VMEM((seq, hd), jnp.float32),
                            pltpu.VMEM((seq, hd), jnp.float32)]),
        compiler_params=pltpu.CompilerParams(
            dimension_semantics=("arbitrary", "arbitrary"),
            vmem_limit_bytes=48 * 1024 * 1024),
        cost_estimate=pl.CostEstimate(
            flops=10 * heads * seq * seq * hd, transcendentals=heads * seq * seq,
            bytes_accessed=8 * heads * seq * hd * 2),
    )(prefix, q, k, v, grad_out, lse)


def on_device(
    tokens,
    pass_ids,
    prefix,
    cotangent,
    qkv_weight,
    out_weight,
    fc1_weight,
    fc2_weight,
    ln1_gain,
    ln1_bias,
    qv_bias,
    out_bias,
    ln2_gain,
    ln2_bias,
    fc1_bias,
    fc2_bias,
    pass_table,
):
    tp_count = lax.axis_size("tp")
    tp_rank = lax.axis_index("tp")
    local_rows = tokens.shape[0]
    seq_len = local_rows * tp_count
    cols_here = qkv_weight.shape[2]
    heads_here = cols_here // HD
    scale = HD ** (-0.5)
    prefix_len = prefix[0]
    gelu_tanh = partial(jax.nn.gelu, approximate=True)
    fsdp_count = lax.axis_size("fsdp")
    qkv_cols = lax.all_gather(qkv_weight, "fsdp", axis=1, tiled=True)
    qkv_full = qkv_cols
    hidden_here = fc1_weight.shape[1]
    qv_here = lax.dynamic_slice_in_dim(qv_bias, tp_rank * cols_here, cols_here, 1)
    one_hot = (pass_ids[:, None] == jnp.arange(NPASS, dtype=jnp.int32)[None, :]).astype(jnp.float32)
    block_in = tokens.astype(jnp.float32) + jnp.dot(
        one_hot, pass_table, precision=HIGH, preferred_element_type=jnp.float32
    )
    normed, unit_one, inv_one = norm_forward(block_in, ln1_gain, ln1_bias)
    normed_all = lax.all_gather(normed.astype(jnp.bfloat16), "tp", axis=0, tiled=True)
    shards = (out_weight, fc1_weight, fc2_weight)
    packed = jnp.concatenate([piece.reshape(-1) for piece in shards])
    packed, qkv_cols, normed_all = lax.optimization_barrier((packed, qkv_cols, normed_all))
    qkv_full = qkv_cols
    gathered = lax.all_gather(packed, "fsdp", axis=0, tiled=False)
    qkv_copies = jnp.broadcast_to(qkv_cols[None], (tp_count,) + qkv_cols.shape)
    qkv_all = lax.all_to_all(qkv_copies, "tp", 0, 0, tiled=True)
    grad_rows = lax.all_gather(cotangent, "tp", axis=0, tiled=True)
    projected = jnp.einsum("rd,kdc->krc", normed_all, qkv_full, preferred_element_type=jnp.float32)
    queries = (projected[0] + qv_here[0]).astype(jnp.bfloat16).reshape(seq_len, heads_here, HD)
    keys_all = projected[1].astype(jnp.bfloat16).reshape(seq_len, heads_here, HD)
    values_all = (projected[2] + qv_here[1]).astype(jnp.bfloat16).reshape(seq_len, heads_here, HD)
    q_heads = jnp.transpose(queries, (1, 0, 2))
    k_heads = jnp.transpose(keys_all, (1, 0, 2))
    v_heads = jnp.transpose(values_all, (1, 0, 2))
    mixed, log_mass = attn_forward(prefix, q_heads, k_heads, v_heads, scale, tp_count)
    mixed, qkv_all = lax.optimization_barrier((mixed, qkv_all))
    pieces = []
    offset = 0
    for piece in shards:
        size = piece.size
        pieces.append(gathered[:, offset : offset + size].reshape((fsdp_count,) + piece.shape))
        offset += size
    out_full = jnp.moveaxis(pieces[0], 0, 1).reshape(out_weight.shape[0], -1)
    fc1_part = pieces[1].reshape(-1, fc1_weight.shape[1])
    fc2_part = jnp.moveaxis(pieces[2], 0, 1).reshape(fc2_weight.shape[0], -1)
    out_all = lax.all_gather(out_full, "tp", axis=0, tiled=True)
    mixed, grad_rows, out_all, fc1_part, fc2_part = lax.optimization_barrier(
        (mixed, grad_rows, out_all, fc1_part, fc2_part)
    )
    mixed_rows = lax.all_to_all(mixed, "tp", 0, 0, tiled=True)
    middle = (
        block_in
        + jnp.einsum(
            "shre,shem->rm",
            mixed_rows,
            out_all.reshape(tp_count, heads_here, HD, -1),
            preferred_element_type=jnp.float32,
        )
        + out_bias
    )
    normed_two, unit_two, inv_two = norm_forward(middle, ln2_gain, ln2_bias)
    normed_two = normed_two.astype(jnp.bfloat16)
    grad_top = cotangent.astype(jnp.float32)
    fc1_bias_here = lax.dynamic_slice_in_dim(fc1_bias, tp_rank * hidden_here, hidden_here, 0)
    normed_rows = lax.all_gather(normed_two, "tp", axis=0, tiled=True)
    before = jnp.dot(normed_rows, fc1_part, preferred_element_type=jnp.float32) + fc1_bias_here
    hidden = gelu_tanh(before).astype(jnp.bfloat16)
    fc2_partial = jnp.dot(hidden, fc2_part, preferred_element_type=jnp.float32).astype(jnp.bfloat16)
    grad_hidden = matmul_nt(grad_rows, fc2_part)
    grad_before = jax.vjp(gelu_tanh, before)[1](grad_hidden)[0].astype(jnp.bfloat16)
    grad_fc1_bias = lax.dynamic_update_slice_in_dim(
        jnp.zeros(fc1_bias.shape, jnp.float32),
        jnp.sum(grad_before.astype(jnp.float32), axis=0),
        tp_rank * hidden_here,
        0,
    )
    grad_fc1 = matmul_tn(normed_rows, grad_before)
    grad_fc2 = matmul_tn(hidden, grad_rows)
    grad_normed_two = lax.psum_scatter(
        matmul_nt(grad_before, fc1_part), "tp", scatter_dimension=0, tiled=True
    )
    grad_normed_two, fc2_partial, grad_fc1, grad_fc2 = lax.optimization_barrier(
        (grad_normed_two, fc2_partial, grad_fc1, grad_fc2)
    )
    grad_fc2_bias = jnp.sum(grad_top, axis=0)
    grad_from_norm, grad_ln2_gain, grad_ln2_bias = norm_backward(
        grad_normed_two, unit_two, inv_two, ln2_gain
    )
    grad_middle = grad_top + grad_from_norm
    grad_out_bias = jnp.sum(grad_middle, axis=0)
    grad_attn_rows = lax.all_gather(grad_middle.astype(jnp.bfloat16), "tp", axis=0, tiled=True)
    fc2_partial, grad_attn_rows = lax.optimization_barrier((fc2_partial, grad_attn_rows))
    fc2_parts = lax.all_to_all(
        fc2_partial.reshape(tp_count, local_rows, -1), "tp", 0, 0, tiled=True
    )
    result = middle + jnp.sum(fc2_parts.astype(jnp.float32), axis=0) + fc2_bias
    grad_out_w = jnp.einsum(
        "thre,trm->hem",
        mixed,
        grad_attn_rows.reshape(tp_count, local_rows, -1),
        preferred_element_type=jnp.float32,
    ).reshape(cols_here, -1)
    fsdp_count = lax.axis_size("fsdp")
    dense_grads = (
        jnp.moveaxis(grad_out_w.reshape(grad_out_w.shape[0], fsdp_count, -1), 1, 0),
        grad_fc1.reshape(fsdp_count, -1, grad_fc1.shape[1]),
        jnp.moveaxis(grad_fc2.reshape(grad_fc2.shape[0], fsdp_count, -1), 1, 0),
    )
    dense_packed = jnp.concatenate([g.reshape(fsdp_count, -1) for g in dense_grads], axis=1)
    dense_summed = lax.psum_scatter(
        dense_packed.reshape(-1, grad_fc1.shape[1]), "fsdp", scatter_dimension=0, tiled=True
    ).reshape(1, -1)
    grad_mixed = (
        matmul_nt(grad_attn_rows, out_full).astype(jnp.bfloat16).reshape(seq_len, heads_here, HD)
    )
    grad_q_heads, grad_k_heads, grad_v_heads = attn_backward(
        prefix, q_heads, k_heads, v_heads, jnp.transpose(grad_mixed, (1, 0, 2)), log_mass, scale,
        tp_count,
    )
    grad_q_heads, grad_k_heads, grad_v_heads, result, dense_summed = lax.optimization_barrier(
        (grad_q_heads, grad_k_heads, grad_v_heads, result, dense_summed)
    )
    grad_kinds = (grad_q_heads, grad_k_heads, grad_v_heads)
    grad_qv_here = jnp.stack(
        [
            jnp.sum(grad_q_heads.astype(jnp.float32), axis=(0, 2)).reshape(-1),
            jnp.sum(grad_v_heads.astype(jnp.float32), axis=(0, 2)).reshape(-1),
        ],
        axis=0,
    )
    grad_qv_bias = lax.dynamic_update_slice_in_dim(
        jnp.zeros(qv_bias.shape, jnp.float32), grad_qv_here, tp_rank * cols_here, 1
    )
    normed_groups = normed_all.reshape(tp_count, local_rows, -1)
    grad_qkv_w = jnp.stack(
        [
            jnp.einsum("trd,thre->dhe", normed_groups, g, preferred_element_type=jnp.float32)
            for g in grad_kinds
        ]
    ).reshape(3, normed_all.shape[1], cols_here)
    grad_rows_kinds = [lax.all_to_all(g, "tp", 0, 0, tiled=True) for g in grad_kinds]
    qkv_split = qkv_all.reshape(tp_count, 3, qkv_all.shape[2], heads_here, HD)
    grad_normed = sum(
        jnp.einsum("shre,sdhe->rd", g, qkv_split[:, kind], preferred_element_type=jnp.float32)
        for kind, g in enumerate(grad_rows_kinds)
    )
    dense_shards = []
    offset = 0
    for g in dense_grads:
        size = g[0].size
        dense_shards.append(dense_summed[0, offset : offset + size].reshape(g.shape[1:]))
        offset += size
    out_shard, fc1_shard, fc2_shard = dense_shards
    grad_in_norm, grad_ln1_gain, grad_ln1_bias = norm_backward(
        grad_normed, unit_one, inv_one, ln1_gain
    )
    grad_input = grad_middle + grad_in_norm
    grad_table = lax.dot_general(
        one_hot,
        grad_input,
        (((0,), (0,)), ((), ())),
        precision=HIGH,
        preferred_element_type=jnp.float32,
    )
    qkv_shard = lax.psum_scatter(grad_qkv_w, "fsdp", scatter_dimension=1, tiled=True)
    summed = lax.psum(
        (
            grad_ln1_gain,
            grad_ln1_bias,
            grad_qv_bias,
            grad_out_bias,
            grad_ln2_gain,
            grad_ln2_bias,
            grad_fc1_bias,
            grad_fc2_bias,
            grad_table,
        ),
        ("fsdp", "tp"),
    )
    return (
        result.astype(jnp.bfloat16),
        grad_input,
        qkv_shard,
        out_shard,
        fc1_shard,
        fc2_shard,
        summed[0],
        summed[1],
        summed[2],
        summed[3],
        summed[4],
        summed[5],
        summed[6],
        summed[7],
        summed[8],
    )


def solution(mesh):
    placed = (
        P(("fsdp", "tp"), None),
        P(("fsdp", "tp")),
        P("fsdp"),
        P(("fsdp", "tp"), None),
        P(None, "fsdp", "tp"),
        P("tp", "fsdp"),
        P("fsdp", "tp"),
        P("tp", "fsdp"),
        P(),
        P(),
        P(),
        P(),
        P(),
        P(),
        P(),
        P(),
        P(),
    )
    return jax.shard_map(
        on_device,
        mesh=mesh,
        in_specs=placed,
        out_specs=(
            P(("fsdp", "tp"), None),
            P(("fsdp", "tp"), None),
            P(None, "fsdp", "tp"),
            P("tp", "fsdp"),
            P("fsdp", "tp"),
            P("tp", "fsdp"),
            P(),
            P(),
            P(),
            P(),
            P(),
            P(),
            P(),
            P(),
            P(),
        ),
        check_vma=False,
    )
```

```python
import functools
from functools import partial

import jax
import jax.numpy as jnp
from jax import lax
from jax.experimental import pallas as pl
from jax.experimental.pallas import tpu as pltpu
from jax.sharding import PartitionSpec as P

HD = 64
NPASS = 5
QBLOCK = 512


HIGH = lax.Precision.HIGHEST
EPS = 1e-05
NEG_FILL = -1e30


def norm_forward(rows_in, gain, shift):
    center = rows_in - jnp.mean(rows_in, axis=-1, keepdims=True)
    scale_inv = lax.rsqrt(jnp.mean(center * center, axis=-1, keepdims=True) + EPS)
    unit_rows = center * scale_inv
    return (unit_rows * gain + shift, unit_rows, scale_inv)


def norm_backward(grad_out, unit_rows, scale_inv, gain):
    grad_unit = grad_out * gain
    first_mean = jnp.mean(grad_unit, axis=-1, keepdims=True)
    second_mean = jnp.mean(grad_unit * unit_rows, axis=-1, keepdims=True)
    grad_rows = scale_inv * (grad_unit - first_mean - unit_rows * second_mean)
    return (grad_rows, jnp.sum(grad_out * unit_rows, axis=0), jnp.sum(grad_out, axis=0))


def matmul_nt(left, right):
    return lax.dot_general(
        left, right, (((1,), (1,)), ((), ())), preferred_element_type=jnp.float32
    )


def matmul_tn(left, right):
    return lax.dot_general(
        left, right, (((0,), (0,)), ((), ())), preferred_element_type=jnp.float32
    )


def block_scores(query_block, keys_all, row_start, prefix_len, scale):
    raw = (
        jnp.einsum("qhe,khe->hqk", query_block, keys_all, preferred_element_type=jnp.float32)
        * scale
    )
    row_ids = row_start + jnp.arange(query_block.shape[0], dtype=jnp.int32)
    col_ids = jnp.arange(keys_all.shape[0], dtype=jnp.int32)
    allowed = (col_ids[None, :] <= row_ids[:, None]) | (col_ids[None, :] < prefix_len)
    return jnp.where(allowed[None], raw, NEG_FILL)


ATT_QB = 256


def _mask(prefix_len, qb, rows, cols):
    row = qb * rows + lax.broadcasted_iota(jnp.int32, (rows, cols), 0)
    col = lax.broadcasted_iota(jnp.int32, (rows, cols), 1)
    return (col <= row) | (col < prefix_len)


def _nt(a, b):
    return lax.dot_general(a, b, (((1,), (1,)), ((), ())), preferred_element_type=jnp.float32)


def _tn(a, b):
    return lax.dot_general(a, b, (((0,), (0,)), ((), ())), preferred_element_type=jnp.float32)


def _fwd_kernel(scale, prefix_ref, q_ref, k_ref, v_ref, o_ref, lse_ref):
    qb = pl.program_id(1)
    q = q_ref[0]
    rows, cols = q.shape[0], k_ref.shape[1]
    scores = _nt(q, k_ref[0]) * scale
    scores = jnp.where(_mask(prefix_ref[0], qb, rows, cols), scores, NEG_FILL)
    peak = jnp.max(scores, axis=-1, keepdims=True)
    expo = jnp.exp(scores - peak)
    total = jnp.sum(expo, axis=-1, keepdims=True)
    probs_low = (expo / total).astype(jnp.bfloat16)
    out = jnp.dot(probs_low, v_ref[0], preferred_element_type=jnp.float32)
    o_ref[0, 0] = out.astype(o_ref.dtype)
    lse_ref[0] = peak + jnp.log(total)


def _bwd_kernel(scale, prefix_ref, q_ref, k_ref, v_ref, do_ref, lse_ref,
                dq_ref, dk_ref, dv_ref, dk_acc, dv_acc):
    qb = pl.program_id(1)

    @pl.when(qb == 0)
    def _():
        dk_acc[...] = jnp.zeros_like(dk_acc)
        dv_acc[...] = jnp.zeros_like(dv_acc)

    q = q_ref[0]
    k = k_ref[0]
    grad_out = do_ref[0]
    rows, cols = q.shape[0], k.shape[0]
    scores = _nt(q, k) * scale
    scores = jnp.where(_mask(prefix_ref[0], qb, rows, cols), scores, NEG_FILL)
    probs = jnp.exp(scores - lse_ref[0])
    dv_acc[...] += _tn(probs.astype(jnp.bfloat16), grad_out)
    grad_probs = _nt(grad_out, v_ref[0])
    inner = jnp.sum(probs * grad_probs, axis=-1, keepdims=True)
    grad_scores = (probs * (grad_probs - inner)).astype(jnp.bfloat16)
    dq_ref[0, 0] = (jnp.dot(grad_scores, k, preferred_element_type=jnp.float32) * scale).astype(dq_ref.dtype)
    dk_acc[...] += _tn(grad_scores, q)

    @pl.when(qb == pl.num_programs(1) - 1)
    def _():
        groups, rows, hd = dk_ref.shape[0], dk_ref.shape[2], dk_ref.shape[3]
        dk_ref[:, 0] = (dk_acc[...] * scale).astype(dk_ref.dtype).reshape(groups, rows, hd)
        dv_ref[:, 0] = dv_acc[...].astype(dv_ref.dtype).reshape(groups, rows, hd)


def attn_forward(prefix, q, k, v, scale, groups):
    heads, seq, hd = q.shape
    qb = min(ATT_QB, seq // groups)
    per = seq // groups // qb
    grid = (heads, seq // qb)
    q_spec = pl.BlockSpec((1, qb, hd), lambda h, i, p: (h, i, 0))
    kv_spec = pl.BlockSpec((1, seq, hd), lambda h, i, p: (h, 0, 0))
    lse_spec = pl.BlockSpec((1, qb, 1), lambda h, i, p: (h, i, 0))
    o_spec = pl.BlockSpec((1, 1, qb, hd), lambda h, i, p: (i // per, h, i % per, 0))
    return pl.pallas_call(
        functools.partial(_fwd_kernel, scale),
        out_shape=(jax.ShapeDtypeStruct((groups, heads, seq // groups, hd), jnp.bfloat16),
                   jax.ShapeDtypeStruct((heads, seq, 1), jnp.float32)),
        grid_spec=pltpu.PrefetchScalarGridSpec(
            num_scalar_prefetch=1, grid=grid,
            in_specs=[q_spec, kv_spec, kv_spec],
            out_specs=[o_spec, lse_spec]),
        compiler_params=pltpu.CompilerParams(
            dimension_semantics=("arbitrary", "arbitrary"),
            vmem_limit_bytes=48 * 1024 * 1024),
        cost_estimate=pl.CostEstimate(
            flops=4 * heads * seq * seq * hd, transcendentals=heads * seq * seq,
            bytes_accessed=4 * heads * seq * hd * 2),
    )(prefix, q, k, v)


def attn_backward(prefix, q, k, v, grad_out, lse, scale, groups):
    heads, seq, hd = q.shape
    qb = min(ATT_QB, seq // groups)
    per = seq // groups // qb
    grid = (heads, seq // qb)
    q_spec = pl.BlockSpec((1, qb, hd), lambda h, i, p: (h, i, 0))
    kv_spec = pl.BlockSpec((1, seq, hd), lambda h, i, p: (h, 0, 0))
    lse_spec = pl.BlockSpec((1, qb, 1), lambda h, i, p: (h, i, 0))
    dq_spec = pl.BlockSpec((1, 1, qb, hd), lambda h, i, p: (i // per, h, i % per, 0))
    dkv_spec = pl.BlockSpec((groups, 1, seq // groups, hd), lambda h, i, p: (0, h, 0, 0))
    shape = jax.ShapeDtypeStruct((groups, heads, seq // groups, hd), jnp.bfloat16)
    return pl.pallas_call(
        functools.partial(_bwd_kernel, scale),
        out_shape=(shape, shape, shape),
        grid_spec=pltpu.PrefetchScalarGridSpec(
            num_scalar_prefetch=1, grid=grid,
            in_specs=[q_spec, kv_spec, kv_spec, q_spec, lse_spec],
            out_specs=[dq_spec, dkv_spec, dkv_spec],
            scratch_shapes=[pltpu.VMEM((seq, hd), jnp.float32),
                            pltpu.VMEM((seq, hd), jnp.float32)]),
        compiler_params=pltpu.CompilerParams(
            dimension_semantics=("arbitrary", "arbitrary"),
            vmem_limit_bytes=48 * 1024 * 1024),
        cost_estimate=pl.CostEstimate(
            flops=10 * heads * seq * seq * hd, transcendentals=heads * seq * seq,
            bytes_accessed=8 * heads * seq * hd * 2),
    )(prefix, q, k, v, grad_out, lse)


def on_device(
    tokens,
    pass_ids,
    prefix,
    cotangent,
    qkv_weight,
    out_weight,
    fc1_weight,
    fc2_weight,
    ln1_gain,
    ln1_bias,
    qv_bias,
    out_bias,
    ln2_gain,
    ln2_bias,
    fc1_bias,
    fc2_bias,
    pass_table,
):
    tp_count = lax.axis_size("tp")
    tp_rank = lax.axis_index("tp")
    local_rows = tokens.shape[0]
    seq_len = local_rows * tp_count
    cols_here = qkv_weight.shape[2]
    heads_here = cols_here // HD
    scale = HD ** (-0.5)
    prefix_len = prefix[0]
    gelu_tanh = partial(jax.nn.gelu, approximate=True)
    fsdp_count = lax.axis_size("fsdp")
    qkv_cols = lax.all_gather(qkv_weight, "fsdp", axis=1, tiled=True)
    qkv_full = qkv_cols
    hidden_here = fc1_weight.shape[1]
    qv_here = lax.dynamic_slice_in_dim(qv_bias, tp_rank * cols_here, cols_here, 1)
    one_hot = (pass_ids[:, None] == jnp.arange(NPASS, dtype=jnp.int32)[None, :]).astype(jnp.float32)
    block_in = tokens.astype(jnp.float32) + jnp.dot(
        one_hot, pass_table, precision=HIGH, preferred_element_type=jnp.float32
    )
    normed, unit_one, inv_one = norm_forward(block_in, ln1_gain, ln1_bias)
    normed_all = lax.all_gather(normed.astype(jnp.bfloat16), "tp", axis=0, tiled=True)
    shards = (out_weight, fc1_weight, fc2_weight)
    packed = jnp.concatenate([piece.reshape(-1) for piece in shards])
    packed, qkv_cols, normed_all = lax.optimization_barrier((packed, qkv_cols, normed_all))
    qkv_full = qkv_cols
    gathered = lax.all_gather(packed, "fsdp", axis=0, tiled=False)
    qkv_copies = jnp.broadcast_to(qkv_cols[None], (tp_count,) + qkv_cols.shape)
    qkv_all = lax.all_to_all(qkv_copies, "tp", 0, 0, tiled=True)
    grad_rows = lax.all_gather(cotangent, "tp", axis=0, tiled=True)
    projected = jnp.einsum("rd,kdc->krc", normed_all, qkv_full, preferred_element_type=jnp.float32)
    queries = (projected[0] + qv_here[0]).astype(jnp.bfloat16).reshape(seq_len, heads_here, HD)
    keys_all = projected[1].astype(jnp.bfloat16).reshape(seq_len, heads_here, HD)
    values_all = (projected[2] + qv_here[1]).astype(jnp.bfloat16).reshape(seq_len, heads_here, HD)
    q_heads = jnp.transpose(queries, (1, 0, 2))
    k_heads = jnp.transpose(keys_all, (1, 0, 2))
    v_heads = jnp.transpose(values_all, (1, 0, 2))
    mixed, log_mass = attn_forward(prefix, q_heads, k_heads, v_heads, scale, tp_count)
    mixed, qkv_all = lax.optimization_barrier((mixed, qkv_all))
    pieces = []
    offset = 0
    for piece in shards:
        size = piece.size
        pieces.append(gathered[:, offset : offset + size].reshape((fsdp_count,) + piece.shape))
        offset += size
    out_full = jnp.moveaxis(pieces[0], 0, 1).reshape(out_weight.shape[0], -1)
    fc1_part = pieces[1].reshape(-1, fc1_weight.shape[1])
    fc2_part = jnp.moveaxis(pieces[2], 0, 1).reshape(fc2_weight.shape[0], -1)
    out_all = lax.all_gather(out_full, "tp", axis=0, tiled=True)
    mixed, grad_rows, out_all, fc1_part, fc2_part = lax.optimization_barrier(
        (mixed, grad_rows, out_all, fc1_part, fc2_part)
    )
    mixed_rows = lax.all_to_all(mixed, "tp", 0, 0, tiled=True)
    middle = (
        block_in
        + jnp.einsum(
            "shre,shem->rm",
            mixed_rows,
            out_all.reshape(tp_count, heads_here, HD, -1),
            preferred_element_type=jnp.float32,
        )
        + out_bias
    )
    normed_two, unit_two, inv_two = norm_forward(middle, ln2_gain, ln2_bias)
    normed_two = normed_two.astype(jnp.bfloat16)
    grad_top = cotangent.astype(jnp.float32)
    fc1_bias_here = lax.dynamic_slice_in_dim(fc1_bias, tp_rank * hidden_here, hidden_here, 0)
    normed_rows = lax.all_gather(normed_two, "tp", axis=0, tiled=True)
    before = jnp.dot(normed_rows, fc1_part, preferred_element_type=jnp.float32) + fc1_bias_here
    hidden = gelu_tanh(before).astype(jnp.bfloat16)
    fc2_partial = jnp.dot(hidden, fc2_part, preferred_element_type=jnp.float32).astype(jnp.bfloat16)
    grad_hidden = matmul_nt(grad_rows, fc2_part)
    grad_before = jax.vjp(gelu_tanh, before)[1](grad_hidden)[0].astype(jnp.bfloat16)
    grad_fc1_bias = lax.dynamic_update_slice_in_dim(
        jnp.zeros(fc1_bias.shape, jnp.float32),
        jnp.sum(grad_before.astype(jnp.float32), axis=0),
        tp_rank * hidden_here,
        0,
    )
    grad_fc1 = matmul_tn(normed_rows, grad_before)
    grad_fc2 = matmul_tn(hidden, grad_rows)
    grad_normed_two = lax.psum_scatter(
        matmul_nt(grad_before, fc1_part).astype(jnp.bfloat16), "tp", scatter_dimension=0, tiled=True
    ).astype(jnp.float32)
    grad_normed_two, fc2_partial, grad_fc1, grad_fc2 = lax.optimization_barrier(
        (grad_normed_two, fc2_partial, grad_fc1, grad_fc2)
    )
    grad_fc2_bias = jnp.sum(grad_top, axis=0)
    grad_from_norm, grad_ln2_gain, grad_ln2_bias = norm_backward(
        grad_normed_two, unit_two, inv_two, ln2_gain
    )
    grad_middle = grad_top + grad_from_norm
    grad_out_bias = jnp.sum(grad_middle, axis=0)
    grad_attn_rows = lax.all_gather(grad_middle.astype(jnp.bfloat16), "tp", axis=0, tiled=True)
    fc2_partial, grad_attn_rows = lax.optimization_barrier((fc2_partial, grad_attn_rows))
    fc2_parts = lax.all_to_all(
        fc2_partial.reshape(tp_count, local_rows, -1), "tp", 0, 0, tiled=True
    )
    result = middle + jnp.sum(fc2_parts.astype(jnp.float32), axis=0) + fc2_bias
    grad_out_w = jnp.einsum(
        "thre,trm->hem",
        mixed,
        grad_attn_rows.reshape(tp_count, local_rows, -1),
        preferred_element_type=jnp.float32,
    ).reshape(cols_here, -1)
    fsdp_count = lax.axis_size("fsdp")
    dense_grads = (
        jnp.moveaxis(grad_out_w.reshape(grad_out_w.shape[0], fsdp_count, -1), 1, 0),
        grad_fc1.reshape(fsdp_count, -1, grad_fc1.shape[1]),
        jnp.moveaxis(grad_fc2.reshape(grad_fc2.shape[0], fsdp_count, -1), 1, 0),
    )
    dense_packed = jnp.concatenate([g.reshape(fsdp_count, -1) for g in dense_grads], axis=1)
    dense_summed = lax.psum_scatter(
        dense_packed.reshape(-1, grad_fc1.shape[1]).astype(jnp.bfloat16),
        "fsdp",
        scatter_dimension=0,
        tiled=True,
    ).reshape(1, -1).astype(jnp.float32)
    grad_mixed = (
        matmul_nt(grad_attn_rows, out_full).astype(jnp.bfloat16).reshape(seq_len, heads_here, HD)
    )
    grad_q_heads, grad_k_heads, grad_v_heads = attn_backward(
        prefix, q_heads, k_heads, v_heads, jnp.transpose(grad_mixed, (1, 0, 2)), log_mass, scale,
        tp_count,
    )
    grad_q_heads, grad_k_heads, grad_v_heads, result, dense_summed = lax.optimization_barrier(
        (grad_q_heads, grad_k_heads, grad_v_heads, result, dense_summed)
    )
    grad_kinds = (grad_q_heads, grad_k_heads, grad_v_heads)
    grad_qv_here = jnp.stack(
        [
            jnp.sum(grad_q_heads.astype(jnp.float32), axis=(0, 2)).reshape(-1),
            jnp.sum(grad_v_heads.astype(jnp.float32), axis=(0, 2)).reshape(-1),
        ],
        axis=0,
    )
    grad_qv_bias = lax.dynamic_update_slice_in_dim(
        jnp.zeros(qv_bias.shape, jnp.float32), grad_qv_here, tp_rank * cols_here, 1
    )
    normed_groups = normed_all.reshape(tp_count, local_rows, -1)
    grad_qkv_w = jnp.stack(
        [
            jnp.einsum("trd,thre->dhe", normed_groups, g, preferred_element_type=jnp.float32)
            for g in grad_kinds
        ]
    ).reshape(3, normed_all.shape[1], cols_here)
    grad_rows_kinds = [lax.all_to_all(g, "tp", 0, 0, tiled=True) for g in grad_kinds]
    qkv_split = qkv_all.reshape(tp_count, 3, qkv_all.shape[2], heads_here, HD)
    grad_normed = sum(
        jnp.einsum("shre,sdhe->rd", g, qkv_split[:, kind], preferred_element_type=jnp.float32)
        for kind, g in enumerate(grad_rows_kinds)
    )
    dense_shards = []
    offset = 0
    for g in dense_grads:
        size = g[0].size
        dense_shards.append(dense_summed[0, offset : offset + size].reshape(g.shape[1:]))
        offset += size
    out_shard, fc1_shard, fc2_shard = dense_shards
    grad_in_norm, grad_ln1_gain, grad_ln1_bias = norm_backward(
        grad_normed, unit_one, inv_one, ln1_gain
    )
    grad_input = grad_middle + grad_in_norm
    grad_table = lax.dot_general(
        one_hot,
        grad_input,
        (((0,), (0,)), ((), ())),
        precision=HIGH,
        preferred_element_type=jnp.float32,
    )
    qkv_shard = lax.psum_scatter(grad_qkv_w, "fsdp", scatter_dimension=1, tiled=True)
    summed = lax.psum(
        (
            grad_ln1_gain,
            grad_ln1_bias,
            grad_qv_bias,
            grad_out_bias,
            grad_ln2_gain,
            grad_ln2_bias,
            grad_fc1_bias,
            grad_fc2_bias,
            grad_table,
        ),
        ("fsdp", "tp"),
    )
    return (
        result.astype(jnp.bfloat16),
        grad_input,
        qkv_shard,
        out_shard,
        fc1_shard,
        fc2_shard,
        summed[0],
        summed[1],
        summed[2],
        summed[3],
        summed[4],
        summed[5],
        summed[6],
        summed[7],
        summed[8],
    )


def solution(mesh):
    placed = (
        P(("fsdp", "tp"), None),
        P(("fsdp", "tp")),
        P("fsdp"),
        P(("fsdp", "tp"), None),
        P(None, "fsdp", "tp"),
        P("tp", "fsdp"),
        P("fsdp", "tp"),
        P("tp", "fsdp"),
        P(),
        P(),
        P(),
        P(),
        P(),
        P(),
        P(),
        P(),
        P(),
    )
    return jax.shard_map(
        on_device,
        mesh=mesh,
        in_specs=placed,
        out_specs=(
            P(("fsdp", "tp"), None),
            P(("fsdp", "tp"), None),
            P(None, "fsdp", "tp"),
            P("tp", "fsdp"),
            P("fsdp", "tp"),
            P("tp", "fsdp"),
            P(),
            P(),
            P(),
            P(),
            P(),
            P(),
            P(),
            P(),
            P(),
        ),
        check_vma=False,
    )
```

```python
import functools
from functools import partial

import jax
import jax.numpy as jnp
from jax import lax
from jax.experimental import pallas as pl
from jax.experimental.pallas import tpu as pltpu
from jax.sharding import PartitionSpec as P

HD = 64
NPASS = 5
QBLOCK = 512


HIGH = lax.Precision.HIGHEST
EPS = 1e-05
NEG_FILL = -1e30


def norm_forward(rows_in, gain, shift):
    center = rows_in - jnp.mean(rows_in, axis=-1, keepdims=True)
    scale_inv = lax.rsqrt(jnp.mean(center * center, axis=-1, keepdims=True) + EPS)
    unit_rows = center * scale_inv
    return (unit_rows * gain + shift, unit_rows, scale_inv)


def norm_backward(grad_out, unit_rows, scale_inv, gain):
    grad_unit = grad_out * gain
    first_mean = jnp.mean(grad_unit, axis=-1, keepdims=True)
    second_mean = jnp.mean(grad_unit * unit_rows, axis=-1, keepdims=True)
    grad_rows = scale_inv * (grad_unit - first_mean - unit_rows * second_mean)
    return (grad_rows, jnp.sum(grad_out * unit_rows, axis=0), jnp.sum(grad_out, axis=0))


def matmul_nt(left, right):
    return lax.dot_general(
        left, right, (((1,), (1,)), ((), ())), preferred_element_type=jnp.float32
    )


def matmul_tn(left, right):
    return lax.dot_general(
        left, right, (((0,), (0,)), ((), ())), preferred_element_type=jnp.float32
    )


def block_scores(query_block, keys_all, row_start, prefix_len, scale):
    raw = (
        jnp.einsum("qhe,khe->hqk", query_block, keys_all, preferred_element_type=jnp.float32)
        * scale
    )
    row_ids = row_start + jnp.arange(query_block.shape[0], dtype=jnp.int32)
    col_ids = jnp.arange(keys_all.shape[0], dtype=jnp.int32)
    allowed = (col_ids[None, :] <= row_ids[:, None]) | (col_ids[None, :] < prefix_len)
    return jnp.where(allowed[None], raw, NEG_FILL)


ATT_QB = 256


def _mask(prefix_len, qb, rows, cols):
    row = qb * rows + lax.broadcasted_iota(jnp.int32, (rows, cols), 0)
    col = lax.broadcasted_iota(jnp.int32, (rows, cols), 1)
    return (col <= row) | (col < prefix_len)


def _nt(a, b):
    return lax.dot_general(a, b, (((1,), (1,)), ((), ())), preferred_element_type=jnp.float32)


def _tn(a, b):
    return lax.dot_general(a, b, (((0,), (0,)), ((), ())), preferred_element_type=jnp.float32)


def _fwd_kernel(scale, prefix_ref, q_ref, k_ref, v_ref, o_ref, lse_ref):
    qb = pl.program_id(1)
    q = q_ref[0]
    rows, cols = q.shape[0], k_ref.shape[1]
    scores = _nt(q, k_ref[0]) * scale
    scores = jnp.where(_mask(prefix_ref[0], qb, rows, cols), scores, NEG_FILL)
    peak = jnp.max(scores, axis=-1, keepdims=True)
    expo = jnp.exp(scores - peak)
    total = jnp.sum(expo, axis=-1, keepdims=True)
    probs_low = (expo / total).astype(jnp.bfloat16)
    out = jnp.dot(probs_low, v_ref[0], preferred_element_type=jnp.float32)
    o_ref[0, 0] = out.astype(o_ref.dtype)
    lse_ref[0] = peak + jnp.log(total)


def _bwd_kernel(scale, prefix_ref, q_ref, k_ref, v_ref, do_ref, lse_ref,
                g_ref, dk_acc, dv_acc):
    qb = pl.program_id(1)

    @pl.when(qb == 0)
    def _():
        dk_acc[...] = jnp.zeros_like(dk_acc)
        dv_acc[...] = jnp.zeros_like(dv_acc)

    q = q_ref[0]
    k = k_ref[0]
    grad_out = do_ref[0]
    rows, cols = q.shape[0], k.shape[0]
    scores = _nt(q, k) * scale
    scores = jnp.where(_mask(prefix_ref[0], qb, rows, cols), scores, NEG_FILL)
    probs = jnp.exp(scores - lse_ref[0])
    dv_acc[...] += _tn(probs.astype(jnp.bfloat16), grad_out)
    grad_probs = _nt(grad_out, v_ref[0])
    inner = jnp.sum(probs * grad_probs, axis=-1, keepdims=True)
    grad_scores = (probs * (grad_probs - inner)).astype(jnp.bfloat16)
    groups, rows_per = g_ref.shape[0], g_ref.shape[3]
    per = rows_per // rows
    start = pl.multiple_of((qb % per) * rows, rows)
    g_ref[qb // per, 0, 0, pl.ds(start, rows), :] = (
        jnp.dot(grad_scores, k, preferred_element_type=jnp.float32) * scale
    ).astype(g_ref.dtype)
    dk_acc[...] += _tn(grad_scores, q)

    @pl.when(qb == pl.num_programs(1) - 1)
    def _():
        hd = g_ref.shape[4]
        g_ref[:, 1, 0] = (dk_acc[...] * scale).astype(g_ref.dtype).reshape(groups, rows_per, hd)
        g_ref[:, 2, 0] = dv_acc[...].astype(g_ref.dtype).reshape(groups, rows_per, hd)


def attn_forward(prefix, q, k, v, scale, groups):
    heads, seq, hd = q.shape
    qb = min(ATT_QB, seq // groups)
    per = seq // groups // qb
    grid = (heads, seq // qb)
    q_spec = pl.BlockSpec((1, qb, hd), lambda h, i, p: (h, i, 0))
    kv_spec = pl.BlockSpec((1, seq, hd), lambda h, i, p: (h, 0, 0))
    lse_spec = pl.BlockSpec((1, qb, 1), lambda h, i, p: (h, i, 0))
    o_spec = pl.BlockSpec((1, 1, qb, hd), lambda h, i, p: (i // per, h, i % per, 0))
    return pl.pallas_call(
        functools.partial(_fwd_kernel, scale),
        out_shape=(jax.ShapeDtypeStruct((groups, heads, seq // groups, hd), jnp.bfloat16),
                   jax.ShapeDtypeStruct((heads, seq, 1), jnp.float32)),
        grid_spec=pltpu.PrefetchScalarGridSpec(
            num_scalar_prefetch=1, grid=grid,
            in_specs=[q_spec, kv_spec, kv_spec],
            out_specs=[o_spec, lse_spec]),
        compiler_params=pltpu.CompilerParams(
            dimension_semantics=("arbitrary", "arbitrary"),
            vmem_limit_bytes=48 * 1024 * 1024),
        cost_estimate=pl.CostEstimate(
            flops=4 * heads * seq * seq * hd, transcendentals=heads * seq * seq,
            bytes_accessed=4 * heads * seq * hd * 2),
    )(prefix, q, k, v)


def attn_backward(prefix, q, k, v, grad_out, lse, scale, groups):
    heads, seq, hd = q.shape
    qb = min(ATT_QB, seq // groups)
    per = seq // groups // qb
    grid = (heads, seq // qb)
    q_spec = pl.BlockSpec((1, qb, hd), lambda h, i, p: (h, i, 0))
    kv_spec = pl.BlockSpec((1, seq, hd), lambda h, i, p: (h, 0, 0))
    lse_spec = pl.BlockSpec((1, qb, 1), lambda h, i, p: (h, i, 0))
    g_spec = pl.BlockSpec((groups, 3, 1, seq // groups, hd), lambda h, i, p: (0, 0, h, 0, 0))
    shape = jax.ShapeDtypeStruct((groups, 3, heads, seq // groups, hd), jnp.bfloat16)
    return pl.pallas_call(
        functools.partial(_bwd_kernel, scale),
        out_shape=shape,
        grid_spec=pltpu.PrefetchScalarGridSpec(
            num_scalar_prefetch=1, grid=grid,
            in_specs=[q_spec, kv_spec, kv_spec, q_spec, lse_spec],
            out_specs=g_spec,
            scratch_shapes=[pltpu.VMEM((seq, hd), jnp.float32),
                            pltpu.VMEM((seq, hd), jnp.float32)]),
        compiler_params=pltpu.CompilerParams(
            dimension_semantics=("arbitrary", "arbitrary"),
            vmem_limit_bytes=48 * 1024 * 1024),
        cost_estimate=pl.CostEstimate(
            flops=10 * heads * seq * seq * hd, transcendentals=heads * seq * seq,
            bytes_accessed=8 * heads * seq * hd * 2),
    )(prefix, q, k, v, grad_out, lse)


def on_device(
    tokens,
    pass_ids,
    prefix,
    cotangent,
    qkv_weight,
    out_weight,
    fc1_weight,
    fc2_weight,
    ln1_gain,
    ln1_bias,
    qv_bias,
    out_bias,
    ln2_gain,
    ln2_bias,
    fc1_bias,
    fc2_bias,
    pass_table,
):
    tp_count = lax.axis_size("tp")
    tp_rank = lax.axis_index("tp")
    local_rows = tokens.shape[0]
    seq_len = local_rows * tp_count
    cols_here = qkv_weight.shape[2]
    heads_here = cols_here // HD
    scale = HD ** (-0.5)
    prefix_len = prefix[0]
    gelu_tanh = partial(jax.nn.gelu, approximate=True)
    fsdp_count = lax.axis_size("fsdp")
    qkv_cols = lax.all_gather(qkv_weight, "fsdp", axis=1, tiled=True)
    qkv_full = qkv_cols
    hidden_here = fc1_weight.shape[1]
    qv_here = lax.dynamic_slice_in_dim(qv_bias, tp_rank * cols_here, cols_here, 1)
    one_hot = (pass_ids[:, None] == jnp.arange(NPASS, dtype=jnp.int32)[None, :]).astype(jnp.float32)
    block_in = tokens.astype(jnp.float32) + jnp.dot(
        one_hot, pass_table, precision=HIGH, preferred_element_type=jnp.float32
    )
    normed, unit_one, inv_one = norm_forward(block_in, ln1_gain, ln1_bias)
    normed_all = lax.all_gather(normed.astype(jnp.bfloat16), "tp", axis=0, tiled=True)
    shards = (out_weight, fc1_weight, fc2_weight)
    packed = jnp.concatenate([piece.reshape(-1) for piece in shards])
    packed, qkv_cols, normed_all = lax.optimization_barrier((packed, qkv_cols, normed_all))
    qkv_full = qkv_cols
    gathered = lax.all_gather(packed, "fsdp", axis=0, tiled=False)
    qkv_copies = jnp.broadcast_to(qkv_cols[None], (tp_count,) + qkv_cols.shape)
    qkv_all = lax.all_to_all(qkv_copies, "tp", 0, 0, tiled=True)
    grad_rows = lax.all_gather(cotangent, "tp", axis=0, tiled=True)
    projected = jnp.einsum("rd,kdc->krc", normed_all, qkv_full, preferred_element_type=jnp.float32)
    queries = (projected[0] + qv_here[0]).astype(jnp.bfloat16).reshape(seq_len, heads_here, HD)
    keys_all = projected[1].astype(jnp.bfloat16).reshape(seq_len, heads_here, HD)
    values_all = (projected[2] + qv_here[1]).astype(jnp.bfloat16).reshape(seq_len, heads_here, HD)
    q_heads = jnp.transpose(queries, (1, 0, 2))
    k_heads = jnp.transpose(keys_all, (1, 0, 2))
    v_heads = jnp.transpose(values_all, (1, 0, 2))
    mixed, log_mass = attn_forward(prefix, q_heads, k_heads, v_heads, scale, tp_count)
    mixed, qkv_all = lax.optimization_barrier((mixed, qkv_all))
    pieces = []
    offset = 0
    for piece in shards:
        size = piece.size
        pieces.append(gathered[:, offset : offset + size].reshape((fsdp_count,) + piece.shape))
        offset += size
    out_full = jnp.moveaxis(pieces[0], 0, 1).reshape(out_weight.shape[0], -1)
    fc1_part = pieces[1].reshape(-1, fc1_weight.shape[1])
    fc2_part = jnp.moveaxis(pieces[2], 0, 1).reshape(fc2_weight.shape[0], -1)
    out_all = lax.all_gather(out_full, "tp", axis=0, tiled=True)
    mixed, grad_rows, out_all, fc1_part, fc2_part = lax.optimization_barrier(
        (mixed, grad_rows, out_all, fc1_part, fc2_part)
    )
    mixed_rows = lax.all_to_all(mixed, "tp", 0, 0, tiled=True)
    middle = (
        block_in
        + jnp.einsum(
            "shre,shem->rm",
            mixed_rows,
            out_all.reshape(tp_count, heads_here, HD, -1),
            preferred_element_type=jnp.float32,
        )
        + out_bias
    )
    normed_two, unit_two, inv_two = norm_forward(middle, ln2_gain, ln2_bias)
    normed_two = normed_two.astype(jnp.bfloat16)
    grad_top = cotangent.astype(jnp.float32)
    fc1_bias_here = lax.dynamic_slice_in_dim(fc1_bias, tp_rank * hidden_here, hidden_here, 0)
    normed_rows = lax.all_gather(normed_two, "tp", axis=0, tiled=True)
    before = jnp.dot(normed_rows, fc1_part, preferred_element_type=jnp.float32) + fc1_bias_here
    hidden = gelu_tanh(before).astype(jnp.bfloat16)
    fc2_partial = jnp.dot(hidden, fc2_part, preferred_element_type=jnp.float32).astype(jnp.bfloat16)
    grad_hidden = matmul_nt(grad_rows, fc2_part)
    grad_before = jax.vjp(gelu_tanh, before)[1](grad_hidden)[0].astype(jnp.bfloat16)
    grad_fc1_bias = lax.dynamic_update_slice_in_dim(
        jnp.zeros(fc1_bias.shape, jnp.float32),
        jnp.sum(grad_before.astype(jnp.float32), axis=0),
        tp_rank * hidden_here,
        0,
    )
    grad_fc1 = matmul_tn(normed_rows, grad_before)
    grad_fc2 = matmul_tn(hidden, grad_rows)
    grad_normed_two = lax.psum_scatter(
        matmul_nt(grad_before, fc1_part).astype(jnp.bfloat16), "tp", scatter_dimension=0, tiled=True
    ).astype(jnp.float32)
    grad_normed_two, fc2_partial, grad_fc1, grad_fc2 = lax.optimization_barrier(
        (grad_normed_two, fc2_partial, grad_fc1, grad_fc2)
    )
    grad_fc2_bias = jnp.sum(grad_top, axis=0)
    grad_from_norm, grad_ln2_gain, grad_ln2_bias = norm_backward(
        grad_normed_two, unit_two, inv_two, ln2_gain
    )
    grad_middle = grad_top + grad_from_norm
    grad_out_bias = jnp.sum(grad_middle, axis=0)
    grad_attn_rows = lax.all_gather(grad_middle.astype(jnp.bfloat16), "tp", axis=0, tiled=True)
    fc2_partial, grad_attn_rows = lax.optimization_barrier((fc2_partial, grad_attn_rows))
    fc2_parts = lax.all_to_all(
        fc2_partial.reshape(tp_count, local_rows, -1), "tp", 0, 0, tiled=True
    )
    result = middle + jnp.sum(fc2_parts.astype(jnp.float32), axis=0) + fc2_bias
    grad_out_w = jnp.einsum(
        "thre,trm->hem",
        mixed,
        grad_attn_rows.reshape(tp_count, local_rows, -1),
        preferred_element_type=jnp.float32,
    ).reshape(cols_here, -1)
    fsdp_count = lax.axis_size("fsdp")
    dense_grads = (
        jnp.moveaxis(grad_out_w.reshape(grad_out_w.shape[0], fsdp_count, -1), 1, 0),
        grad_fc1.reshape(fsdp_count, -1, grad_fc1.shape[1]),
        jnp.moveaxis(grad_fc2.reshape(grad_fc2.shape[0], fsdp_count, -1), 1, 0),
    )
    dense_packed = jnp.concatenate([g.reshape(fsdp_count, -1) for g in dense_grads], axis=1)
    dense_summed = lax.psum_scatter(
        dense_packed.reshape(-1, grad_fc1.shape[1]).astype(jnp.bfloat16),
        "fsdp",
        scatter_dimension=0,
        tiled=True,
    ).reshape(1, -1).astype(jnp.float32)
    grad_mixed = (
        matmul_nt(grad_attn_rows, out_full).astype(jnp.bfloat16).reshape(seq_len, heads_here, HD)
    )
    grad_all = attn_backward(
        prefix, q_heads, k_heads, v_heads, jnp.transpose(grad_mixed, (1, 0, 2)), log_mass, scale,
        tp_count,
    )
    grad_all, result, dense_summed = lax.optimization_barrier((grad_all, result, dense_summed))
    grad_q_heads, grad_v_heads = grad_all[:, 0], grad_all[:, 2]
    grad_qv_here = jnp.stack(
        [
            jnp.sum(grad_q_heads.astype(jnp.float32), axis=(0, 2)).reshape(-1),
            jnp.sum(grad_v_heads.astype(jnp.float32), axis=(0, 2)).reshape(-1),
        ],
        axis=0,
    )
    grad_qv_bias = lax.dynamic_update_slice_in_dim(
        jnp.zeros(qv_bias.shape, jnp.float32), grad_qv_here, tp_rank * cols_here, 1
    )
    normed_groups = normed_all.reshape(tp_count, local_rows, -1)
    grad_qkv_w = jnp.einsum(
        "trd,tkhre->kdhe", normed_groups, grad_all, preferred_element_type=jnp.float32
    ).reshape(3, normed_all.shape[1], cols_here)
    grad_rows_all = lax.all_to_all(grad_all, "tp", 0, 0, tiled=True)
    qkv_split = qkv_all.reshape(tp_count, 3, qkv_all.shape[2], heads_here, HD)
    grad_normed = jnp.einsum(
        "skhre,skdhe->rd", grad_rows_all, qkv_split, preferred_element_type=jnp.float32
    )
    dense_shards = []
    offset = 0
    for g in dense_grads:
        size = g[0].size
        dense_shards.append(dense_summed[0, offset : offset + size].reshape(g.shape[1:]))
        offset += size
    out_shard, fc1_shard, fc2_shard = dense_shards
    grad_in_norm, grad_ln1_gain, grad_ln1_bias = norm_backward(
        grad_normed, unit_one, inv_one, ln1_gain
    )
    grad_input = grad_middle + grad_in_norm
    grad_table = lax.dot_general(
        one_hot,
        grad_input,
        (((0,), (0,)), ((), ())),
        precision=HIGH,
        preferred_element_type=jnp.float32,
    )
    qkv_shard = lax.psum_scatter(grad_qkv_w, "fsdp", scatter_dimension=1, tiled=True)
    summed = lax.psum(
        (
            grad_ln1_gain,
            grad_ln1_bias,
            grad_qv_bias,
            grad_out_bias,
            grad_ln2_gain,
            grad_ln2_bias,
            grad_fc1_bias,
            grad_fc2_bias,
            grad_table,
        ),
        ("fsdp", "tp"),
    )
    return (
        result.astype(jnp.bfloat16),
        grad_input,
        qkv_shard,
        out_shard,
        fc1_shard,
        fc2_shard,
        summed[0],
        summed[1],
        summed[2],
        summed[3],
        summed[4],
        summed[5],
        summed[6],
        summed[7],
        summed[8],
    )


def solution(mesh):
    placed = (
        P(("fsdp", "tp"), None),
        P(("fsdp", "tp")),
        P("fsdp"),
        P(("fsdp", "tp"), None),
        P(None, "fsdp", "tp"),
        P("tp", "fsdp"),
        P("fsdp", "tp"),
        P("tp", "fsdp"),
        P(),
        P(),
        P(),
        P(),
        P(),
        P(),
        P(),
        P(),
        P(),
    )
    return jax.shard_map(
        on_device,
        mesh=mesh,
        in_specs=placed,
        out_specs=(
            P(("fsdp", "tp"), None),
            P(("fsdp", "tp"), None),
            P(None, "fsdp", "tp"),
            P("tp", "fsdp"),
            P("fsdp", "tp"),
            P("tp", "fsdp"),
            P(),
            P(),
            P(),
            P(),
            P(),
            P(),
            P(),
            P(),
            P(),
        ),
        check_vma=False,
    )
```

```python
import functools
from functools import partial

import jax
import jax.numpy as jnp
from jax import lax
from jax.experimental import pallas as pl
from jax.experimental.pallas import tpu as pltpu
from jax.sharding import PartitionSpec as P

HD = 64
NPASS = 5
QBLOCK = 512


HIGH = lax.Precision.HIGHEST
EPS = 1e-05
NEG_FILL = -1e30


def norm_forward(rows_in, gain, shift):
    center = rows_in - jnp.mean(rows_in, axis=-1, keepdims=True)
    scale_inv = lax.rsqrt(jnp.mean(center * center, axis=-1, keepdims=True) + EPS)
    unit_rows = center * scale_inv
    return (unit_rows * gain + shift, unit_rows, scale_inv)


def norm_backward(grad_out, unit_rows, scale_inv, gain):
    grad_unit = grad_out * gain
    first_mean = jnp.mean(grad_unit, axis=-1, keepdims=True)
    second_mean = jnp.mean(grad_unit * unit_rows, axis=-1, keepdims=True)
    grad_rows = scale_inv * (grad_unit - first_mean - unit_rows * second_mean)
    return (grad_rows, jnp.sum(grad_out * unit_rows, axis=0), jnp.sum(grad_out, axis=0))


def matmul_nt(left, right):
    return lax.dot_general(
        left, right, (((1,), (1,)), ((), ())), preferred_element_type=jnp.float32
    )


def matmul_tn(left, right):
    return lax.dot_general(
        left, right, (((0,), (0,)), ((), ())), preferred_element_type=jnp.float32
    )


def block_scores(query_block, keys_all, row_start, prefix_len, scale):
    raw = (
        jnp.einsum("qhe,khe->hqk", query_block, keys_all, preferred_element_type=jnp.float32)
        * scale
    )
    row_ids = row_start + jnp.arange(query_block.shape[0], dtype=jnp.int32)
    col_ids = jnp.arange(keys_all.shape[0], dtype=jnp.int32)
    allowed = (col_ids[None, :] <= row_ids[:, None]) | (col_ids[None, :] < prefix_len)
    return jnp.where(allowed[None], raw, NEG_FILL)


ATT_QB = 256


def _mask(prefix_len, qb, rows, cols):
    row = qb * rows + lax.broadcasted_iota(jnp.int32, (rows, cols), 0)
    col = lax.broadcasted_iota(jnp.int32, (rows, cols), 1)
    return (col <= row) | (col < prefix_len)


def _nt(a, b):
    return lax.dot_general(a, b, (((1,), (1,)), ((), ())), preferred_element_type=jnp.float32)


def _tn(a, b):
    return lax.dot_general(a, b, (((0,), (0,)), ((), ())), preferred_element_type=jnp.float32)


def _fwd_kernel(scale, prefix_ref, q_ref, k_ref, v_ref, o_ref, lse_ref):
    qb = pl.program_id(1)
    q = q_ref[0]
    rows, cols = q.shape[0], k_ref.shape[1]
    scores = _nt(q, k_ref[0]) * scale
    scores = jnp.where(_mask(prefix_ref[0], qb, rows, cols), scores, NEG_FILL)
    peak = jnp.max(scores, axis=-1, keepdims=True)
    expo = jnp.exp(scores - peak)
    total = jnp.sum(expo, axis=-1, keepdims=True)
    probs_low = (expo / total).astype(jnp.bfloat16)
    out = jnp.dot(probs_low, v_ref[0], preferred_element_type=jnp.float32)
    o_ref[0, 0] = out.astype(o_ref.dtype)
    lse_ref[0] = peak + jnp.log(total)


def _bwd_kernel(scale, prefix_ref, q_ref, k_ref, v_ref, do_ref, lse_ref,
                g_ref, dk_acc, dv_acc):
    qb = pl.program_id(1)

    @pl.when(qb == 0)
    def _():
        dk_acc[...] = jnp.zeros_like(dk_acc)
        dv_acc[...] = jnp.zeros_like(dv_acc)

    q = q_ref[0]
    k = k_ref[0]
    grad_out = do_ref[0]
    rows, cols = q.shape[0], k.shape[0]
    scores = _nt(q, k) * scale
    scores = jnp.where(_mask(prefix_ref[0], qb, rows, cols), scores, NEG_FILL)
    probs = jnp.exp(scores - lse_ref[0])
    dv_acc[...] += _tn(probs.astype(jnp.bfloat16), grad_out)
    grad_probs = _nt(grad_out, v_ref[0])
    inner = jnp.sum(probs * grad_probs, axis=-1, keepdims=True)
    grad_scores = (probs * (grad_probs - inner)).astype(jnp.bfloat16)
    groups, rows_per = g_ref.shape[0], g_ref.shape[3]
    per = rows_per // rows
    start = pl.multiple_of((qb % per) * rows, rows)
    g_ref[qb // per, 0, 0, pl.ds(start, rows), :] = (
        jnp.dot(grad_scores, k, preferred_element_type=jnp.float32) * scale
    ).astype(g_ref.dtype)
    dk_acc[...] += _tn(grad_scores, q)

    @pl.when(qb == pl.num_programs(1) - 1)
    def _():
        hd = g_ref.shape[4]
        g_ref[:, 1, 0] = (dk_acc[...] * scale).astype(g_ref.dtype).reshape(groups, rows_per, hd)
        g_ref[:, 2, 0] = dv_acc[...].astype(g_ref.dtype).reshape(groups, rows_per, hd)


def attn_forward(prefix, q, k, v, scale, groups):
    heads, seq, hd = q.shape
    qb = min(ATT_QB, seq // groups)
    per = seq // groups // qb
    grid = (heads, seq // qb)
    q_spec = pl.BlockSpec((1, qb, hd), lambda h, i, p: (h, i, 0))
    kv_spec = pl.BlockSpec((1, seq, hd), lambda h, i, p: (h, 0, 0))
    lse_spec = pl.BlockSpec((1, qb, 1), lambda h, i, p: (h, i, 0))
    o_spec = pl.BlockSpec((1, 1, qb, hd), lambda h, i, p: (i // per, h, i % per, 0))
    return pl.pallas_call(
        functools.partial(_fwd_kernel, scale),
        out_shape=(jax.ShapeDtypeStruct((groups, heads, seq // groups, hd), jnp.bfloat16),
                   jax.ShapeDtypeStruct((heads, seq, 1), jnp.float32)),
        grid_spec=pltpu.PrefetchScalarGridSpec(
            num_scalar_prefetch=1, grid=grid,
            in_specs=[q_spec, kv_spec, kv_spec],
            out_specs=[o_spec, lse_spec]),
        compiler_params=pltpu.CompilerParams(
            dimension_semantics=("arbitrary", "arbitrary"),
            vmem_limit_bytes=48 * 1024 * 1024),
        cost_estimate=pl.CostEstimate(
            flops=4 * heads * seq * seq * hd, transcendentals=heads * seq * seq,
            bytes_accessed=4 * heads * seq * hd * 2),
    )(prefix, q, k, v)


def attn_backward(prefix, q, k, v, grad_out, lse, scale, groups):
    heads, seq, hd = q.shape
    qb = min(ATT_QB, seq // groups)
    per = seq // groups // qb
    grid = (heads, seq // qb)
    q_spec = pl.BlockSpec((1, qb, hd), lambda h, i, p: (h, i, 0))
    kv_spec = pl.BlockSpec((1, seq, hd), lambda h, i, p: (h, 0, 0))
    lse_spec = pl.BlockSpec((1, qb, 1), lambda h, i, p: (h, i, 0))
    g_spec = pl.BlockSpec((groups, 3, 1, seq // groups, hd), lambda h, i, p: (0, 0, h, 0, 0))
    shape = jax.ShapeDtypeStruct((groups, 3, heads, seq // groups, hd), jnp.bfloat16)
    return pl.pallas_call(
        functools.partial(_bwd_kernel, scale),
        out_shape=shape,
        grid_spec=pltpu.PrefetchScalarGridSpec(
            num_scalar_prefetch=1, grid=grid,
            in_specs=[q_spec, kv_spec, kv_spec, q_spec, lse_spec],
            out_specs=g_spec,
            scratch_shapes=[pltpu.VMEM((seq, hd), jnp.float32),
                            pltpu.VMEM((seq, hd), jnp.float32)]),
        compiler_params=pltpu.CompilerParams(
            dimension_semantics=("arbitrary", "arbitrary"),
            vmem_limit_bytes=48 * 1024 * 1024),
        cost_estimate=pl.CostEstimate(
            flops=10 * heads * seq * seq * hd, transcendentals=heads * seq * seq,
            bytes_accessed=8 * heads * seq * hd * 2),
    )(prefix, q, k, v, grad_out, lse)


def on_device(
    tokens,
    pass_ids,
    prefix,
    cotangent,
    qkv_weight,
    out_weight,
    fc1_weight,
    fc2_weight,
    ln1_gain,
    ln1_bias,
    qv_bias,
    out_bias,
    ln2_gain,
    ln2_bias,
    fc1_bias,
    fc2_bias,
    pass_table,
):
    tp_count = lax.axis_size("tp")
    tp_rank = lax.axis_index("tp")
    local_rows = tokens.shape[0]
    seq_len = local_rows * tp_count
    cols_here = qkv_weight.shape[2]
    heads_here = cols_here // HD
    scale = HD ** (-0.5)
    prefix_len = prefix[0]
    gelu_tanh = partial(jax.nn.gelu, approximate=True)
    fsdp_count = lax.axis_size("fsdp")
    qkv_cols = lax.all_gather(qkv_weight, "fsdp", axis=1, tiled=True)
    qkv_full = qkv_cols
    hidden_here = fc1_weight.shape[1]
    qv_here = lax.dynamic_slice_in_dim(qv_bias, tp_rank * cols_here, cols_here, 1)
    one_hot = (pass_ids[:, None] == jnp.arange(NPASS, dtype=jnp.int32)[None, :]).astype(jnp.float32)
    block_in = tokens.astype(jnp.float32) + jnp.dot(
        one_hot, pass_table, precision=HIGH, preferred_element_type=jnp.float32
    )
    normed, unit_one, inv_one = norm_forward(block_in, ln1_gain, ln1_bias)
    normed_all = lax.all_gather(normed.astype(jnp.bfloat16), "tp", axis=0, tiled=True)
    shards = (out_weight, fc1_weight, fc2_weight)
    packed = jnp.concatenate([piece.reshape(-1) for piece in shards])
    packed, qkv_cols, normed_all = lax.optimization_barrier((packed, qkv_cols, normed_all))
    qkv_full = qkv_cols
    gathered = lax.all_gather(packed, "fsdp", axis=0, tiled=False)
    qkv_copies = jnp.broadcast_to(qkv_cols[None], (tp_count,) + qkv_cols.shape)
    qkv_all = lax.all_to_all(qkv_copies, "tp", 0, 0, tiled=True)
    grad_rows = lax.all_gather(cotangent, "tp", axis=0, tiled=True)
    projected = jnp.einsum("rd,kdc->krc", normed_all, qkv_full, preferred_element_type=jnp.float32)
    queries = (projected[0] + qv_here[0]).astype(jnp.bfloat16).reshape(seq_len, heads_here, HD)
    keys_all = projected[1].astype(jnp.bfloat16).reshape(seq_len, heads_here, HD)
    values_all = (projected[2] + qv_here[1]).astype(jnp.bfloat16).reshape(seq_len, heads_here, HD)
    q_heads = jnp.transpose(queries, (1, 0, 2))
    k_heads = jnp.transpose(keys_all, (1, 0, 2))
    v_heads = jnp.transpose(values_all, (1, 0, 2))
    mixed, log_mass = attn_forward(prefix, q_heads, k_heads, v_heads, scale, tp_count)
    mixed, qkv_all = lax.optimization_barrier((mixed, qkv_all))
    pieces = []
    offset = 0
    for piece in shards:
        size = piece.size
        pieces.append(gathered[:, offset : offset + size].reshape((fsdp_count,) + piece.shape))
        offset += size
    out_full = jnp.moveaxis(pieces[0], 0, 1).reshape(out_weight.shape[0], -1)
    fc1_part = pieces[1].reshape(-1, fc1_weight.shape[1])
    fc2_part = jnp.moveaxis(pieces[2], 0, 1).reshape(fc2_weight.shape[0], -1)
    out_all = lax.all_gather(out_full, "tp", axis=0, tiled=True)
    mixed, grad_rows, out_all, fc1_part, fc2_part = lax.optimization_barrier(
        (mixed, grad_rows, out_all, fc1_part, fc2_part)
    )
    mixed_rows = lax.all_to_all(mixed, "tp", 0, 0, tiled=True)
    middle = (
        block_in
        + jnp.einsum(
            "shre,shem->rm",
            mixed_rows,
            out_all.reshape(tp_count, heads_here, HD, -1),
            preferred_element_type=jnp.float32,
        )
        + out_bias
    )
    normed_two, unit_two, inv_two = norm_forward(middle, ln2_gain, ln2_bias)
    normed_two = normed_two.astype(jnp.bfloat16)
    grad_top = cotangent.astype(jnp.float32)
    fc1_bias_here = lax.dynamic_slice_in_dim(fc1_bias, tp_rank * hidden_here, hidden_here, 0)
    normed_rows = lax.all_gather(normed_two, "tp", axis=0, tiled=True)
    before = jnp.dot(normed_rows, fc1_part, preferred_element_type=jnp.float32) + fc1_bias_here
    hidden = gelu_tanh(before).astype(jnp.bfloat16)
    fc2_partial = jnp.dot(hidden, fc2_part, preferred_element_type=jnp.float32).astype(jnp.bfloat16)
    grad_hidden = matmul_nt(grad_rows, fc2_part)
    grad_before = jax.vjp(gelu_tanh, before)[1](grad_hidden)[0].astype(jnp.bfloat16)
    grad_fc1_bias = lax.dynamic_update_slice_in_dim(
        jnp.zeros(fc1_bias.shape, jnp.float32),
        jnp.sum(grad_before.astype(jnp.float32), axis=0),
        tp_rank * hidden_here,
        0,
    )
    grad_fc1 = matmul_tn(normed_rows, grad_before)
    grad_fc2 = matmul_tn(hidden, grad_rows)
    grad_normed_two = lax.psum_scatter(
        matmul_nt(grad_before, fc1_part).astype(jnp.bfloat16), "tp", scatter_dimension=0, tiled=True
    ).astype(jnp.float32)
    grad_normed_two, fc2_partial, grad_fc1, grad_fc2 = lax.optimization_barrier(
        (grad_normed_two, fc2_partial, grad_fc1, grad_fc2)
    )
    grad_fc2_bias = jnp.sum(grad_top, axis=0)
    grad_from_norm, grad_ln2_gain, grad_ln2_bias = norm_backward(
        grad_normed_two, unit_two, inv_two, ln2_gain
    )
    grad_middle = grad_top + grad_from_norm
    grad_out_bias = jnp.sum(grad_middle, axis=0)
    grad_attn_rows = lax.all_gather(grad_middle.astype(jnp.bfloat16), "tp", axis=0, tiled=True)
    fc2_partial, grad_attn_rows = lax.optimization_barrier((fc2_partial, grad_attn_rows))
    fc2_parts = lax.all_to_all(
        fc2_partial.reshape(tp_count, local_rows, -1), "tp", 0, 0, tiled=True
    )
    result = middle + jnp.sum(fc2_parts.astype(jnp.float32), axis=0) + fc2_bias
    grad_out_w = jnp.einsum(
        "thre,trm->hem",
        mixed,
        grad_attn_rows.reshape(tp_count, local_rows, -1),
        preferred_element_type=jnp.float32,
    ).reshape(cols_here, -1)
    fsdp_count = lax.axis_size("fsdp")
    dense_grads = (
        jnp.moveaxis(grad_out_w.reshape(grad_out_w.shape[0], fsdp_count, -1), 1, 0),
        grad_fc1.reshape(fsdp_count, -1, grad_fc1.shape[1]),
        jnp.moveaxis(grad_fc2.reshape(grad_fc2.shape[0], fsdp_count, -1), 1, 0),
    )
    dense_packed = jnp.concatenate([g.reshape(fsdp_count, -1) for g in dense_grads], axis=1)
    dense_summed = lax.psum_scatter(
        dense_packed.reshape(-1, grad_fc1.shape[1]).astype(jnp.bfloat16),
        "fsdp",
        scatter_dimension=0,
        tiled=True,
    ).reshape(1, -1).astype(jnp.float32)
    grad_mixed = (
        matmul_nt(grad_attn_rows, out_full).astype(jnp.bfloat16).reshape(seq_len, heads_here, HD)
    )
    grad_all = attn_backward(
        prefix, q_heads, k_heads, v_heads, jnp.transpose(grad_mixed, (1, 0, 2)), log_mass, scale,
        tp_count,
    )
    grad_all, result, dense_summed = lax.optimization_barrier((grad_all, result, dense_summed))
    grad_q_heads, grad_v_heads = grad_all[:, 0], grad_all[:, 2]
    grad_qv_here = jnp.stack(
        [
            jnp.sum(grad_q_heads.astype(jnp.float32), axis=(0, 2)).reshape(-1),
            jnp.sum(grad_v_heads.astype(jnp.float32), axis=(0, 2)).reshape(-1),
        ],
        axis=0,
    )
    grad_qv_bias = lax.dynamic_update_slice_in_dim(
        jnp.zeros(qv_bias.shape, jnp.float32), grad_qv_here, tp_rank * cols_here, 1
    )
    normed_groups = normed_all.reshape(tp_count, local_rows, -1)
    grad_qkv_w = jnp.einsum(
        "trd,tkhre->kdhe", normed_groups, grad_all, preferred_element_type=jnp.float32
    ).reshape(3, normed_all.shape[1], cols_here)
    grad_rows_all = lax.all_to_all(grad_all, "tp", 0, 0, tiled=True)
    qkv_split = qkv_all.reshape(tp_count, 3, qkv_all.shape[2], heads_here, HD)
    grad_normed = jnp.einsum(
        "skhre,skdhe->rd", grad_rows_all, qkv_split, preferred_element_type=jnp.float32
    )
    dense_shards = []
    offset = 0
    for g in dense_grads:
        size = g[0].size
        dense_shards.append(dense_summed[0, offset : offset + size].reshape(g.shape[1:]))
        offset += size
    out_shard, fc1_shard, fc2_shard = dense_shards
    grad_in_norm, grad_ln1_gain, grad_ln1_bias = norm_backward(
        grad_normed, unit_one, inv_one, ln1_gain
    )
    grad_input = grad_middle + grad_in_norm
    grad_table = lax.dot_general(
        one_hot,
        grad_input,
        (((0,), (0,)), ((), ())),
        precision=HIGH,
        preferred_element_type=jnp.float32,
    )
    qkv_shard = lax.psum_scatter(grad_qkv_w, "fsdp", scatter_dimension=1, tiled=True)
    summed = lax.psum(
        (
            grad_ln1_gain,
            grad_ln1_bias,
            grad_qv_bias,
            grad_out_bias,
            grad_ln2_gain,
            grad_ln2_bias,
            grad_fc1_bias,
            grad_fc2_bias,
            grad_table,
        ),
        "fsdp",
    )
    summed = lax.psum(summed, "tp")
    return (
        result.astype(jnp.bfloat16),
        grad_input,
        qkv_shard,
        out_shard,
        fc1_shard,
        fc2_shard,
        summed[0],
        summed[1],
        summed[2],
        summed[3],
        summed[4],
        summed[5],
        summed[6],
        summed[7],
        summed[8],
    )


def solution(mesh):
    placed = (
        P(("fsdp", "tp"), None),
        P(("fsdp", "tp")),
        P("fsdp"),
        P(("fsdp", "tp"), None),
        P(None, "fsdp", "tp"),
        P("tp", "fsdp"),
        P("fsdp", "tp"),
        P("tp", "fsdp"),
        P(),
        P(),
        P(),
        P(),
        P(),
        P(),
        P(),
        P(),
        P(),
    )
    return jax.shard_map(
        on_device,
        mesh=mesh,
        in_specs=placed,
        out_specs=(
            P(("fsdp", "tp"), None),
            P(("fsdp", "tp"), None),
            P(None, "fsdp", "tp"),
            P("tp", "fsdp"),
            P("fsdp", "tp"),
            P("tp", "fsdp"),
            P(),
            P(),
            P(),
            P(),
            P(),
            P(),
            P(),
            P(),
            P(),
        ),
        check_vma=False,
    )
```

```python
import functools
from functools import partial

import jax
import jax.numpy as jnp
from jax import lax
from jax.experimental import pallas as pl
from jax.experimental.pallas import tpu as pltpu
from jax.sharding import PartitionSpec as P

HD = 64
NPASS = 5
QBLOCK = 512


HIGH = lax.Precision.HIGHEST
EPS = 1e-05
NEG_FILL = -1e30


def norm_forward(rows_in, gain, shift):
    center = rows_in - jnp.mean(rows_in, axis=-1, keepdims=True)
    scale_inv = lax.rsqrt(jnp.mean(center * center, axis=-1, keepdims=True) + EPS)
    unit_rows = center * scale_inv
    return (unit_rows * gain + shift, unit_rows, scale_inv)


def norm_backward(grad_out, unit_rows, scale_inv, gain):
    grad_unit = grad_out * gain
    first_mean = jnp.mean(grad_unit, axis=-1, keepdims=True)
    second_mean = jnp.mean(grad_unit * unit_rows, axis=-1, keepdims=True)
    grad_rows = scale_inv * (grad_unit - first_mean - unit_rows * second_mean)
    return (grad_rows, jnp.sum(grad_out * unit_rows, axis=0), jnp.sum(grad_out, axis=0))


def matmul_nt(left, right):
    return lax.dot_general(
        left, right, (((1,), (1,)), ((), ())), preferred_element_type=jnp.float32
    )


def matmul_tn(left, right):
    return lax.dot_general(
        left, right, (((0,), (0,)), ((), ())), preferred_element_type=jnp.float32
    )


def block_scores(query_block, keys_all, row_start, prefix_len, scale):
    raw = (
        jnp.einsum("qhe,khe->hqk", query_block, keys_all, preferred_element_type=jnp.float32)
        * scale
    )
    row_ids = row_start + jnp.arange(query_block.shape[0], dtype=jnp.int32)
    col_ids = jnp.arange(keys_all.shape[0], dtype=jnp.int32)
    allowed = (col_ids[None, :] <= row_ids[:, None]) | (col_ids[None, :] < prefix_len)
    return jnp.where(allowed[None], raw, NEG_FILL)


ATT_QB = 512


def _mask(prefix_len, qb, rows, cols):
    row = qb * rows + lax.broadcasted_iota(jnp.int32, (rows, cols), 0)
    col = lax.broadcasted_iota(jnp.int32, (rows, cols), 1)
    return (col <= row) | (col < prefix_len)


def _nt(a, b):
    return lax.dot_general(a, b, (((1,), (1,)), ((), ())), preferred_element_type=jnp.float32)


def _tn(a, b):
    return lax.dot_general(a, b, (((0,), (0,)), ((), ())), preferred_element_type=jnp.float32)


def _fwd_kernel(scale, prefix_ref, q_ref, k_ref, v_ref, o_ref, lse_ref):
    qb = pl.program_id(1)
    q = q_ref[0]
    rows, cols = q.shape[0], k_ref.shape[1]
    scores = _nt(q, k_ref[0]) * scale
    scores = jnp.where(_mask(prefix_ref[0], qb, rows, cols), scores, NEG_FILL)
    peak = jnp.max(scores, axis=-1, keepdims=True)
    expo = jnp.exp(scores - peak)
    total = jnp.sum(expo, axis=-1, keepdims=True)
    probs_low = (expo / total).astype(jnp.bfloat16)
    out = jnp.dot(probs_low, v_ref[0], preferred_element_type=jnp.float32)
    o_ref[0, 0] = out.astype(o_ref.dtype)
    lse_ref[0] = peak + jnp.log(total)


def _bwd_kernel(scale, prefix_ref, q_ref, k_ref, v_ref, do_ref, lse_ref,
                g_ref, dk_acc, dv_acc):
    qb = pl.program_id(1)

    @pl.when(qb == 0)
    def _():
        dk_acc[...] = jnp.zeros_like(dk_acc)
        dv_acc[...] = jnp.zeros_like(dv_acc)

    q = q_ref[0]
    k = k_ref[0]
    grad_out = do_ref[0]
    rows, cols = q.shape[0], k.shape[0]
    scores = _nt(q, k) * scale
    scores = jnp.where(_mask(prefix_ref[0], qb, rows, cols), scores, NEG_FILL)
    probs = jnp.exp(scores - lse_ref[0])
    dv_acc[...] += _tn(probs.astype(jnp.bfloat16), grad_out)
    grad_probs = _nt(grad_out, v_ref[0])
    inner = jnp.sum(probs * grad_probs, axis=-1, keepdims=True)
    grad_scores = (probs * (grad_probs - inner)).astype(jnp.bfloat16)
    groups, rows_per = g_ref.shape[0], g_ref.shape[3]
    per = rows_per // rows
    start = pl.multiple_of((qb % per) * rows, rows)
    g_ref[qb // per, 0, 0, pl.ds(start, rows), :] = (
        jnp.dot(grad_scores, k, preferred_element_type=jnp.float32) * scale
    ).astype(g_ref.dtype)
    dk_acc[...] += _tn(grad_scores, q)

    @pl.when(qb == pl.num_programs(1) - 1)
    def _():
        hd = g_ref.shape[4]
        g_ref[:, 1, 0] = (dk_acc[...] * scale).astype(g_ref.dtype).reshape(groups, rows_per, hd)
        g_ref[:, 2, 0] = dv_acc[...].astype(g_ref.dtype).reshape(groups, rows_per, hd)


def attn_forward(prefix, q, k, v, scale, groups):
    heads, seq, hd = q.shape
    qb = min(ATT_QB, seq // groups)
    per = seq // groups // qb
    grid = (heads, seq // qb)
    q_spec = pl.BlockSpec((1, qb, hd), lambda h, i, p: (h, i, 0))
    kv_spec = pl.BlockSpec((1, seq, hd), lambda h, i, p: (h, 0, 0))
    lse_spec = pl.BlockSpec((1, qb, 1), lambda h, i, p: (h, i, 0))
    o_spec = pl.BlockSpec((1, 1, qb, hd), lambda h, i, p: (i // per, h, i % per, 0))
    return pl.pallas_call(
        functools.partial(_fwd_kernel, scale),
        out_shape=(jax.ShapeDtypeStruct((groups, heads, seq // groups, hd), jnp.bfloat16),
                   jax.ShapeDtypeStruct((heads, seq, 1), jnp.float32)),
        grid_spec=pltpu.PrefetchScalarGridSpec(
            num_scalar_prefetch=1, grid=grid,
            in_specs=[q_spec, kv_spec, kv_spec],
            out_specs=[o_spec, lse_spec]),
        compiler_params=pltpu.CompilerParams(
            dimension_semantics=("arbitrary", "arbitrary"),
            vmem_limit_bytes=48 * 1024 * 1024),
        cost_estimate=pl.CostEstimate(
            flops=4 * heads * seq * seq * hd, transcendentals=heads * seq * seq,
            bytes_accessed=4 * heads * seq * hd * 2),
    )(prefix, q, k, v)


def attn_backward(prefix, q, k, v, grad_out, lse, scale, groups):
    heads, seq, hd = q.shape
    qb = min(ATT_QB, seq // groups)
    per = seq // groups // qb
    grid = (heads, seq // qb)
    q_spec = pl.BlockSpec((1, qb, hd), lambda h, i, p: (h, i, 0))
    kv_spec = pl.BlockSpec((1, seq, hd), lambda h, i, p: (h, 0, 0))
    lse_spec = pl.BlockSpec((1, qb, 1), lambda h, i, p: (h, i, 0))
    g_spec = pl.BlockSpec((groups, 3, 1, seq // groups, hd), lambda h, i, p: (0, 0, h, 0, 0))
    shape = jax.ShapeDtypeStruct((groups, 3, heads, seq // groups, hd), jnp.bfloat16)
    return pl.pallas_call(
        functools.partial(_bwd_kernel, scale),
        out_shape=shape,
        grid_spec=pltpu.PrefetchScalarGridSpec(
            num_scalar_prefetch=1, grid=grid,
            in_specs=[q_spec, kv_spec, kv_spec, q_spec, lse_spec],
            out_specs=g_spec,
            scratch_shapes=[pltpu.VMEM((seq, hd), jnp.float32),
                            pltpu.VMEM((seq, hd), jnp.float32)]),
        compiler_params=pltpu.CompilerParams(
            dimension_semantics=("arbitrary", "arbitrary"),
            vmem_limit_bytes=48 * 1024 * 1024),
        cost_estimate=pl.CostEstimate(
            flops=10 * heads * seq * seq * hd, transcendentals=heads * seq * seq,
            bytes_accessed=8 * heads * seq * hd * 2),
    )(prefix, q, k, v, grad_out, lse)


def on_device(
    tokens,
    pass_ids,
    prefix,
    cotangent,
    qkv_weight,
    out_weight,
    fc1_weight,
    fc2_weight,
    ln1_gain,
    ln1_bias,
    qv_bias,
    out_bias,
    ln2_gain,
    ln2_bias,
    fc1_bias,
    fc2_bias,
    pass_table,
):
    tp_count = lax.axis_size("tp")
    tp_rank = lax.axis_index("tp")
    local_rows = tokens.shape[0]
    seq_len = local_rows * tp_count
    cols_here = qkv_weight.shape[2]
    heads_here = cols_here // HD
    scale = HD ** (-0.5)
    prefix_len = prefix[0]
    gelu_tanh = partial(jax.nn.gelu, approximate=True)
    fsdp_count = lax.axis_size("fsdp")
    qkv_cols = lax.all_gather(qkv_weight, "fsdp", axis=1, tiled=True)
    qkv_full = qkv_cols
    hidden_here = fc1_weight.shape[1]
    qv_here = lax.dynamic_slice_in_dim(qv_bias, tp_rank * cols_here, cols_here, 1)
    one_hot = (pass_ids[:, None] == jnp.arange(NPASS, dtype=jnp.int32)[None, :]).astype(jnp.float32)
    block_in = tokens.astype(jnp.float32) + jnp.dot(
        one_hot, pass_table, precision=HIGH, preferred_element_type=jnp.float32
    )
    normed, unit_one, inv_one = norm_forward(block_in, ln1_gain, ln1_bias)
    normed_all = lax.all_gather(normed.astype(jnp.bfloat16), "tp", axis=0, tiled=True)
    shards = (out_weight, fc1_weight, fc2_weight)
    packed = jnp.concatenate([piece.reshape(-1) for piece in shards])
    packed, qkv_cols, normed_all = lax.optimization_barrier((packed, qkv_cols, normed_all))
    qkv_full = qkv_cols
    gathered = lax.all_gather(packed, "fsdp", axis=0, tiled=False)
    qkv_copies = jnp.broadcast_to(qkv_cols[None], (tp_count,) + qkv_cols.shape)
    qkv_all = lax.all_to_all(qkv_copies, "tp", 0, 0, tiled=True)
    grad_rows = lax.all_gather(cotangent, "tp", axis=0, tiled=True)
    projected = jnp.einsum("rd,kdc->krc", normed_all, qkv_full, preferred_element_type=jnp.float32)
    queries = (projected[0] + qv_here[0]).astype(jnp.bfloat16).reshape(seq_len, heads_here, HD)
    keys_all = projected[1].astype(jnp.bfloat16).reshape(seq_len, heads_here, HD)
    values_all = (projected[2] + qv_here[1]).astype(jnp.bfloat16).reshape(seq_len, heads_here, HD)
    q_heads = jnp.transpose(queries, (1, 0, 2))
    k_heads = jnp.transpose(keys_all, (1, 0, 2))
    v_heads = jnp.transpose(values_all, (1, 0, 2))
    mixed, log_mass = attn_forward(prefix, q_heads, k_heads, v_heads, scale, tp_count)
    mixed, qkv_all = lax.optimization_barrier((mixed, qkv_all))
    pieces = []
    offset = 0
    for piece in shards:
        size = piece.size
        pieces.append(gathered[:, offset : offset + size].reshape((fsdp_count,) + piece.shape))
        offset += size
    out_full = jnp.moveaxis(pieces[0], 0, 1).reshape(out_weight.shape[0], -1)
    fc1_part = pieces[1].reshape(-1, fc1_weight.shape[1])
    fc2_part = jnp.moveaxis(pieces[2], 0, 1).reshape(fc2_weight.shape[0], -1)
    out_all = lax.all_gather(out_full, "tp", axis=0, tiled=True)
    mixed, grad_rows, out_all, fc1_part, fc2_part = lax.optimization_barrier(
        (mixed, grad_rows, out_all, fc1_part, fc2_part)
    )
    mixed_rows = lax.all_to_all(mixed, "tp", 0, 0, tiled=True)
    middle = (
        block_in
        + jnp.einsum(
            "shre,shem->rm",
            mixed_rows,
            out_all.reshape(tp_count, heads_here, HD, -1),
            preferred_element_type=jnp.float32,
        )
        + out_bias
    )
    normed_two, unit_two, inv_two = norm_forward(middle, ln2_gain, ln2_bias)
    normed_two = normed_two.astype(jnp.bfloat16)
    grad_top = cotangent.astype(jnp.float32)
    fc1_bias_here = lax.dynamic_slice_in_dim(fc1_bias, tp_rank * hidden_here, hidden_here, 0)
    normed_rows = lax.all_gather(normed_two, "tp", axis=0, tiled=True)
    before = jnp.dot(normed_rows, fc1_part, preferred_element_type=jnp.float32) + fc1_bias_here
    hidden = gelu_tanh(before).astype(jnp.bfloat16)
    fc2_partial = jnp.dot(hidden, fc2_part, preferred_element_type=jnp.float32).astype(jnp.bfloat16)
    grad_hidden = matmul_nt(grad_rows, fc2_part)
    grad_before = jax.vjp(gelu_tanh, before)[1](grad_hidden)[0].astype(jnp.bfloat16)
    grad_fc1_bias = lax.dynamic_update_slice_in_dim(
        jnp.zeros(fc1_bias.shape, jnp.float32),
        jnp.sum(grad_before.astype(jnp.float32), axis=0),
        tp_rank * hidden_here,
        0,
    )
    grad_fc1 = matmul_tn(normed_rows, grad_before)
    grad_fc2 = matmul_tn(hidden, grad_rows)
    grad_normed_two = lax.psum_scatter(
        matmul_nt(grad_before, fc1_part).astype(jnp.bfloat16), "tp", scatter_dimension=0, tiled=True
    ).astype(jnp.float32)
    grad_normed_two, fc2_partial, grad_fc1, grad_fc2 = lax.optimization_barrier(
        (grad_normed_two, fc2_partial, grad_fc1, grad_fc2)
    )
    grad_fc2_bias = jnp.sum(grad_top, axis=0)
    grad_from_norm, grad_ln2_gain, grad_ln2_bias = norm_backward(
        grad_normed_two, unit_two, inv_two, ln2_gain
    )
    grad_middle = grad_top + grad_from_norm
    grad_out_bias = jnp.sum(grad_middle, axis=0)
    grad_attn_rows = lax.all_gather(grad_middle.astype(jnp.bfloat16), "tp", axis=0, tiled=True)
    fc2_partial, grad_attn_rows = lax.optimization_barrier((fc2_partial, grad_attn_rows))
    fc2_parts = lax.all_to_all(
        fc2_partial.reshape(tp_count, local_rows, -1), "tp", 0, 0, tiled=True
    )
    result = middle + jnp.sum(fc2_parts.astype(jnp.float32), axis=0) + fc2_bias
    grad_out_w = jnp.einsum(
        "thre,trm->hem",
        mixed,
        grad_attn_rows.reshape(tp_count, local_rows, -1),
        preferred_element_type=jnp.float32,
    ).reshape(cols_here, -1)
    fsdp_count = lax.axis_size("fsdp")
    dense_grads = (
        jnp.moveaxis(grad_out_w.reshape(grad_out_w.shape[0], fsdp_count, -1), 1, 0),
        grad_fc1.reshape(fsdp_count, -1, grad_fc1.shape[1]),
        jnp.moveaxis(grad_fc2.reshape(grad_fc2.shape[0], fsdp_count, -1), 1, 0),
    )
    dense_packed = jnp.concatenate([g.reshape(fsdp_count, -1) for g in dense_grads], axis=1)
    dense_summed = lax.psum_scatter(
        dense_packed.reshape(-1, grad_fc1.shape[1]).astype(jnp.bfloat16),
        "fsdp",
        scatter_dimension=0,
        tiled=True,
    ).reshape(1, -1).astype(jnp.float32)
    grad_mixed = (
        matmul_nt(grad_attn_rows, out_full).astype(jnp.bfloat16).reshape(seq_len, heads_here, HD)
    )
    grad_all = attn_backward(
        prefix, q_heads, k_heads, v_heads, jnp.transpose(grad_mixed, (1, 0, 2)), log_mass, scale,
        tp_count,
    )
    grad_all, result, dense_summed = lax.optimization_barrier((grad_all, result, dense_summed))
    grad_q_heads, grad_v_heads = grad_all[:, 0], grad_all[:, 2]
    grad_qv_here = jnp.stack(
        [
            jnp.sum(grad_q_heads.astype(jnp.float32), axis=(0, 2)).reshape(-1),
            jnp.sum(grad_v_heads.astype(jnp.float32), axis=(0, 2)).reshape(-1),
        ],
        axis=0,
    )
    grad_qv_bias = lax.dynamic_update_slice_in_dim(
        jnp.zeros(qv_bias.shape, jnp.float32), grad_qv_here, tp_rank * cols_here, 1
    )
    normed_groups = normed_all.reshape(tp_count, local_rows, -1)
    grad_qkv_w = jnp.einsum(
        "trd,tkhre->kdhe", normed_groups, grad_all, preferred_element_type=jnp.float32
    ).reshape(3, normed_all.shape[1], cols_here)
    grad_rows_all = lax.all_to_all(grad_all, "tp", 0, 0, tiled=True)
    qkv_split = qkv_all.reshape(tp_count, 3, qkv_all.shape[2], heads_here, HD)
    grad_normed = jnp.einsum(
        "skhre,skdhe->rd", grad_rows_all, qkv_split, preferred_element_type=jnp.float32
    )
    dense_shards = []
    offset = 0
    for g in dense_grads:
        size = g[0].size
        dense_shards.append(dense_summed[0, offset : offset + size].reshape(g.shape[1:]))
        offset += size
    out_shard, fc1_shard, fc2_shard = dense_shards
    grad_in_norm, grad_ln1_gain, grad_ln1_bias = norm_backward(
        grad_normed, unit_one, inv_one, ln1_gain
    )
    grad_input = grad_middle + grad_in_norm
    grad_table = lax.dot_general(
        one_hot,
        grad_input,
        (((0,), (0,)), ((), ())),
        precision=HIGH,
        preferred_element_type=jnp.float32,
    )
    qkv_shard = lax.psum_scatter(grad_qkv_w, "fsdp", scatter_dimension=1, tiled=True)
    summed = lax.psum(
        (
            grad_ln1_gain,
            grad_ln1_bias,
            grad_qv_bias,
            grad_out_bias,
            grad_ln2_gain,
            grad_ln2_bias,
            grad_fc1_bias,
            grad_fc2_bias,
            grad_table,
        ),
        ("fsdp", "tp"),
    )
    return (
        result.astype(jnp.bfloat16),
        grad_input,
        qkv_shard,
        out_shard,
        fc1_shard,
        fc2_shard,
        summed[0],
        summed[1],
        summed[2],
        summed[3],
        summed[4],
        summed[5],
        summed[6],
        summed[7],
        summed[8],
    )


def solution(mesh):
    placed = (
        P(("fsdp", "tp"), None),
        P(("fsdp", "tp")),
        P("fsdp"),
        P(("fsdp", "tp"), None),
        P(None, "fsdp", "tp"),
        P("tp", "fsdp"),
        P("fsdp", "tp"),
        P("tp", "fsdp"),
        P(),
        P(),
        P(),
        P(),
        P(),
        P(),
        P(),
        P(),
        P(),
    )
    return jax.shard_map(
        on_device,
        mesh=mesh,
        in_specs=placed,
        out_specs=(
            P(("fsdp", "tp"), None),
            P(("fsdp", "tp"), None),
            P(None, "fsdp", "tp"),
            P("tp", "fsdp"),
            P("fsdp", "tp"),
            P("tp", "fsdp"),
            P(),
            P(),
            P(),
            P(),
            P(),
            P(),
            P(),
            P(),
            P(),
        ),
        check_vma=False,
    )
```

```python
import functools
from functools import partial

import jax
import jax.numpy as jnp
from jax import lax
from jax.experimental import pallas as pl
from jax.experimental.pallas import tpu as pltpu
from jax.sharding import PartitionSpec as P

HD = 64
NPASS = 5
QBLOCK = 512


HIGH = lax.Precision.HIGHEST
EPS = 1e-05
NEG_FILL = -1e30


def norm_forward(rows_in, gain, shift):
    center = rows_in - jnp.mean(rows_in, axis=-1, keepdims=True)
    scale_inv = lax.rsqrt(jnp.mean(center * center, axis=-1, keepdims=True) + EPS)
    unit_rows = center * scale_inv
    return (unit_rows * gain + shift, unit_rows, scale_inv)


def norm_backward(grad_out, unit_rows, scale_inv, gain):
    grad_unit = grad_out * gain
    first_mean = jnp.mean(grad_unit, axis=-1, keepdims=True)
    second_mean = jnp.mean(grad_unit * unit_rows, axis=-1, keepdims=True)
    grad_rows = scale_inv * (grad_unit - first_mean - unit_rows * second_mean)
    return (grad_rows, jnp.sum(grad_out * unit_rows, axis=0), jnp.sum(grad_out, axis=0))


def matmul_nt(left, right):
    return lax.dot_general(
        left, right, (((1,), (1,)), ((), ())), preferred_element_type=jnp.float32
    )


def matmul_tn(left, right):
    return lax.dot_general(
        left, right, (((0,), (0,)), ((), ())), preferred_element_type=jnp.float32
    )


def block_scores(query_block, keys_all, row_start, prefix_len, scale):
    raw = (
        jnp.einsum("qhe,khe->hqk", query_block, keys_all, preferred_element_type=jnp.float32)
        * scale
    )
    row_ids = row_start + jnp.arange(query_block.shape[0], dtype=jnp.int32)
    col_ids = jnp.arange(keys_all.shape[0], dtype=jnp.int32)
    allowed = (col_ids[None, :] <= row_ids[:, None]) | (col_ids[None, :] < prefix_len)
    return jnp.where(allowed[None], raw, NEG_FILL)


ATT_QB = 256
ATT_QB_BACK = 512


def _mask(prefix_len, qb, rows, cols):
    row = qb * rows + lax.broadcasted_iota(jnp.int32, (rows, cols), 0)
    col = lax.broadcasted_iota(jnp.int32, (rows, cols), 1)
    return (col <= row) | (col < prefix_len)


def _nt(a, b):
    return lax.dot_general(a, b, (((1,), (1,)), ((), ())), preferred_element_type=jnp.float32)


def _tn(a, b):
    return lax.dot_general(a, b, (((0,), (0,)), ((), ())), preferred_element_type=jnp.float32)


def _fwd_kernel(scale, prefix_ref, q_ref, k_ref, v_ref, o_ref, lse_ref):
    qb = pl.program_id(1)
    q = q_ref[0]
    rows, cols = q.shape[0], k_ref.shape[1]
    scores = _nt(q, k_ref[0]) * scale
    scores = jnp.where(_mask(prefix_ref[0], qb, rows, cols), scores, NEG_FILL)
    peak = jnp.max(scores, axis=-1, keepdims=True)
    expo = jnp.exp(scores - peak)
    total = jnp.sum(expo, axis=-1, keepdims=True)
    probs_low = (expo / total).astype(jnp.bfloat16)
    out = jnp.dot(probs_low, v_ref[0], preferred_element_type=jnp.float32)
    o_ref[0, 0] = out.astype(o_ref.dtype)
    lse_ref[0] = peak + jnp.log(total)


def _bwd_kernel(scale, prefix_ref, q_ref, k_ref, v_ref, do_ref, lse_ref,
                g_ref, dk_acc, dv_acc):
    qb = pl.program_id(1)

    @pl.when(qb == 0)
    def _():
        dk_acc[...] = jnp.zeros_like(dk_acc)
        dv_acc[...] = jnp.zeros_like(dv_acc)

    q = q_ref[0]
    k = k_ref[0]
    grad_out = do_ref[0]
    rows, cols = q.shape[0], k.shape[0]
    scores = _nt(q, k) * scale
    scores = jnp.where(_mask(prefix_ref[0], qb, rows, cols), scores, NEG_FILL)
    probs = jnp.exp(scores - lse_ref[0])
    dv_acc[...] += _tn(probs.astype(jnp.bfloat16), grad_out)
    grad_probs = _nt(grad_out, v_ref[0])
    inner = jnp.sum(probs * grad_probs, axis=-1, keepdims=True)
    grad_scores = (probs * (grad_probs - inner)).astype(jnp.bfloat16)
    groups, rows_per = g_ref.shape[0], g_ref.shape[3]
    per = rows_per // rows
    start = pl.multiple_of((qb % per) * rows, rows)
    g_ref[qb // per, 0, 0, pl.ds(start, rows), :] = (
        jnp.dot(grad_scores, k, preferred_element_type=jnp.float32) * scale
    ).astype(g_ref.dtype)
    dk_acc[...] += _tn(grad_scores, q)

    @pl.when(qb == pl.num_programs(1) - 1)
    def _():
        hd = g_ref.shape[4]
        g_ref[:, 1, 0] = (dk_acc[...] * scale).astype(g_ref.dtype).reshape(groups, rows_per, hd)
        g_ref[:, 2, 0] = dv_acc[...].astype(g_ref.dtype).reshape(groups, rows_per, hd)


def attn_forward(prefix, q, k, v, scale, groups):
    heads, seq, hd = q.shape
    qb = min(ATT_QB, seq // groups)
    per = seq // groups // qb
    grid = (heads, seq // qb)
    q_spec = pl.BlockSpec((1, qb, hd), lambda h, i, p: (h, i, 0))
    kv_spec = pl.BlockSpec((1, seq, hd), lambda h, i, p: (h, 0, 0))
    lse_spec = pl.BlockSpec((1, qb, 1), lambda h, i, p: (h, i, 0))
    o_spec = pl.BlockSpec((1, 1, qb, hd), lambda h, i, p: (i // per, h, i % per, 0))
    return pl.pallas_call(
        functools.partial(_fwd_kernel, scale),
        out_shape=(jax.ShapeDtypeStruct((groups, heads, seq // groups, hd), jnp.bfloat16),
                   jax.ShapeDtypeStruct((heads, seq, 1), jnp.float32)),
        grid_spec=pltpu.PrefetchScalarGridSpec(
            num_scalar_prefetch=1, grid=grid,
            in_specs=[q_spec, kv_spec, kv_spec],
            out_specs=[o_spec, lse_spec]),
        compiler_params=pltpu.CompilerParams(
            dimension_semantics=("arbitrary", "arbitrary"),
            vmem_limit_bytes=48 * 1024 * 1024),
        cost_estimate=pl.CostEstimate(
            flops=4 * heads * seq * seq * hd, transcendentals=heads * seq * seq,
            bytes_accessed=4 * heads * seq * hd * 2),
    )(prefix, q, k, v)


def attn_backward(prefix, q, k, v, grad_out, lse, scale, groups):
    heads, seq, hd = q.shape
    qb = min(ATT_QB_BACK, seq // groups)
    per = seq // groups // qb
    grid = (heads, seq // qb)
    q_spec = pl.BlockSpec((1, qb, hd), lambda h, i, p: (h, i, 0))
    kv_spec = pl.BlockSpec((1, seq, hd), lambda h, i, p: (h, 0, 0))
    lse_spec = pl.BlockSpec((1, qb, 1), lambda h, i, p: (h, i, 0))
    g_spec = pl.BlockSpec((groups, 3, 1, seq // groups, hd), lambda h, i, p: (0, 0, h, 0, 0))
    shape = jax.ShapeDtypeStruct((groups, 3, heads, seq // groups, hd), jnp.bfloat16)
    return pl.pallas_call(
        functools.partial(_bwd_kernel, scale),
        out_shape=shape,
        grid_spec=pltpu.PrefetchScalarGridSpec(
            num_scalar_prefetch=1, grid=grid,
            in_specs=[q_spec, kv_spec, kv_spec, q_spec, lse_spec],
            out_specs=g_spec,
            scratch_shapes=[pltpu.VMEM((seq, hd), jnp.float32),
                            pltpu.VMEM((seq, hd), jnp.float32)]),
        compiler_params=pltpu.CompilerParams(
            dimension_semantics=("arbitrary", "arbitrary"),
            vmem_limit_bytes=48 * 1024 * 1024),
        cost_estimate=pl.CostEstimate(
            flops=10 * heads * seq * seq * hd, transcendentals=heads * seq * seq,
            bytes_accessed=8 * heads * seq * hd * 2),
    )(prefix, q, k, v, grad_out, lse)


def on_device(
    tokens,
    pass_ids,
    prefix,
    cotangent,
    qkv_weight,
    out_weight,
    fc1_weight,
    fc2_weight,
    ln1_gain,
    ln1_bias,
    qv_bias,
    out_bias,
    ln2_gain,
    ln2_bias,
    fc1_bias,
    fc2_bias,
    pass_table,
):
    tp_count = lax.axis_size("tp")
    tp_rank = lax.axis_index("tp")
    local_rows = tokens.shape[0]
    seq_len = local_rows * tp_count
    cols_here = qkv_weight.shape[2]
    heads_here = cols_here // HD
    scale = HD ** (-0.5)
    prefix_len = prefix[0]
    gelu_tanh = partial(jax.nn.gelu, approximate=True)
    fsdp_count = lax.axis_size("fsdp")
    qkv_cols = lax.all_gather(qkv_weight, "fsdp", axis=1, tiled=True)
    qkv_full = qkv_cols
    hidden_here = fc1_weight.shape[1]
    qv_here = lax.dynamic_slice_in_dim(qv_bias, tp_rank * cols_here, cols_here, 1)
    one_hot = (pass_ids[:, None] == jnp.arange(NPASS, dtype=jnp.int32)[None, :]).astype(jnp.float32)
    block_in = tokens.astype(jnp.float32) + jnp.dot(
        one_hot, pass_table, precision=HIGH, preferred_element_type=jnp.float32
    )
    normed, unit_one, inv_one = norm_forward(block_in, ln1_gain, ln1_bias)
    normed_all = lax.all_gather(normed.astype(jnp.bfloat16), "tp", axis=0, tiled=True)
    shards = (out_weight, fc1_weight, fc2_weight)
    packed = jnp.concatenate([piece.reshape(-1) for piece in shards])
    packed, qkv_cols, normed_all = lax.optimization_barrier((packed, qkv_cols, normed_all))
    qkv_full = qkv_cols
    gathered = lax.all_gather(packed, "fsdp", axis=0, tiled=False)
    qkv_copies = jnp.broadcast_to(qkv_cols[None], (tp_count,) + qkv_cols.shape)
    qkv_all = lax.all_to_all(qkv_copies, "tp", 0, 0, tiled=True)
    grad_rows = lax.all_gather(cotangent, "tp", axis=0, tiled=True)
    projected = jnp.einsum("rd,kdc->krc", normed_all, qkv_full, preferred_element_type=jnp.float32)
    queries = (projected[0] + qv_here[0]).astype(jnp.bfloat16).reshape(seq_len, heads_here, HD)
    keys_all = projected[1].astype(jnp.bfloat16).reshape(seq_len, heads_here, HD)
    values_all = (projected[2] + qv_here[1]).astype(jnp.bfloat16).reshape(seq_len, heads_here, HD)
    q_heads = jnp.transpose(queries, (1, 0, 2))
    k_heads = jnp.transpose(keys_all, (1, 0, 2))
    v_heads = jnp.transpose(values_all, (1, 0, 2))
    mixed, log_mass = attn_forward(prefix, q_heads, k_heads, v_heads, scale, tp_count)
    mixed, qkv_all = lax.optimization_barrier((mixed, qkv_all))
    pieces = []
    offset = 0
    for piece in shards:
        size = piece.size
        pieces.append(gathered[:, offset : offset + size].reshape((fsdp_count,) + piece.shape))
        offset += size
    out_full = jnp.moveaxis(pieces[0], 0, 1).reshape(out_weight.shape[0], -1)
    fc1_part = pieces[1].reshape(-1, fc1_weight.shape[1])
    fc2_part = jnp.moveaxis(pieces[2], 0, 1).reshape(fc2_weight.shape[0], -1)
    out_all = lax.all_gather(out_full, "tp", axis=0, tiled=True)
    mixed, grad_rows, out_all, fc1_part, fc2_part = lax.optimization_barrier(
        (mixed, grad_rows, out_all, fc1_part, fc2_part)
    )
    mixed_rows = lax.all_to_all(mixed, "tp", 0, 0, tiled=True)
    middle = (
        block_in
        + jnp.einsum(
            "shre,shem->rm",
            mixed_rows,
            out_all.reshape(tp_count, heads_here, HD, -1),
            preferred_element_type=jnp.float32,
        )
        + out_bias
    )
    normed_two, unit_two, inv_two = norm_forward(middle, ln2_gain, ln2_bias)
    normed_two = normed_two.astype(jnp.bfloat16)
    grad_top = cotangent.astype(jnp.float32)
    fc1_bias_here = lax.dynamic_slice_in_dim(fc1_bias, tp_rank * hidden_here, hidden_here, 0)
    normed_rows = lax.all_gather(normed_two, "tp", axis=0, tiled=True)
    before = jnp.dot(normed_rows, fc1_part, preferred_element_type=jnp.float32) + fc1_bias_here
    hidden = gelu_tanh(before).astype(jnp.bfloat16)
    fc2_partial = jnp.dot(hidden, fc2_part, preferred_element_type=jnp.float32).astype(jnp.bfloat16)
    grad_hidden = matmul_nt(grad_rows, fc2_part)
    grad_before = jax.vjp(gelu_tanh, before)[1](grad_hidden)[0].astype(jnp.bfloat16)
    grad_fc1_bias = lax.dynamic_update_slice_in_dim(
        jnp.zeros(fc1_bias.shape, jnp.float32),
        jnp.sum(grad_before.astype(jnp.float32), axis=0),
        tp_rank * hidden_here,
        0,
    )
    grad_fc1 = matmul_tn(normed_rows, grad_before)
    grad_fc2 = matmul_tn(hidden, grad_rows)
    grad_normed_two = lax.psum_scatter(
        matmul_nt(grad_before, fc1_part).astype(jnp.bfloat16), "tp", scatter_dimension=0, tiled=True
    ).astype(jnp.float32)
    grad_normed_two, fc2_partial, grad_fc1, grad_fc2 = lax.optimization_barrier(
        (grad_normed_two, fc2_partial, grad_fc1, grad_fc2)
    )
    grad_fc2_bias = jnp.sum(grad_top, axis=0)
    grad_from_norm, grad_ln2_gain, grad_ln2_bias = norm_backward(
        grad_normed_two, unit_two, inv_two, ln2_gain
    )
    grad_middle = grad_top + grad_from_norm
    grad_out_bias = jnp.sum(grad_middle, axis=0)
    grad_attn_rows = lax.all_gather(grad_middle.astype(jnp.bfloat16), "tp", axis=0, tiled=True)
    fc2_partial, grad_attn_rows = lax.optimization_barrier((fc2_partial, grad_attn_rows))
    fc2_parts = lax.all_to_all(
        fc2_partial.reshape(tp_count, local_rows, -1), "tp", 0, 0, tiled=True
    )
    result = middle + jnp.sum(fc2_parts.astype(jnp.float32), axis=0) + fc2_bias
    grad_out_w = jnp.einsum(
        "thre,trm->hem",
        mixed,
        grad_attn_rows.reshape(tp_count, local_rows, -1),
        preferred_element_type=jnp.float32,
    ).reshape(cols_here, -1)
    fsdp_count = lax.axis_size("fsdp")
    dense_grads = (
        jnp.moveaxis(grad_out_w.reshape(grad_out_w.shape[0], fsdp_count, -1), 1, 0),
        grad_fc1.reshape(fsdp_count, -1, grad_fc1.shape[1]),
        jnp.moveaxis(grad_fc2.reshape(grad_fc2.shape[0], fsdp_count, -1), 1, 0),
    )
    dense_packed = jnp.concatenate([g.reshape(fsdp_count, -1) for g in dense_grads], axis=1)
    dense_summed = lax.psum_scatter(
        dense_packed.reshape(-1, grad_fc1.shape[1]).astype(jnp.bfloat16),
        "fsdp",
        scatter_dimension=0,
        tiled=True,
    ).reshape(1, -1).astype(jnp.float32)
    grad_mixed = (
        matmul_nt(grad_attn_rows, out_full).astype(jnp.bfloat16).reshape(seq_len, heads_here, HD)
    )
    grad_all = attn_backward(
        prefix, q_heads, k_heads, v_heads, jnp.transpose(grad_mixed, (1, 0, 2)), log_mass, scale,
        tp_count,
    )
    grad_all, result, dense_summed = lax.optimization_barrier((grad_all, result, dense_summed))
    grad_q_heads, grad_v_heads = grad_all[:, 0], grad_all[:, 2]
    grad_qv_here = jnp.stack(
        [
            jnp.sum(grad_q_heads.astype(jnp.float32), axis=(0, 2)).reshape(-1),
            jnp.sum(grad_v_heads.astype(jnp.float32), axis=(0, 2)).reshape(-1),
        ],
        axis=0,
    )
    grad_qv_bias = lax.dynamic_update_slice_in_dim(
        jnp.zeros(qv_bias.shape, jnp.float32), grad_qv_here, tp_rank * cols_here, 1
    )
    normed_groups = normed_all.reshape(tp_count, local_rows, -1)
    grad_qkv_w = jnp.einsum(
        "trd,tkhre->kdhe", normed_groups, grad_all, preferred_element_type=jnp.float32
    ).reshape(3, normed_all.shape[1], cols_here)
    grad_rows_all = lax.all_to_all(grad_all, "tp", 0, 0, tiled=True)
    qkv_split = qkv_all.reshape(tp_count, 3, qkv_all.shape[2], heads_here, HD)
    grad_normed = jnp.einsum(
        "skhre,skdhe->rd", grad_rows_all, qkv_split, preferred_element_type=jnp.float32
    )
    dense_shards = []
    offset = 0
    for g in dense_grads:
        size = g[0].size
        dense_shards.append(dense_summed[0, offset : offset + size].reshape(g.shape[1:]))
        offset += size
    out_shard, fc1_shard, fc2_shard = dense_shards
    grad_in_norm, grad_ln1_gain, grad_ln1_bias = norm_backward(
        grad_normed, unit_one, inv_one, ln1_gain
    )
    grad_input = grad_middle + grad_in_norm
    grad_table = lax.dot_general(
        one_hot,
        grad_input,
        (((0,), (0,)), ((), ())),
        precision=HIGH,
        preferred_element_type=jnp.float32,
    )
    qkv_shard = lax.psum_scatter(grad_qkv_w, "fsdp", scatter_dimension=1, tiled=True)
    summed = lax.psum(
        (
            grad_ln1_gain,
            grad_ln1_bias,
            grad_qv_bias,
            grad_out_bias,
            grad_ln2_gain,
            grad_ln2_bias,
            grad_fc1_bias,
            grad_fc2_bias,
            grad_table,
        ),
        ("fsdp", "tp"),
    )
    return (
        result.astype(jnp.bfloat16),
        grad_input,
        qkv_shard,
        out_shard,
        fc1_shard,
        fc2_shard,
        summed[0],
        summed[1],
        summed[2],
        summed[3],
        summed[4],
        summed[5],
        summed[6],
        summed[7],
        summed[8],
    )


def solution(mesh):
    placed = (
        P(("fsdp", "tp"), None),
        P(("fsdp", "tp")),
        P("fsdp"),
        P(("fsdp", "tp"), None),
        P(None, "fsdp", "tp"),
        P("tp", "fsdp"),
        P("fsdp", "tp"),
        P("tp", "fsdp"),
        P(),
        P(),
        P(),
        P(),
        P(),
        P(),
        P(),
        P(),
        P(),
    )
    return jax.shard_map(
        on_device,
        mesh=mesh,
        in_specs=placed,
        out_specs=(
            P(("fsdp", "tp"), None),
            P(("fsdp", "tp"), None),
            P(None, "fsdp", "tp"),
            P("tp", "fsdp"),
            P("fsdp", "tp"),
            P("tp", "fsdp"),
            P(),
            P(),
            P(),
            P(),
            P(),
            P(),
            P(),
            P(),
            P(),
        ),
        check_vma=False,
    )
```

```python
import functools
from functools import partial

import jax
import jax.numpy as jnp
from jax import lax
from jax.experimental import pallas as pl
from jax.experimental.pallas import tpu as pltpu
from jax.sharding import PartitionSpec as P

HD = 64
NPASS = 5
QBLOCK = 512


HIGH = lax.Precision.HIGHEST
EPS = 1e-05
NEG_FILL = -1e30


def norm_forward(rows_in, gain, shift):
    center = rows_in - jnp.mean(rows_in, axis=-1, keepdims=True)
    scale_inv = lax.rsqrt(jnp.mean(center * center, axis=-1, keepdims=True) + EPS)
    unit_rows = center * scale_inv
    return (unit_rows * gain + shift, unit_rows, scale_inv)


def norm_backward(grad_out, unit_rows, scale_inv, gain):
    grad_unit = grad_out * gain
    first_mean = jnp.mean(grad_unit, axis=-1, keepdims=True)
    second_mean = jnp.mean(grad_unit * unit_rows, axis=-1, keepdims=True)
    grad_rows = scale_inv * (grad_unit - first_mean - unit_rows * second_mean)
    return (grad_rows, jnp.sum(grad_out * unit_rows, axis=0), jnp.sum(grad_out, axis=0))


def matmul_nt(left, right):
    return lax.dot_general(
        left, right, (((1,), (1,)), ((), ())), preferred_element_type=jnp.float32
    )


def matmul_tn(left, right):
    return lax.dot_general(
        left, right, (((0,), (0,)), ((), ())), preferred_element_type=jnp.float32
    )


def block_scores(query_block, keys_all, row_start, prefix_len, scale):
    raw = (
        jnp.einsum("qhe,khe->hqk", query_block, keys_all, preferred_element_type=jnp.float32)
        * scale
    )
    row_ids = row_start + jnp.arange(query_block.shape[0], dtype=jnp.int32)
    col_ids = jnp.arange(keys_all.shape[0], dtype=jnp.int32)
    allowed = (col_ids[None, :] <= row_ids[:, None]) | (col_ids[None, :] < prefix_len)
    return jnp.where(allowed[None], raw, NEG_FILL)


ATT_QB = 512


def _mask(prefix_len, qb, rows, cols):
    row = qb * rows + lax.broadcasted_iota(jnp.int32, (rows, cols), 0)
    col = lax.broadcasted_iota(jnp.int32, (rows, cols), 1)
    return (col <= row) | (col < prefix_len)


def _nt(a, b):
    return lax.dot_general(a, b, (((1,), (1,)), ((), ())), preferred_element_type=jnp.float32)


def _tn(a, b):
    return lax.dot_general(a, b, (((0,), (0,)), ((), ())), preferred_element_type=jnp.float32)


def _fwd_kernel(scale, prefix_ref, q_ref, k_ref, v_ref, o_ref, lse_ref):
    qb = pl.program_id(1)
    q = q_ref[0]
    rows, cols = q.shape[0], k_ref.shape[1]
    scores = _nt(q, k_ref[0]) * scale
    scores = jnp.where(_mask(prefix_ref[0], qb, rows, cols), scores, NEG_FILL)
    peak = jnp.max(scores, axis=-1, keepdims=True)
    expo = jnp.exp(scores - peak)
    total = jnp.sum(expo, axis=-1, keepdims=True)
    probs_low = (expo / total).astype(jnp.bfloat16)
    out = jnp.dot(probs_low, v_ref[0], preferred_element_type=jnp.float32)
    o_ref[0, 0] = out.astype(o_ref.dtype)
    lse_ref[0] = peak + jnp.log(total)


def _bwd_kernel(scale, prefix_ref, q_ref, k_ref, v_ref, do_ref, lse_ref,
                g_ref, dk_acc, dv_acc):
    qb = pl.program_id(1)

    @pl.when(qb == 0)
    def _():
        dk_acc[...] = jnp.zeros_like(dk_acc)
        dv_acc[...] = jnp.zeros_like(dv_acc)

    q = q_ref[0]
    k = k_ref[0]
    grad_out = do_ref[0]
    rows, cols = q.shape[0], k.shape[0]
    scores = _nt(q, k) * scale
    scores = jnp.where(_mask(prefix_ref[0], qb, rows, cols), scores, NEG_FILL)
    probs = jnp.exp(scores - lse_ref[0])
    dv_acc[...] += _tn(probs.astype(jnp.bfloat16), grad_out)
    grad_probs = _nt(grad_out, v_ref[0])
    inner = jnp.sum(probs * grad_probs, axis=-1, keepdims=True)
    grad_scores = (probs * (grad_probs - inner)).astype(jnp.bfloat16)
    groups, rows_per = g_ref.shape[0], g_ref.shape[3]
    per = rows_per // rows
    start = pl.multiple_of((qb % per) * rows, rows)
    g_ref[qb // per, 0, 0, pl.ds(start, rows), :] = (
        jnp.dot(grad_scores, k, preferred_element_type=jnp.float32) * scale
    ).astype(g_ref.dtype)
    dk_acc[...] += _tn(grad_scores, q)

    @pl.when(qb == pl.num_programs(1) - 1)
    def _():
        hd = g_ref.shape[4]
        g_ref[:, 1, 0] = (dk_acc[...] * scale).astype(g_ref.dtype).reshape(groups, rows_per, hd)
        g_ref[:, 2, 0] = dv_acc[...].astype(g_ref.dtype).reshape(groups, rows_per, hd)


def attn_forward(prefix, q, k, v, scale, groups):
    heads, seq, hd = q.shape
    qb = min(ATT_QB, seq // groups)
    per = seq // groups // qb
    grid = (heads, seq // qb)
    q_spec = pl.BlockSpec((1, qb, hd), lambda h, i, p: (h, i, 0))
    kv_spec = pl.BlockSpec((1, seq, hd), lambda h, i, p: (h, 0, 0))
    lse_spec = pl.BlockSpec((1, qb, 1), lambda h, i, p: (h, i, 0))
    o_spec = pl.BlockSpec((1, 1, qb, hd), lambda h, i, p: (i // per, h, i % per, 0))
    return pl.pallas_call(
        functools.partial(_fwd_kernel, scale),
        out_shape=(jax.ShapeDtypeStruct((groups, heads, seq // groups, hd), jnp.bfloat16),
                   jax.ShapeDtypeStruct((heads, seq, 1), jnp.float32)),
        grid_spec=pltpu.PrefetchScalarGridSpec(
            num_scalar_prefetch=1, grid=grid,
            in_specs=[q_spec, kv_spec, kv_spec],
            out_specs=[o_spec, lse_spec]),
        compiler_params=pltpu.CompilerParams(
            dimension_semantics=("arbitrary", "arbitrary"),
            vmem_limit_bytes=48 * 1024 * 1024),
        cost_estimate=pl.CostEstimate(
            flops=4 * heads * seq * seq * hd, transcendentals=heads * seq * seq,
            bytes_accessed=4 * heads * seq * hd * 2),
    )(prefix, q, k, v)


def attn_backward(prefix, q, k, v, grad_out, lse, scale, groups):
    heads, seq, hd = q.shape
    qb = min(ATT_QB, seq // groups)
    per = seq // groups // qb
    grid = (heads, seq // qb)
    q_spec = pl.BlockSpec((1, qb, hd), lambda h, i, p: (h, i, 0))
    kv_spec = pl.BlockSpec((1, seq, hd), lambda h, i, p: (h, 0, 0))
    lse_spec = pl.BlockSpec((1, qb, 1), lambda h, i, p: (h, i, 0))
    g_spec = pl.BlockSpec((groups, 3, 1, seq // groups, hd), lambda h, i, p: (0, 0, h, 0, 0))
    shape = jax.ShapeDtypeStruct((groups, 3, heads, seq // groups, hd), jnp.bfloat16)
    return pl.pallas_call(
        functools.partial(_bwd_kernel, scale),
        out_shape=shape,
        grid_spec=pltpu.PrefetchScalarGridSpec(
            num_scalar_prefetch=1, grid=grid,
            in_specs=[q_spec, kv_spec, kv_spec, q_spec, lse_spec],
            out_specs=g_spec,
            scratch_shapes=[pltpu.VMEM((seq, hd), jnp.float32),
                            pltpu.VMEM((seq, hd), jnp.float32)]),
        compiler_params=pltpu.CompilerParams(
            dimension_semantics=("arbitrary", "arbitrary"),
            vmem_limit_bytes=48 * 1024 * 1024),
        cost_estimate=pl.CostEstimate(
            flops=10 * heads * seq * seq * hd, transcendentals=heads * seq * seq,
            bytes_accessed=8 * heads * seq * hd * 2),
    )(prefix, q, k, v, grad_out, lse)


def on_device(
    tokens,
    pass_ids,
    prefix,
    cotangent,
    qkv_weight,
    out_weight,
    fc1_weight,
    fc2_weight,
    ln1_gain,
    ln1_bias,
    qv_bias,
    out_bias,
    ln2_gain,
    ln2_bias,
    fc1_bias,
    fc2_bias,
    pass_table,
):
    tp_count = lax.axis_size("tp")
    tp_rank = lax.axis_index("tp")
    local_rows = tokens.shape[0]
    seq_len = local_rows * tp_count
    cols_here = qkv_weight.shape[2]
    heads_here = cols_here // HD
    scale = HD ** (-0.5)
    prefix_len = prefix[0]
    gelu_tanh = partial(jax.nn.gelu, approximate=True)
    fsdp_count = lax.axis_size("fsdp")
    qkv_cols = lax.all_gather(qkv_weight, "fsdp", axis=1, tiled=True)
    qkv_full = qkv_cols
    hidden_here = fc1_weight.shape[1]
    qv_here = lax.dynamic_slice_in_dim(qv_bias, tp_rank * cols_here, cols_here, 1)
    one_hot = (pass_ids[:, None] == jnp.arange(NPASS, dtype=jnp.int32)[None, :]).astype(jnp.float32)
    block_in = tokens.astype(jnp.float32) + jnp.dot(
        one_hot, pass_table, precision=HIGH, preferred_element_type=jnp.float32
    )
    normed, unit_one, inv_one = norm_forward(block_in, ln1_gain, ln1_bias)
    normed_all = lax.all_gather(normed.astype(jnp.bfloat16), "tp", axis=0, tiled=True)
    shards = (out_weight, fc1_weight, fc2_weight)
    packed = jnp.concatenate([piece.reshape(-1) for piece in shards])
    packed, qkv_cols, normed_all = lax.optimization_barrier((packed, qkv_cols, normed_all))
    qkv_full = qkv_cols
    gathered = lax.all_gather(packed, "fsdp", axis=0, tiled=False)
    qkv_copies = jnp.broadcast_to(qkv_cols[None], (tp_count,) + qkv_cols.shape)
    qkv_all = lax.all_to_all(qkv_copies, "tp", 0, 0, tiled=True)
    grad_rows = lax.all_gather(cotangent, "tp", axis=0, tiled=True)
    projected = jnp.einsum("rd,kdc->krc", normed_all, qkv_full, preferred_element_type=jnp.float32)
    queries = (projected[0] + qv_here[0]).astype(jnp.bfloat16).reshape(seq_len, heads_here, HD)
    keys_all = projected[1].astype(jnp.bfloat16).reshape(seq_len, heads_here, HD)
    values_all = (projected[2] + qv_here[1]).astype(jnp.bfloat16).reshape(seq_len, heads_here, HD)
    q_heads = jnp.transpose(queries, (1, 0, 2))
    k_heads = jnp.transpose(keys_all, (1, 0, 2))
    v_heads = jnp.transpose(values_all, (1, 0, 2))
    mixed, log_mass = attn_forward(prefix, q_heads, k_heads, v_heads, scale, tp_count)
    mixed, qkv_all = lax.optimization_barrier((mixed, qkv_all))
    pieces = []
    offset = 0
    for piece in shards:
        size = piece.size
        pieces.append(gathered[:, offset : offset + size].reshape((fsdp_count,) + piece.shape))
        offset += size
    out_full = jnp.moveaxis(pieces[0], 0, 1).reshape(out_weight.shape[0], -1)
    fc1_part = pieces[1].reshape(-1, fc1_weight.shape[1])
    fc2_part = jnp.moveaxis(pieces[2], 0, 1).reshape(fc2_weight.shape[0], -1)
    out_all = lax.all_gather(out_full, "tp", axis=0, tiled=True)
    mixed, grad_rows, out_all, fc1_part, fc2_part = lax.optimization_barrier(
        (mixed, grad_rows, out_all, fc1_part, fc2_part)
    )
    mixed_rows = lax.all_to_all(mixed, "tp", 0, 0, tiled=True)
    middle = (
        block_in
        + jnp.einsum(
            "shre,shem->rm",
            mixed_rows,
            out_all.reshape(tp_count, heads_here, HD, -1),
            preferred_element_type=jnp.float32,
        )
        + out_bias
    )
    normed_two, unit_two, inv_two = norm_forward(middle, ln2_gain, ln2_bias)
    normed_two = normed_two.astype(jnp.bfloat16)
    grad_top = cotangent.astype(jnp.float32)
    fc1_bias_here = lax.dynamic_slice_in_dim(fc1_bias, tp_rank * hidden_here, hidden_here, 0)
    normed_rows = lax.all_gather(normed_two, "tp", axis=0, tiled=True)
    before = jnp.dot(normed_rows, fc1_part, preferred_element_type=jnp.float32) + fc1_bias_here
    hidden = gelu_tanh(before).astype(jnp.bfloat16)
    fc2_partial = jnp.dot(hidden, fc2_part, preferred_element_type=jnp.float32).astype(jnp.bfloat16)
    grad_hidden = matmul_nt(grad_rows, fc2_part)
    grad_before = jax.vjp(gelu_tanh, before)[1](grad_hidden)[0].astype(jnp.bfloat16)
    grad_fc1_bias = lax.dynamic_update_slice_in_dim(
        jnp.zeros(fc1_bias.shape, jnp.float32),
        jnp.sum(grad_before.astype(jnp.float32), axis=0),
        tp_rank * hidden_here,
        0,
    )
    grad_fc1 = matmul_tn(normed_rows, grad_before)
    grad_fc2 = matmul_tn(hidden, grad_rows)
    grad_normed_two = lax.psum_scatter(
        matmul_nt(grad_before, fc1_part).astype(jnp.bfloat16), "tp", scatter_dimension=0, tiled=True
    ).astype(jnp.float32)
    grad_normed_two, fc2_partial, grad_fc1, grad_fc2 = lax.optimization_barrier(
        (grad_normed_two, fc2_partial, grad_fc1, grad_fc2)
    )
    grad_fc2_bias = jnp.sum(grad_top, axis=0)
    grad_from_norm, grad_ln2_gain, grad_ln2_bias = norm_backward(
        grad_normed_two, unit_two, inv_two, ln2_gain
    )
    grad_middle = grad_top + grad_from_norm
    grad_out_bias = jnp.sum(grad_middle, axis=0)
    width = grad_fc1.shape[1]
    fsdp_count = lax.axis_size("fsdp")
    dense_grads = (
        grad_fc1.reshape(fsdp_count, -1, width),
        jnp.moveaxis(grad_fc2.reshape(grad_fc2.shape[0], fsdp_count, -1), 1, 0),
    )
    dense_packed = jnp.concatenate(
        [g.reshape(fsdp_count, -1, width) for g in dense_grads], axis=1
    ).astype(jnp.bfloat16)
    grad_attn_rows = lax.all_gather(grad_middle.astype(jnp.bfloat16), "tp", axis=0, tiled=True)
    fc2_partial, grad_attn_rows, dense_packed = lax.optimization_barrier(
        (fc2_partial, grad_attn_rows, dense_packed)
    )
    fc2_parts = lax.all_to_all(
        fc2_partial.reshape(tp_count, local_rows, -1), "tp", 0, 0, tiled=True
    )
    result = middle + jnp.sum(fc2_parts.astype(jnp.float32), axis=0) + fc2_bias
    grad_out_w = jnp.einsum(
        "thre,trm->hem",
        mixed,
        grad_attn_rows.reshape(tp_count, local_rows, -1),
        preferred_element_type=jnp.float32,
    ).reshape(cols_here, -1)
    dense_summed = lax.psum_scatter(
        dense_packed.reshape(-1, width), "fsdp", scatter_dimension=0, tiled=True
    ).reshape(1, -1).astype(jnp.float32)
    grad_mixed = (
        matmul_nt(grad_attn_rows, out_full).astype(jnp.bfloat16).reshape(seq_len, heads_here, HD)
    )
    grad_all = attn_backward(
        prefix, q_heads, k_heads, v_heads, jnp.transpose(grad_mixed, (1, 0, 2)), log_mass, scale,
        tp_count,
    )
    grad_all, result, dense_summed = lax.optimization_barrier((grad_all, result, dense_summed))
    grad_q_heads, grad_v_heads = grad_all[:, 0], grad_all[:, 2]
    grad_qv_here = jnp.stack(
        [
            jnp.sum(grad_q_heads.astype(jnp.float32), axis=(0, 2)).reshape(-1),
            jnp.sum(grad_v_heads.astype(jnp.float32), axis=(0, 2)).reshape(-1),
        ],
        axis=0,
    )
    grad_qv_bias = lax.dynamic_update_slice_in_dim(
        jnp.zeros(qv_bias.shape, jnp.float32), grad_qv_here, tp_rank * cols_here, 1
    )
    normed_groups = normed_all.reshape(tp_count, local_rows, -1)
    grad_qkv_w = jnp.einsum(
        "trd,tkhre->kdhe", normed_groups, grad_all, preferred_element_type=jnp.float32
    ).reshape(3, normed_all.shape[1], cols_here)
    grad_rows_all = lax.all_to_all(grad_all, "tp", 0, 0, tiled=True)
    qkv_split = qkv_all.reshape(tp_count, 3, qkv_all.shape[2], heads_here, HD)
    grad_normed = jnp.einsum(
        "skhre,skdhe->rd", grad_rows_all, qkv_split, preferred_element_type=jnp.float32
    )
    dense_shards = []
    offset = 0
    for g in dense_grads:
        size = g[0].size
        dense_shards.append(dense_summed[0, offset : offset + size].reshape(g.shape[1:]))
        offset += size
    fc1_shard, fc2_shard = dense_shards
    grad_in_norm, grad_ln1_gain, grad_ln1_bias = norm_backward(
        grad_normed, unit_one, inv_one, ln1_gain
    )
    grad_input = grad_middle + grad_in_norm
    grad_table = lax.dot_general(
        one_hot,
        grad_input,
        (((0,), (0,)), ((), ())),
        precision=HIGH,
        preferred_element_type=jnp.float32,
    )
    tail_grads = (
        jnp.moveaxis(grad_qkv_w.reshape(3, fsdp_count, -1, cols_here), 1, 0),
        jnp.moveaxis(grad_out_w.reshape(grad_out_w.shape[0], fsdp_count, -1), 1, 0),
    )
    tail_packed = jnp.concatenate([g.reshape(fsdp_count, -1, width) for g in tail_grads], axis=1)
    tail_summed = lax.psum_scatter(
        tail_packed.reshape(-1, width), "fsdp", scatter_dimension=0, tiled=True
    ).reshape(-1)
    tail_shards = []
    offset = 0
    for g in tail_grads:
        size = g[0].size
        tail_shards.append(tail_summed[offset : offset + size].reshape(g.shape[1:]))
        offset += size
    qkv_shard, out_shard = tail_shards
    summed = lax.psum(
        (
            grad_ln1_gain,
            grad_ln1_bias,
            grad_qv_bias,
            grad_out_bias,
            grad_ln2_gain,
            grad_ln2_bias,
            grad_fc1_bias,
            grad_fc2_bias,
            grad_table,
        ),
        ("fsdp", "tp"),
    )
    return (
        result.astype(jnp.bfloat16),
        grad_input,
        qkv_shard,
        out_shard,
        fc1_shard,
        fc2_shard,
        summed[0],
        summed[1],
        summed[2],
        summed[3],
        summed[4],
        summed[5],
        summed[6],
        summed[7],
        summed[8],
    )


def solution(mesh):
    placed = (
        P(("fsdp", "tp"), None),
        P(("fsdp", "tp")),
        P("fsdp"),
        P(("fsdp", "tp"), None),
        P(None, "fsdp", "tp"),
        P("tp", "fsdp"),
        P("fsdp", "tp"),
        P("tp", "fsdp"),
        P(),
        P(),
        P(),
        P(),
        P(),
        P(),
        P(),
        P(),
        P(),
    )
    return jax.shard_map(
        on_device,
        mesh=mesh,
        in_specs=placed,
        out_specs=(
            P(("fsdp", "tp"), None),
            P(("fsdp", "tp"), None),
            P(None, "fsdp", "tp"),
            P("tp", "fsdp"),
            P("fsdp", "tp"),
            P("tp", "fsdp"),
            P(),
            P(),
            P(),
            P(),
            P(),
            P(),
            P(),
            P(),
            P(),
        ),
        check_vma=False,
    )
```

```python
import functools
from functools import partial

import jax
import jax.numpy as jnp
from jax import lax
from jax.experimental import pallas as pl
from jax.experimental.pallas import tpu as pltpu
from jax.sharding import PartitionSpec as P

HD = 64
NPASS = 5
QBLOCK = 512


HIGH = lax.Precision.HIGHEST
EPS = 1e-05
NEG_FILL = -1e30


def norm_forward(rows_in, gain, shift):
    center = rows_in - jnp.mean(rows_in, axis=-1, keepdims=True)
    scale_inv = lax.rsqrt(jnp.mean(center * center, axis=-1, keepdims=True) + EPS)
    unit_rows = center * scale_inv
    return (unit_rows * gain + shift, unit_rows, scale_inv)


def norm_backward(grad_out, unit_rows, scale_inv, gain):
    grad_unit = grad_out * gain
    first_mean = jnp.mean(grad_unit, axis=-1, keepdims=True)
    second_mean = jnp.mean(grad_unit * unit_rows, axis=-1, keepdims=True)
    grad_rows = scale_inv * (grad_unit - first_mean - unit_rows * second_mean)
    return (grad_rows, jnp.sum(grad_out * unit_rows, axis=0), jnp.sum(grad_out, axis=0))


def matmul_nt(left, right):
    return lax.dot_general(
        left, right, (((1,), (1,)), ((), ())), preferred_element_type=jnp.float32
    )


def matmul_tn(left, right):
    return lax.dot_general(
        left, right, (((0,), (0,)), ((), ())), preferred_element_type=jnp.float32
    )


def block_scores(query_block, keys_all, row_start, prefix_len, scale):
    raw = (
        jnp.einsum("qhe,khe->hqk", query_block, keys_all, preferred_element_type=jnp.float32)
        * scale
    )
    row_ids = row_start + jnp.arange(query_block.shape[0], dtype=jnp.int32)
    col_ids = jnp.arange(keys_all.shape[0], dtype=jnp.int32)
    allowed = (col_ids[None, :] <= row_ids[:, None]) | (col_ids[None, :] < prefix_len)
    return jnp.where(allowed[None], raw, NEG_FILL)


ATT_QB = 512


def _mask(prefix_len, qb, rows, cols):
    row = qb * rows + lax.broadcasted_iota(jnp.int32, (rows, cols), 0)
    col = lax.broadcasted_iota(jnp.int32, (rows, cols), 1)
    return (col <= row) | (col < prefix_len)


def _nt(a, b):
    return lax.dot_general(a, b, (((1,), (1,)), ((), ())), preferred_element_type=jnp.float32)


def _tn(a, b):
    return lax.dot_general(a, b, (((0,), (0,)), ((), ())), preferred_element_type=jnp.float32)


def _fwd_kernel(scale, prefix_ref, q_ref, k_ref, v_ref, o_ref, lse_ref):
    qb = pl.program_id(1)
    q = q_ref[0]
    rows, cols = q.shape[0], k_ref.shape[1]
    scores = _nt(q, k_ref[0]) * scale
    scores = jnp.where(_mask(prefix_ref[0], qb, rows, cols), scores, NEG_FILL)
    peak = jnp.max(scores, axis=-1, keepdims=True)
    expo = jnp.exp(scores - peak)
    total = jnp.sum(expo, axis=-1, keepdims=True)
    probs_low = (expo / total).astype(jnp.bfloat16)
    out = jnp.dot(probs_low, v_ref[0], preferred_element_type=jnp.float32)
    o_ref[0, 0] = out.astype(o_ref.dtype)
    lse_ref[0] = peak + jnp.log(total)


def _bwd_kernel(scale, prefix_ref, q_ref, k_ref, v_ref, do_ref, lse_ref,
                g_ref, dk_acc, dv_acc):
    qb = pl.program_id(1)

    @pl.when(qb == 0)
    def _():
        dk_acc[...] = jnp.zeros_like(dk_acc)
        dv_acc[...] = jnp.zeros_like(dv_acc)

    q = q_ref[0]
    k = k_ref[0]
    grad_out = do_ref[0]
    rows, cols = q.shape[0], k.shape[0]
    scores = _nt(q, k) * scale
    scores = jnp.where(_mask(prefix_ref[0], qb, rows, cols), scores, NEG_FILL)
    probs = jnp.exp(scores - lse_ref[0])
    dv_acc[...] += _tn(probs.astype(jnp.bfloat16), grad_out)
    grad_probs = _nt(grad_out, v_ref[0])
    inner = jnp.sum(probs * grad_probs, axis=-1, keepdims=True)
    grad_scores = (probs * (grad_probs - inner)).astype(jnp.bfloat16)
    groups, rows_per = g_ref.shape[0], g_ref.shape[3]
    per = rows_per // rows
    start = pl.multiple_of((qb % per) * rows, rows)
    g_ref[qb // per, 0, 0, pl.ds(start, rows), :] = (
        jnp.dot(grad_scores, k, preferred_element_type=jnp.float32) * scale
    ).astype(g_ref.dtype)
    dk_acc[...] += _tn(grad_scores, q)

    @pl.when(qb == pl.num_programs(1) - 1)
    def _():
        hd = g_ref.shape[4]
        g_ref[:, 1, 0] = (dk_acc[...] * scale).astype(g_ref.dtype).reshape(groups, rows_per, hd)
        g_ref[:, 2, 0] = dv_acc[...].astype(g_ref.dtype).reshape(groups, rows_per, hd)


def attn_forward(prefix, q, k, v, scale, groups):
    heads, seq, hd = q.shape
    qb = min(ATT_QB, seq // groups)
    per = seq // groups // qb
    grid = (heads, seq // qb)
    q_spec = pl.BlockSpec((1, qb, hd), lambda h, i, p: (h, i, 0))
    kv_spec = pl.BlockSpec((1, seq, hd), lambda h, i, p: (h, 0, 0))
    lse_spec = pl.BlockSpec((1, qb, 1), lambda h, i, p: (h, i, 0))
    o_spec = pl.BlockSpec((1, 1, qb, hd), lambda h, i, p: (i // per, h, i % per, 0))
    return pl.pallas_call(
        functools.partial(_fwd_kernel, scale),
        out_shape=(jax.ShapeDtypeStruct((groups, heads, seq // groups, hd), jnp.bfloat16),
                   jax.ShapeDtypeStruct((heads, seq, 1), jnp.float32)),
        grid_spec=pltpu.PrefetchScalarGridSpec(
            num_scalar_prefetch=1, grid=grid,
            in_specs=[q_spec, kv_spec, kv_spec],
            out_specs=[o_spec, lse_spec]),
        compiler_params=pltpu.CompilerParams(
            dimension_semantics=("arbitrary", "arbitrary"),
            vmem_limit_bytes=48 * 1024 * 1024),
        cost_estimate=pl.CostEstimate(
            flops=4 * heads * seq * seq * hd, transcendentals=heads * seq * seq,
            bytes_accessed=4 * heads * seq * hd * 2),
    )(prefix, q, k, v)


def attn_backward(prefix, q, k, v, grad_out, lse, scale, groups):
    heads, seq, hd = q.shape
    qb = min(ATT_QB, seq // groups)
    per = seq // groups // qb
    grid = (heads, seq // qb)
    q_spec = pl.BlockSpec((1, qb, hd), lambda h, i, p: (h, i, 0))
    kv_spec = pl.BlockSpec((1, seq, hd), lambda h, i, p: (h, 0, 0))
    lse_spec = pl.BlockSpec((1, qb, 1), lambda h, i, p: (h, i, 0))
    g_spec = pl.BlockSpec((groups, 3, 1, seq // groups, hd), lambda h, i, p: (0, 0, h, 0, 0))
    shape = jax.ShapeDtypeStruct((groups, 3, heads, seq // groups, hd), jnp.bfloat16)
    return pl.pallas_call(
        functools.partial(_bwd_kernel, scale),
        out_shape=shape,
        grid_spec=pltpu.PrefetchScalarGridSpec(
            num_scalar_prefetch=1, grid=grid,
            in_specs=[q_spec, kv_spec, kv_spec, q_spec, lse_spec],
            out_specs=g_spec,
            scratch_shapes=[pltpu.VMEM((seq, hd), jnp.float32),
                            pltpu.VMEM((seq, hd), jnp.float32)]),
        compiler_params=pltpu.CompilerParams(
            dimension_semantics=("arbitrary", "arbitrary"),
            vmem_limit_bytes=48 * 1024 * 1024),
        cost_estimate=pl.CostEstimate(
            flops=10 * heads * seq * seq * hd, transcendentals=heads * seq * seq,
            bytes_accessed=8 * heads * seq * hd * 2),
    )(prefix, q, k, v, grad_out, lse)


def on_device(
    tokens,
    pass_ids,
    prefix,
    cotangent,
    qkv_weight,
    out_weight,
    fc1_weight,
    fc2_weight,
    ln1_gain,
    ln1_bias,
    qv_bias,
    out_bias,
    ln2_gain,
    ln2_bias,
    fc1_bias,
    fc2_bias,
    pass_table,
):
    tp_count = lax.axis_size("tp")
    tp_rank = lax.axis_index("tp")
    local_rows = tokens.shape[0]
    seq_len = local_rows * tp_count
    cols_here = qkv_weight.shape[2]
    heads_here = cols_here // HD
    scale = HD ** (-0.5)
    prefix_len = prefix[0]
    gelu_tanh = partial(jax.nn.gelu, approximate=True)
    fsdp_count = lax.axis_size("fsdp")
    qkv_cols = lax.all_gather(qkv_weight, "fsdp", axis=1, tiled=True)
    qkv_full = qkv_cols
    hidden_here = fc1_weight.shape[1]
    qv_here = lax.dynamic_slice_in_dim(qv_bias, tp_rank * cols_here, cols_here, 1)
    one_hot = (pass_ids[:, None] == jnp.arange(NPASS, dtype=jnp.int32)[None, :]).astype(jnp.float32)
    block_in = tokens.astype(jnp.float32) + jnp.dot(
        one_hot, pass_table, precision=HIGH, preferred_element_type=jnp.float32
    )
    normed, unit_one, inv_one = norm_forward(block_in, ln1_gain, ln1_bias)
    normed_all = lax.all_gather(normed.astype(jnp.bfloat16), "tp", axis=0, tiled=True)
    shards = (out_weight, fc1_weight, fc2_weight)
    packed = jnp.concatenate([piece.reshape(-1) for piece in shards])
    packed, qkv_cols, normed_all = lax.optimization_barrier((packed, qkv_cols, normed_all))
    qkv_full = qkv_cols
    gathered = lax.all_gather(packed, "fsdp", axis=0, tiled=False)
    qkv_copies = jnp.broadcast_to(qkv_cols[None], (tp_count,) + qkv_cols.shape)
    qkv_all = lax.all_to_all(qkv_copies, "tp", 0, 0, tiled=True)
    grad_rows = lax.all_gather(cotangent, "tp", axis=0, tiled=True)
    projected = jnp.einsum("rd,kdc->krc", normed_all, qkv_full, preferred_element_type=jnp.float32)
    queries = (projected[0] + qv_here[0]).astype(jnp.bfloat16).reshape(seq_len, heads_here, HD)
    keys_all = projected[1].astype(jnp.bfloat16).reshape(seq_len, heads_here, HD)
    values_all = (projected[2] + qv_here[1]).astype(jnp.bfloat16).reshape(seq_len, heads_here, HD)
    q_heads = jnp.transpose(queries, (1, 0, 2))
    k_heads = jnp.transpose(keys_all, (1, 0, 2))
    v_heads = jnp.transpose(values_all, (1, 0, 2))
    mixed, log_mass = attn_forward(prefix, q_heads, k_heads, v_heads, scale, tp_count)
    mixed, qkv_all = lax.optimization_barrier((mixed, qkv_all))
    pieces = []
    offset = 0
    for piece in shards:
        size = piece.size
        pieces.append(gathered[:, offset : offset + size].reshape((fsdp_count,) + piece.shape))
        offset += size
    out_full = jnp.moveaxis(pieces[0], 0, 1).reshape(out_weight.shape[0], -1)
    fc1_part = pieces[1].reshape(-1, fc1_weight.shape[1])
    fc2_part = jnp.moveaxis(pieces[2], 0, 1).reshape(fc2_weight.shape[0], -1)
    out_all = lax.all_gather(out_full, "tp", axis=0, tiled=True)
    mixed, grad_rows, out_all, fc1_part, fc2_part = lax.optimization_barrier(
        (mixed, grad_rows, out_all, fc1_part, fc2_part)
    )
    mixed_rows = lax.all_to_all(mixed, "tp", 0, 0, tiled=True)
    middle = (
        block_in
        + jnp.einsum(
            "shre,shem->rm",
            mixed_rows,
            out_all.reshape(tp_count, heads_here, HD, -1),
            preferred_element_type=jnp.float32,
        )
        + out_bias
    )
    normed_two, unit_two, inv_two = norm_forward(middle, ln2_gain, ln2_bias)
    normed_two = normed_two.astype(jnp.bfloat16)
    grad_top = cotangent.astype(jnp.float32)
    fc1_bias_here = lax.dynamic_slice_in_dim(fc1_bias, tp_rank * hidden_here, hidden_here, 0)
    normed_rows = lax.all_gather(normed_two, "tp", axis=0, tiled=True)
    before = jnp.dot(normed_rows, fc1_part, preferred_element_type=jnp.float32) + fc1_bias_here
    hidden = gelu_tanh(before).astype(jnp.bfloat16)
    fc2_partial = jnp.dot(hidden, fc2_part, preferred_element_type=jnp.float32).astype(jnp.bfloat16)
    grad_hidden = matmul_nt(grad_rows, fc2_part)
    grad_before = jax.vjp(gelu_tanh, before)[1](grad_hidden)[0].astype(jnp.bfloat16)
    grad_fc1_bias = lax.dynamic_update_slice_in_dim(
        jnp.zeros(fc1_bias.shape, jnp.float32),
        jnp.sum(grad_before.astype(jnp.float32), axis=0),
        tp_rank * hidden_here,
        0,
    )
    grad_fc1 = matmul_tn(normed_rows, grad_before)
    grad_fc2 = matmul_tn(hidden, grad_rows)
    grad_normed_two = lax.psum_scatter(
        matmul_nt(grad_before, fc1_part).astype(jnp.bfloat16), "tp", scatter_dimension=0, tiled=True
    ).astype(jnp.float32)
    grad_normed_two, fc2_partial, grad_fc1, grad_fc2 = lax.optimization_barrier(
        (grad_normed_two, fc2_partial, grad_fc1, grad_fc2)
    )
    grad_fc2_bias = jnp.sum(grad_top, axis=0)
    grad_from_norm, grad_ln2_gain, grad_ln2_bias = norm_backward(
        grad_normed_two, unit_two, inv_two, ln2_gain
    )
    grad_middle = grad_top + grad_from_norm
    grad_out_bias = jnp.sum(grad_middle, axis=0)
    width = grad_fc1.shape[1]
    fsdp_count = lax.axis_size("fsdp")
    dense_grads = (
        grad_fc1.reshape(fsdp_count, -1, width),
        jnp.moveaxis(grad_fc2.reshape(grad_fc2.shape[0], fsdp_count, -1), 1, 0),
    )
    dense_packed = jnp.concatenate(
        [g.reshape(fsdp_count, -1, width) for g in dense_grads], axis=1
    ).astype(jnp.bfloat16)
    grad_attn_rows = lax.all_gather(grad_middle.astype(jnp.bfloat16), "tp", axis=0, tiled=True)
    fc2_partial, grad_attn_rows, dense_packed = lax.optimization_barrier(
        (fc2_partial, grad_attn_rows, dense_packed)
    )
    fc2_parts = lax.all_to_all(
        fc2_partial.reshape(tp_count, local_rows, -1), "tp", 0, 0, tiled=True
    )
    result = middle + jnp.sum(fc2_parts.astype(jnp.float32), axis=0) + fc2_bias
    dense_summed = lax.psum_scatter(
        dense_packed.reshape(-1, width), "fsdp", scatter_dimension=0, tiled=True
    ).reshape(1, -1).astype(jnp.float32)
    grad_mixed = (
        matmul_nt(grad_attn_rows, out_full).astype(jnp.bfloat16).reshape(seq_len, heads_here, HD)
    )
    grad_all = attn_backward(
        prefix, q_heads, k_heads, v_heads, jnp.transpose(grad_mixed, (1, 0, 2)), log_mass, scale,
        tp_count,
    )
    grad_all, result, dense_summed, grad_attn_late = lax.optimization_barrier(
        (grad_all, result, dense_summed, grad_attn_rows)
    )
    grad_out_w = jnp.einsum(
        "thre,trm->hem",
        mixed,
        grad_attn_late.reshape(tp_count, local_rows, -1),
        preferred_element_type=jnp.float32,
    ).reshape(cols_here, -1)
    grad_q_heads, grad_v_heads = grad_all[:, 0], grad_all[:, 2]
    grad_qv_here = jnp.stack(
        [
            jnp.sum(grad_q_heads.astype(jnp.float32), axis=(0, 2)).reshape(-1),
            jnp.sum(grad_v_heads.astype(jnp.float32), axis=(0, 2)).reshape(-1),
        ],
        axis=0,
    )
    grad_qv_bias = lax.dynamic_update_slice_in_dim(
        jnp.zeros(qv_bias.shape, jnp.float32), grad_qv_here, tp_rank * cols_here, 1
    )
    normed_groups = normed_all.reshape(tp_count, local_rows, -1)
    grad_qkv_w = jnp.einsum(
        "trd,tkhre->kdhe", normed_groups, grad_all, preferred_element_type=jnp.float32
    ).reshape(3, normed_all.shape[1], cols_here)
    grad_rows_all = lax.all_to_all(grad_all, "tp", 0, 0, tiled=True)
    qkv_split = qkv_all.reshape(tp_count, 3, qkv_all.shape[2], heads_here, HD)
    grad_normed = jnp.einsum(
        "skhre,skdhe->rd", grad_rows_all, qkv_split, preferred_element_type=jnp.float32
    )
    dense_shards = []
    offset = 0
    for g in dense_grads:
        size = g[0].size
        dense_shards.append(dense_summed[0, offset : offset + size].reshape(g.shape[1:]))
        offset += size
    fc1_shard, fc2_shard = dense_shards
    grad_in_norm, grad_ln1_gain, grad_ln1_bias = norm_backward(
        grad_normed, unit_one, inv_one, ln1_gain
    )
    grad_input = grad_middle + grad_in_norm
    grad_table = lax.dot_general(
        one_hot,
        grad_input,
        (((0,), (0,)), ((), ())),
        precision=HIGH,
        preferred_element_type=jnp.float32,
    )
    tail_grads = (
        jnp.moveaxis(grad_qkv_w.reshape(3, fsdp_count, -1, cols_here), 1, 0),
        jnp.moveaxis(grad_out_w.reshape(grad_out_w.shape[0], fsdp_count, -1), 1, 0),
    )
    tail_packed = jnp.concatenate([g.reshape(fsdp_count, -1, width) for g in tail_grads], axis=1)
    tail_summed = lax.psum_scatter(
        tail_packed.reshape(-1, width), "fsdp", scatter_dimension=0, tiled=True
    ).reshape(-1)
    tail_shards = []
    offset = 0
    for g in tail_grads:
        size = g[0].size
        tail_shards.append(tail_summed[offset : offset + size].reshape(g.shape[1:]))
        offset += size
    qkv_shard, out_shard = tail_shards
    summed = lax.psum(
        (
            grad_ln1_gain,
            grad_ln1_bias,
            grad_qv_bias,
            grad_out_bias,
            grad_ln2_gain,
            grad_ln2_bias,
            grad_fc1_bias,
            grad_fc2_bias,
            grad_table,
        ),
        ("fsdp", "tp"),
    )
    return (
        result.astype(jnp.bfloat16),
        grad_input,
        qkv_shard,
        out_shard,
        fc1_shard,
        fc2_shard,
        summed[0],
        summed[1],
        summed[2],
        summed[3],
        summed[4],
        summed[5],
        summed[6],
        summed[7],
        summed[8],
    )


def solution(mesh):
    placed = (
        P(("fsdp", "tp"), None),
        P(("fsdp", "tp")),
        P("fsdp"),
        P(("fsdp", "tp"), None),
        P(None, "fsdp", "tp"),
        P("tp", "fsdp"),
        P("fsdp", "tp"),
        P("tp", "fsdp"),
        P(),
        P(),
        P(),
        P(),
        P(),
        P(),
        P(),
        P(),
        P(),
    )
    return jax.shard_map(
        on_device,
        mesh=mesh,
        in_specs=placed,
        out_specs=(
            P(("fsdp", "tp"), None),
            P(("fsdp", "tp"), None),
            P(None, "fsdp", "tp"),
            P("tp", "fsdp"),
            P("fsdp", "tp"),
            P("tp", "fsdp"),
            P(),
            P(),
            P(),
            P(),
            P(),
            P(),
            P(),
            P(),
            P(),
        ),
        check_vma=False,
    )
```

```python
import functools
from functools import partial

import jax
import jax.numpy as jnp
from jax import lax
from jax.experimental import pallas as pl
from jax.experimental.pallas import tpu as pltpu
from jax.sharding import PartitionSpec as P

HD = 64
NPASS = 5
QBLOCK = 512


HIGH = lax.Precision.HIGHEST
EPS = 1e-05
NEG_FILL = -1e30


def norm_forward(rows_in, gain, shift):
    center = rows_in - jnp.mean(rows_in, axis=-1, keepdims=True)
    scale_inv = lax.rsqrt(jnp.mean(center * center, axis=-1, keepdims=True) + EPS)
    unit_rows = center * scale_inv
    return (unit_rows * gain + shift, unit_rows, scale_inv)


def norm_backward(grad_out, unit_rows, scale_inv, gain):
    grad_unit = grad_out * gain
    first_mean = jnp.mean(grad_unit, axis=-1, keepdims=True)
    second_mean = jnp.mean(grad_unit * unit_rows, axis=-1, keepdims=True)
    grad_rows = scale_inv * (grad_unit - first_mean - unit_rows * second_mean)
    return (grad_rows, jnp.sum(grad_out * unit_rows, axis=0), jnp.sum(grad_out, axis=0))


def matmul_nt(left, right):
    return lax.dot_general(
        left, right, (((1,), (1,)), ((), ())), preferred_element_type=jnp.float32
    )


def matmul_tn(left, right):
    return lax.dot_general(
        left, right, (((0,), (0,)), ((), ())), preferred_element_type=jnp.float32
    )


def block_scores(query_block, keys_all, row_start, prefix_len, scale):
    raw = (
        jnp.einsum("qhe,khe->hqk", query_block, keys_all, preferred_element_type=jnp.float32)
        * scale
    )
    row_ids = row_start + jnp.arange(query_block.shape[0], dtype=jnp.int32)
    col_ids = jnp.arange(keys_all.shape[0], dtype=jnp.int32)
    allowed = (col_ids[None, :] <= row_ids[:, None]) | (col_ids[None, :] < prefix_len)
    return jnp.where(allowed[None], raw, NEG_FILL)


ATT_QB = 512


def _mask(prefix_len, qb, rows, cols):
    row = qb * rows + lax.broadcasted_iota(jnp.int32, (rows, cols), 0)
    col = lax.broadcasted_iota(jnp.int32, (rows, cols), 1)
    return (col <= row) | (col < prefix_len)


def _nt(a, b):
    return lax.dot_general(a, b, (((1,), (1,)), ((), ())), preferred_element_type=jnp.float32)


def _tn(a, b):
    return lax.dot_general(a, b, (((0,), (0,)), ((), ())), preferred_element_type=jnp.float32)


def _fwd_kernel(scale, prefix_ref, q_ref, k_ref, v_ref, o_ref, lse_ref):
    qb = pl.program_id(1)
    q = q_ref[0]
    rows, cols = q.shape[0], k_ref.shape[1]
    scores = _nt(q, k_ref[0]) * scale
    scores = jnp.where(_mask(prefix_ref[0], qb, rows, cols), scores, NEG_FILL)
    peak = jnp.max(scores, axis=-1, keepdims=True)
    expo = jnp.exp(scores - peak)
    total = jnp.sum(expo, axis=-1, keepdims=True)
    probs_low = (expo / total).astype(jnp.bfloat16)
    out = jnp.dot(probs_low, v_ref[0], preferred_element_type=jnp.float32)
    o_ref[0, 0] = out.astype(o_ref.dtype)
    lse_ref[0] = peak + jnp.log(total)


def _bwd_kernel(scale, prefix_ref, q_ref, k_ref, v_ref, do_ref, lse_ref,
                g_ref, dk_acc, dv_acc):
    qb = pl.program_id(1)

    @pl.when(qb == 0)
    def _():
        dk_acc[...] = jnp.zeros_like(dk_acc)
        dv_acc[...] = jnp.zeros_like(dv_acc)

    q = q_ref[0]
    k = k_ref[0]
    grad_out = do_ref[0]
    rows, cols = q.shape[0], k.shape[0]
    scores = _nt(q, k) * scale
    scores = jnp.where(_mask(prefix_ref[0], qb, rows, cols), scores, NEG_FILL)
    probs = jnp.exp(scores - lse_ref[0])
    dv_acc[...] += _tn(probs.astype(jnp.bfloat16), grad_out)
    grad_probs = _nt(grad_out, v_ref[0])
    inner = jnp.sum(probs * grad_probs, axis=-1, keepdims=True)
    grad_scores = (probs * (grad_probs - inner)).astype(jnp.bfloat16)
    groups, rows_per = g_ref.shape[0], g_ref.shape[3]
    per = rows_per // rows
    start = pl.multiple_of((qb % per) * rows, rows)
    g_ref[qb // per, 0, 0, pl.ds(start, rows), :] = (
        jnp.dot(grad_scores, k, preferred_element_type=jnp.float32) * scale
    ).astype(g_ref.dtype)
    dk_acc[...] += _tn(grad_scores, q)

    @pl.when(qb == pl.num_programs(1) - 1)
    def _():
        hd = g_ref.shape[4]
        g_ref[:, 1, 0] = (dk_acc[...] * scale).astype(g_ref.dtype).reshape(groups, rows_per, hd)
        g_ref[:, 2, 0] = dv_acc[...].astype(g_ref.dtype).reshape(groups, rows_per, hd)


def attn_forward(prefix, q, k, v, scale, groups):
    heads, seq, hd = q.shape
    qb = min(ATT_QB, seq // groups)
    per = seq // groups // qb
    grid = (heads, seq // qb)
    q_spec = pl.BlockSpec((1, qb, hd), lambda h, i, p: (h, i, 0))
    kv_spec = pl.BlockSpec((1, seq, hd), lambda h, i, p: (h, 0, 0))
    lse_spec = pl.BlockSpec((1, qb, 1), lambda h, i, p: (h, i, 0))
    o_spec = pl.BlockSpec((1, 1, qb, hd), lambda h, i, p: (i // per, h, i % per, 0))
    return pl.pallas_call(
        functools.partial(_fwd_kernel, scale),
        out_shape=(jax.ShapeDtypeStruct((groups, heads, seq // groups, hd), jnp.bfloat16),
                   jax.ShapeDtypeStruct((heads, seq, 1), jnp.float32)),
        grid_spec=pltpu.PrefetchScalarGridSpec(
            num_scalar_prefetch=1, grid=grid,
            in_specs=[q_spec, kv_spec, kv_spec],
            out_specs=[o_spec, lse_spec]),
        compiler_params=pltpu.CompilerParams(
            dimension_semantics=("arbitrary", "arbitrary"),
            vmem_limit_bytes=48 * 1024 * 1024),
        cost_estimate=pl.CostEstimate(
            flops=4 * heads * seq * seq * hd, transcendentals=heads * seq * seq,
            bytes_accessed=4 * heads * seq * hd * 2),
    )(prefix, q, k, v)


def attn_backward(prefix, q, k, v, grad_out, lse, scale, groups):
    heads, seq, hd = q.shape
    qb = min(ATT_QB, seq // groups)
    per = seq // groups // qb
    grid = (heads, seq // qb)
    q_spec = pl.BlockSpec((1, qb, hd), lambda h, i, p: (h, i, 0))
    kv_spec = pl.BlockSpec((1, seq, hd), lambda h, i, p: (h, 0, 0))
    lse_spec = pl.BlockSpec((1, qb, 1), lambda h, i, p: (h, i, 0))
    g_spec = pl.BlockSpec((groups, 3, 1, seq // groups, hd), lambda h, i, p: (0, 0, h, 0, 0))
    shape = jax.ShapeDtypeStruct((groups, 3, heads, seq // groups, hd), jnp.bfloat16)
    return pl.pallas_call(
        functools.partial(_bwd_kernel, scale),
        out_shape=shape,
        grid_spec=pltpu.PrefetchScalarGridSpec(
            num_scalar_prefetch=1, grid=grid,
            in_specs=[q_spec, kv_spec, kv_spec, q_spec, lse_spec],
            out_specs=g_spec,
            scratch_shapes=[pltpu.VMEM((seq, hd), jnp.float32),
                            pltpu.VMEM((seq, hd), jnp.float32)]),
        compiler_params=pltpu.CompilerParams(
            dimension_semantics=("arbitrary", "arbitrary"),
            vmem_limit_bytes=48 * 1024 * 1024),
        cost_estimate=pl.CostEstimate(
            flops=10 * heads * seq * seq * hd, transcendentals=heads * seq * seq,
            bytes_accessed=8 * heads * seq * hd * 2),
    )(prefix, q, k, v, grad_out, lse)


def on_device(
    tokens,
    pass_ids,
    prefix,
    cotangent,
    qkv_weight,
    out_weight,
    fc1_weight,
    fc2_weight,
    ln1_gain,
    ln1_bias,
    qv_bias,
    out_bias,
    ln2_gain,
    ln2_bias,
    fc1_bias,
    fc2_bias,
    pass_table,
):
    tp_count = lax.axis_size("tp")
    tp_rank = lax.axis_index("tp")
    local_rows = tokens.shape[0]
    seq_len = local_rows * tp_count
    cols_here = qkv_weight.shape[2]
    heads_here = cols_here // HD
    scale = HD ** (-0.5)
    prefix_len = prefix[0]
    gelu_tanh = partial(jax.nn.gelu, approximate=True)
    fsdp_count = lax.axis_size("fsdp")
    qkv_cols = lax.all_gather(qkv_weight, "fsdp", axis=1, tiled=True)
    qkv_full = qkv_cols
    hidden_here = fc1_weight.shape[1]
    qv_here = lax.dynamic_slice_in_dim(qv_bias, tp_rank * cols_here, cols_here, 1)
    one_hot = (pass_ids[:, None] == jnp.arange(NPASS, dtype=jnp.int32)[None, :]).astype(jnp.float32)
    block_in = tokens.astype(jnp.float32) + jnp.dot(
        one_hot, pass_table, precision=HIGH, preferred_element_type=jnp.float32
    )
    normed, unit_one, inv_one = norm_forward(block_in, ln1_gain, ln1_bias)
    normed_all = lax.all_gather(normed.astype(jnp.bfloat16), "tp", axis=0, tiled=True)
    shards = (out_weight, fc1_weight, fc2_weight)
    packed = jnp.concatenate([piece.reshape(-1) for piece in shards])
    packed, qkv_cols, normed_all = lax.optimization_barrier((packed, qkv_cols, normed_all))
    qkv_full = qkv_cols
    gathered = lax.all_gather(packed, "fsdp", axis=0, tiled=False)
    qkv_copies = jnp.broadcast_to(qkv_cols[None], (tp_count,) + qkv_cols.shape)
    qkv_all = lax.all_to_all(qkv_copies, "tp", 0, 0, tiled=True)
    grad_rows = lax.all_gather(cotangent, "tp", axis=0, tiled=True)
    projected = jnp.einsum("rd,kdc->krc", normed_all, qkv_full, preferred_element_type=jnp.float32)
    queries = (projected[0] + qv_here[0]).astype(jnp.bfloat16).reshape(seq_len, heads_here, HD)
    keys_all = projected[1].astype(jnp.bfloat16).reshape(seq_len, heads_here, HD)
    values_all = (projected[2] + qv_here[1]).astype(jnp.bfloat16).reshape(seq_len, heads_here, HD)
    q_heads = jnp.transpose(queries, (1, 0, 2))
    k_heads = jnp.transpose(keys_all, (1, 0, 2))
    v_heads = jnp.transpose(values_all, (1, 0, 2))
    mixed, log_mass = attn_forward(prefix, q_heads, k_heads, v_heads, scale, tp_count)
    mixed, qkv_all = lax.optimization_barrier((mixed, qkv_all))
    pieces = []
    offset = 0
    for piece in shards:
        size = piece.size
        pieces.append(gathered[:, offset : offset + size].reshape((fsdp_count,) + piece.shape))
        offset += size
    out_full = jnp.moveaxis(pieces[0], 0, 1).reshape(out_weight.shape[0], -1)
    fc1_part = pieces[1].reshape(-1, fc1_weight.shape[1])
    fc2_part = jnp.moveaxis(pieces[2], 0, 1).reshape(fc2_weight.shape[0], -1)
    out_all = lax.all_gather(out_full, "tp", axis=0, tiled=True)
    mixed, grad_rows, out_all, fc1_part, fc2_part = lax.optimization_barrier(
        (mixed, grad_rows, out_all, fc1_part, fc2_part)
    )
    mixed_rows = lax.all_to_all(mixed, "tp", 0, 0, tiled=True)
    middle = (
        block_in
        + jnp.einsum(
            "shre,shem->rm",
            mixed_rows,
            out_all.reshape(tp_count, heads_here, HD, -1),
            preferred_element_type=jnp.float32,
        )
        + out_bias
    )
    normed_two, unit_two, inv_two = norm_forward(middle, ln2_gain, ln2_bias)
    normed_two = normed_two.astype(jnp.bfloat16)
    grad_top = cotangent.astype(jnp.float32)
    fc1_bias_here = lax.dynamic_slice_in_dim(fc1_bias, tp_rank * hidden_here, hidden_here, 0)
    normed_rows = lax.all_gather(normed_two, "tp", axis=0, tiled=True)
    before = jnp.dot(normed_rows, fc1_part, preferred_element_type=jnp.float32) + fc1_bias_here
    hidden = gelu_tanh(before).astype(jnp.bfloat16)
    fc2_partial = jnp.dot(hidden, fc2_part, preferred_element_type=jnp.float32).astype(jnp.bfloat16)
    grad_hidden = matmul_nt(grad_rows, fc2_part)
    grad_before = jax.vjp(gelu_tanh, before)[1](grad_hidden)[0].astype(jnp.bfloat16)
    grad_fc1_bias = lax.dynamic_update_slice_in_dim(
        jnp.zeros(fc1_bias.shape, jnp.float32),
        jnp.sum(grad_before.astype(jnp.float32), axis=0),
        tp_rank * hidden_here,
        0,
    )
    grad_fc1 = matmul_tn(normed_rows, grad_before)
    grad_fc2 = matmul_tn(hidden, grad_rows)
    grad_normed_two = lax.psum_scatter(
        matmul_nt(grad_before, fc1_part).astype(jnp.bfloat16), "tp", scatter_dimension=0, tiled=True
    ).astype(jnp.float32)
    grad_normed_two, fc2_partial, grad_fc1, grad_fc2 = lax.optimization_barrier(
        (grad_normed_two, fc2_partial, grad_fc1, grad_fc2)
    )
    grad_fc2_bias = jnp.sum(grad_top, axis=0)
    grad_from_norm, grad_ln2_gain, grad_ln2_bias = norm_backward(
        grad_normed_two, unit_two, inv_two, ln2_gain
    )
    grad_middle = grad_top + grad_from_norm
    grad_out_bias = jnp.sum(grad_middle, axis=0)
    width = grad_fc1.shape[1]
    fsdp_count = lax.axis_size("fsdp")
    dense_grads = (
        grad_fc1.reshape(fsdp_count, -1, width),
        jnp.moveaxis(grad_fc2.reshape(grad_fc2.shape[0], fsdp_count, -1), 1, 0),
    )
    dense_packed = jnp.concatenate(
        [g.reshape(fsdp_count, -1, width) for g in dense_grads], axis=1
    ).astype(jnp.bfloat16)
    grad_attn_rows = lax.all_gather(grad_middle.astype(jnp.bfloat16), "tp", axis=0, tiled=True)
    fc2_partial, grad_attn_rows, dense_packed = lax.optimization_barrier(
        (fc2_partial, grad_attn_rows, dense_packed)
    )
    fc2_parts = lax.all_to_all(
        fc2_partial.reshape(tp_count, local_rows, -1), "tp", 0, 0, tiled=True
    )
    result = middle + jnp.sum(fc2_parts.astype(jnp.float32), axis=0) + fc2_bias
    grad_out_w = jnp.einsum(
        "thre,trm->hem",
        mixed,
        grad_attn_rows.reshape(tp_count, local_rows, -1),
        preferred_element_type=jnp.float32,
    ).reshape(cols_here, -1)
    dense_summed = lax.psum_scatter(
        dense_packed.reshape(-1, width), "fsdp", scatter_dimension=0, tiled=True
    ).reshape(1, -1).astype(jnp.float32)
    grad_mixed = (
        matmul_nt(grad_attn_rows, out_full).astype(jnp.bfloat16).reshape(seq_len, heads_here, HD)
    )
    grad_all = attn_backward(
        prefix, q_heads, k_heads, v_heads, jnp.transpose(grad_mixed, (1, 0, 2)), log_mass, scale,
        tp_count,
    )
    grad_all, result, dense_summed = lax.optimization_barrier((grad_all, result, dense_summed))
    grad_q_heads, grad_v_heads = grad_all[:, 0], grad_all[:, 2]
    grad_qv_here = jnp.stack(
        [
            jnp.sum(grad_q_heads.astype(jnp.float32), axis=(0, 2)).reshape(-1),
            jnp.sum(grad_v_heads.astype(jnp.float32), axis=(0, 2)).reshape(-1),
        ],
        axis=0,
    )
    grad_qv_bias = lax.dynamic_update_slice_in_dim(
        jnp.zeros(qv_bias.shape, jnp.float32), grad_qv_here, tp_rank * cols_here, 1
    )
    normed_groups = normed_all.reshape(tp_count, local_rows, -1)
    grad_qkv_w = jnp.einsum(
        "trd,tkhre->kdhe", normed_groups, grad_all, preferred_element_type=jnp.float32
    ).reshape(3, normed_all.shape[1], cols_here)
    grad_rows_all = lax.all_to_all(grad_all, "tp", 0, 0, tiled=True)
    qkv_split = qkv_all.reshape(tp_count, 3, qkv_all.shape[2], heads_here, HD)
    grad_normed = jnp.einsum(
        "skhre,skdhe->rd", grad_rows_all, qkv_split, preferred_element_type=jnp.float32
    )
    dense_shards = []
    offset = 0
    for g in dense_grads:
        size = g[0].size
        dense_shards.append(dense_summed[0, offset : offset + size].reshape(g.shape[1:]))
        offset += size
    fc1_shard, fc2_shard = dense_shards
    grad_in_norm, grad_ln1_gain, grad_ln1_bias = norm_backward(
        grad_normed, unit_one, inv_one, ln1_gain
    )
    grad_input = grad_middle + grad_in_norm
    grad_table = lax.dot_general(
        one_hot,
        grad_input,
        (((0,), (0,)), ((), ())),
        precision=HIGH,
        preferred_element_type=jnp.float32,
    )
    tail_grads = (
        jnp.moveaxis(grad_qkv_w.reshape(3, fsdp_count, -1, cols_here), 1, 0),
        jnp.moveaxis(grad_out_w.reshape(grad_out_w.shape[0], fsdp_count, -1), 1, 0),
    )
    tail_packed = jnp.concatenate([g.reshape(fsdp_count, -1, width) for g in tail_grads], axis=1)
    tail_summed = lax.psum_scatter(
        tail_packed.reshape(-1, width).astype(jnp.bfloat16), "fsdp", scatter_dimension=0, tiled=True
    ).reshape(-1).astype(jnp.float32)
    tail_shards = []
    offset = 0
    for g in tail_grads:
        size = g[0].size
        tail_shards.append(tail_summed[offset : offset + size].reshape(g.shape[1:]))
        offset += size
    qkv_shard, out_shard = tail_shards
    summed = lax.psum(
        (
            grad_ln1_gain,
            grad_ln1_bias,
            grad_qv_bias,
            grad_out_bias,
            grad_ln2_gain,
            grad_ln2_bias,
            grad_fc1_bias,
            grad_fc2_bias,
            grad_table,
        ),
        ("fsdp", "tp"),
    )
    return (
        result.astype(jnp.bfloat16),
        grad_input,
        qkv_shard,
        out_shard,
        fc1_shard,
        fc2_shard,
        summed[0],
        summed[1],
        summed[2],
        summed[3],
        summed[4],
        summed[5],
        summed[6],
        summed[7],
        summed[8],
    )


def solution(mesh):
    placed = (
        P(("fsdp", "tp"), None),
        P(("fsdp", "tp")),
        P("fsdp"),
        P(("fsdp", "tp"), None),
        P(None, "fsdp", "tp"),
        P("tp", "fsdp"),
        P("fsdp", "tp"),
        P("tp", "fsdp"),
        P(),
        P(),
        P(),
        P(),
        P(),
        P(),
        P(),
        P(),
        P(),
    )
    return jax.shard_map(
        on_device,
        mesh=mesh,
        in_specs=placed,
        out_specs=(
            P(("fsdp", "tp"), None),
            P(("fsdp", "tp"), None),
            P(None, "fsdp", "tp"),
            P("tp", "fsdp"),
            P("fsdp", "tp"),
            P("tp", "fsdp"),
            P(),
            P(),
            P(),
            P(),
            P(),
            P(),
            P(),
            P(),
            P(),
        ),
        check_vma=False,
    )
```
